256 devices in a mesh: depth: 8 (over z_hi, x), lat: 32 (over y, z_lo, core).
Axes of the slice: x: 4, y: 4, z: 8 (z_hi: 2, z_lo: 4; z = z_hi * 4 + z_lo), core: 2. Of those that a mesh axis runs over, the one named last changes fastest.
Arguments:
- displacement: float32 [3, 64, 256, 256], P(None, 'depth', 'lat'), may hold values from -6 to 6
- velocity: float32 [3, 64, 256, 256], P(None, 'depth', 'lat'), may hold values from -6 to 6
- inverse_mass: float32 [64, 256, 256], P('depth', 'lat'), may hold values from 0.5 to 2
- material: int32 [64, 256, 256], P('depth', 'lat'), may hold values from 0 to 7
- dilation_table: float32 [8], replicated, may hold values from 0.5 to 2
- shear_table: float32 [8], replicated, may hold values from 0.5 to 2
- stiffness_pair: float32 [2, 24, 24], replicated, may hold values from -1.5 to 3.5, as said below
- impedance: float32 [3], replicated, may hold values from 0.5 to 2
- bedrock_mask: int32 [256, 256], P('lat'), may hold values 0 or 1
- incident: float32 [6, 3, 256, 256], P(None, None, 'lat'), may hold values from -6 to 6
Outputs:
- new_displacement: float32 [3, 64, 256, 256], P(None, 'depth', 'lat')
- new_velocity: float32 [3, 64, 256, 256], P(None, 'depth', 'lat')
The draws below stay inside these ranges and needn't reach their ends.
Inputs may be any that keep to these rules, and one draw needn't show every extreme that they name: `stiffness_pair`: symmetric positive definite.
All inputs are finite; a program needn't handle non-finite values. No bound on the sum of `bedrock_mask` on one device may be relied on, other than what follows from the above.
Results may differ from the reference program's by a relative error of at most 0.00016.
Values sent between devices are 32-bit elements; how exact they have to be, the bound alone decides.
A program may use at most 64 MiB of HBM per device.

```python
import math
import jax
import jax.numpy as jnp
from jax import lax

NXC = 256
STEPS = 6
NMAT = 8
NZ = 64
NY = 256


def draw_stiffness_pair(key, part):
    factor = jax.random.normal(key, (2, 24, 24), jnp.float32)
    square = jnp.einsum('aij,akj->aik', factor, factor) / 48.0
    return 0.5 * jnp.eye(24, dtype=jnp.float32)[None] + square


def touch_ends(result, stream_key, low, top_value):
    longest = result.shape.index(max(result.shape))
    spots = []
    for shift in (0, 1):
        where = [jax.random.randint(jax.random.fold_in(stream_key, axis), (), 0, length) for axis, length in enumerate(result.shape)]
        where[longest] = (where[longest] + shift) % result.shape[longest]
        spots.append(tuple(where))
    return result.at[spots[0]].set(low).at[spots[1]].set(top_value)


def block_levels(key, dims, shards, least, high):
    def one(dim, shards_of):
        heights = jax.random.uniform(jax.random.fold_in(jax.random.fold_in(key, 6), dim), (shards_of,), jnp.float32, least / len(shards), high / len(shards))
        return jnp.repeat(jnp.exp(heights), dims[dim] // shards_of).reshape((-1,) + (1,) * (len(dims) - dim - 1))

    loudness = one(*shards[0])
    for cut in shards[1:]:
        loudness = loudness * one(*cut)
    return loudness


def noise(own_key, dims, width, most, shards=(), held_as=jnp.bfloat16):
    drawn = jax.random.normal(own_key, dims, jnp.float32) * width
    if len(shards) > 0:
        drawn = block_levels(own_key, dims, shards, -0.22, 0.18) * drawn
    return jnp.clip(drawn, min=-most, max=most).astype(held_as)


def setup_inputs(seed: int = 0) -> dict:
    key_of = jax.random.split(jax.random.key(seed), 11)
    return {
        "displacement": noise(key_of[0], (3, NZ, NY, NXC), 1.0, 6.0, ((1, 8), (2, 32)), jnp.float32),
        "velocity": noise(key_of[1], (3, NZ, NY, NXC), 1.0, 6.0, ((1, 8), (2, 32)), jnp.float32),
        "inverse_mass": jnp.clip(jnp.exp(math.log(2.0) - 1.3862944 * jax.random.uniform(key_of[2], (NZ, NY, NXC), jnp.float32) ** block_levels(key_of[2], (NZ, NY, NXC), ((0, 8), (1, 32)), -0.2, 0.2)), 0.5, 2.0),
        "material": touch_ends(jax.random.randint(key_of[3], (NZ, NY, NXC), 0, NMAT), jax.random.fold_in(key_of[3], 1), 0, NMAT - 1).astype(jnp.int32),
        "dilation_table": jnp.clip(jnp.exp(jax.random.uniform(key_of[4], (NMAT,), jnp.float32, math.log(0.5), math.log(2.0))), 0.5, 2.0),
        "shear_table": jnp.clip(jnp.exp(jax.random.uniform(key_of[5], (NMAT,), jnp.float32, math.log(0.5), math.log(2.0))), 0.5, 2.0),
        "stiffness_pair": draw_stiffness_pair(jax.random.fold_in(key_of[10], 71), 0),
        "impedance": jnp.clip(jnp.exp(jax.random.uniform(key_of[7], (3,), jnp.float32, math.log(0.5), math.log(2.0))), 0.5, 2.0),
        "bedrock_mask": touch_ends((jax.random.randint(key_of[8], (NY, NXC), 0, 2) < 1).astype(jnp.int32), jax.random.fold_in(key_of[8], 1), 0, 1),
        "incident": noise(key_of[9], (STEPS, 3, NY, NXC), 1.0, 6.0, ((2, 32),), jnp.float32),
    }


time_step = 0.1
highest = lax.Precision.HIGHEST


def layer_forces(lower_plane, upper_plane, dilation_layer, shear_layer, stiffness_rows):
    rows_y, cells_x = dilation_layer.shape
    corners = []
    for node_plane in (lower_plane, upper_plane):
        for shift_y in (0, 1):
            for shift_x in (0, 1):
                corners.append(node_plane[:, shift_y:shift_y + rows_y, shift_x:shift_x + cells_x])
    values = jnp.stack(corners).reshape(24, rows_y * cells_x)
    products = jnp.dot(stiffness_rows, values, precision=highest).reshape(2, 8, 3, rows_y, cells_x)
    element_force = dilation_layer * products[0] + shear_layer * products[1]
    sides = [jnp.zeros((3, rows_y + 1, cells_x + 1), jnp.float32), jnp.zeros((3, rows_y + 1, cells_x + 1), jnp.float32)]
    corner = 0
    for side in range(2):
        for shift_y in (0, 1):
            for shift_x in (0, 1):
                contribution = jnp.pad(element_force[corner], ((0, 0), (shift_y, 1 - shift_y), (shift_x, 1 - shift_x)))
                sides[side] = sides[side] + contribution
                corner += 1
    return sides[0], sides[1]


def assemble(displacement, dilation_field, shear_field, stiffness_rows):
    padded = jnp.pad(displacement, ((0, 0), (0, 1), (0, 1), (0, 1)))
    planes = jnp.moveaxis(padded, 1, 0)

    def advance(carried, inputs):
        lower_plane, upper_plane, dilation_layer, shear_layer = inputs
        low_part, high_part = layer_forces(lower_plane, upper_plane, dilation_layer, shear_layer, stiffness_rows)
        return high_part, carried + low_part

    initial = jnp.zeros(planes.shape[1:], jnp.float32)
    unused, layers = lax.scan(advance, initial, (planes[:-1], planes[1:], dilation_field, shear_field))
    return jnp.moveaxis(layers, 0, 1)[:, :, :-1, :-1]


def reference(displacement, velocity, inverse_mass, material, dilation_table, shear_table, stiffness_pair, impedance, bedrock_mask, incident):
    dilation_field = dilation_table[material]
    shear_field = shear_table[material]
    stiffness_rows = stiffness_pair.reshape(48, 24)
    mask_value = bedrock_mask.astype(jnp.float32)
    bottom = NZ - 1
    for instant in range(STEPS):
        forces = assemble(displacement, dilation_field, shear_field, stiffness_rows)
        traction = impedance[:, None, None] * (2.0 * mask_value * incident[instant] - velocity[:, bottom])
        net_force = (-forces).at[:, bottom].add(traction)
        velocity = velocity + time_step * inverse_mass[None] * net_force
        displacement = displacement + time_step * velocity
    return displacement, velocity
```

```python
import functools

import jax
import jax.numpy as jnp
from jax import lax
from jax.experimental import pallas as pl
from jax.experimental.pallas import tpu as pltpu
from jax.sharding import PartitionSpec as P

MESH = pl.DeviceIdType.MESH
DT = 0.1
DIRECTIONS = ((1, 0), (-1, 0), (1, 1), (1, -1), (-1, 1), (-1, -1), (0, 1), (0, -1))
OFFSETS = [(oz, oy, ox) for oz in (-1, 0, 1) for oy in (-1, 0, 1) for ox in (-1, 0, 1)]
CELLS = {-1: (-1,), 0: (-1, 0), 1: (0,)}


def kernel(
    nd, nl,
    u_in, v_in, im_ref, mat_ref, dil_ref, she_ref, k_ref, imp_ref, mask_ref, inc_ref,
    u_out, v_out,
    U, S, R, VS, C, F, MZ, MR, MS, TR,
    send_sem, recv_sem, msend_sem, mrecv_sem,
):
    steps = inc_ref.shape[0]
    nz, ny, nx = im_ref.shape
    d = lax.axis_index("depth")
    l = lax.axis_index("lat")

    def exists(dz, dy):
        return ((d + dz >= 0) & (d + dz < nd)) & ((l + dy >= 0) & (l + dy < nl))

    barrier = pltpu.get_barrier_semaphore()
    for dz, dy in DIRECTIONS:
        @pl.when(exists(dz, dy))
        def _():
            pl.semaphore_signal(barrier, inc=1, device_id=(d + dz, l + dy), device_id_type=MESH)
    partners = 0
    for dz, dy in DIRECTIONS:
        partners = partners + exists(dz, dy).astype(jnp.int32)

    def keep_rows(t, z, c, value):
        S[t, 0, z, c] = value[0:1]
        S[t, 1, z, c] = value[ny - 1:ny]

    for z in range(nz):
        MS[z] = mat_ref[z, ny - 1:ny, :]
        for c in range(3):
            value = u_in[c, z]
            U[0, z + 1, c] = value
            keep_rows(0, z, c, value)
            v_out[c, z] = v_in[c, z]

    @pl.when(d == 0)
    def _():
        U[:, 0] = jnp.zeros_like(U[:, 0])
        R[:, :, 0] = jnp.zeros_like(R[:, :, 0])
        MZ[...] = jnp.full_like(MZ, -1)
        MR[0] = jnp.full_like(MR[0], -1)

    @pl.when(d == nd - 1)
    def _():
        U[:, nz + 1] = jnp.zeros_like(U[:, nz + 1])
        R[:, :, nz + 1] = jnp.zeros_like(R[:, :, nz + 1])

    @pl.when(l == 0)
    def _():
        R[:, 0] = jnp.zeros_like(R[:, 0])
        MR[...] = jnp.full_like(MR, -1)

    @pl.when(l == nl - 1)
    def _():
        R[:, 1] = jnp.zeros_like(R[:, 1])

    pl.semaphore_wait(barrier, partners)

    def copy(t, k):
        dz, dy = DIRECTIONS[k]
        if dy == 0:
            src = U.at[t, nz if dz == 1 else 1]
            dst = U.at[t, 0 if dz == 1 else nz + 1]
        else:
            mine = 1 if dy == 1 else 0
            if dz == 0:
                src, dst = S.at[t, mine], R.at[t, 1 - mine, pl.ds(1, nz)]
            elif dz == 1:
                src, dst = S.at[t, mine, nz - 1], R.at[t, 1 - mine, 0]
            else:
                src, dst = S.at[t, mine, 0], R.at[t, 1 - mine, nz + 1]
        return pltpu.make_async_remote_copy(
            src_ref=src, dst_ref=dst, send_sem=send_sem.at[t, k], recv_sem=recv_sem.at[t, k],
            device_id=(d + dz, l + dy), device_id_type=MESH)

    def mat_copy(k):
        dz, dy = ((1, 0), (1, 1), (0, 1))[k]
        if dy == 0:
            src, dst = mat_ref.at[nz - 1], MZ
        elif dz == 0:
            src, dst = MS, MR.at[pl.ds(1, nz)]
        else:
            src, dst = MS.at[nz - 1], MR.at[0]
        return pltpu.make_async_remote_copy(
            src_ref=src, dst_ref=dst, send_sem=msend_sem.at[k], recv_sem=mrecv_sem.at[k],
            device_id=(d + dz, l + dy), device_id_type=MESH)

    def send(t):
        for k, (dz, dy) in enumerate(DIRECTIONS):
            @pl.when(exists(dz, dy))
            def _():
                copy(t, k).start()

    def arrive(t):
        for k, (dz, dy) in enumerate(DIRECTIONS):
            @pl.when(exists(-dz, -dy))
            def _():
                copy(t, k).wait_recv()

    for k, (dz, dy) in enumerate(((1, 0), (1, 1), (0, 1))):
        @pl.when(exists(dz, dy))
        def _():
            mat_copy(k).start()
    send(0)

    row = lax.broadcasted_iota(jnp.int32, (ny, nx), 0)
    lane = lax.broadcasted_iota(jnp.int32, (ny, nx), 1)

    def fields(layer, mat, row_before):
        before = jnp.where(row == 0, jnp.broadcast_to(row_before, (ny, nx)), pltpu.roll(mat, 1, 0))
        for iy, m in ((1, mat), (0, before)):
            for f, table in ((0, dil_ref), (1, she_ref)):
                value = jnp.zeros((ny, nx), jnp.float32)
                for level in range(table.shape[0]):
                    value = jnp.where(m == level, table[level], value)
                F[layer, f, iy, 1] = value
                F[layer, f, iy, 0] = jnp.where(lane == 0, 0.0, pltpu.roll(value, 1, 1))

    @pl.when(exists(0, -1))
    def _():
        mat_copy(2).wait_recv()

    @pl.loop(0, nz)
    def _(z):
        fields(z + 1, mat_ref[z], MR[z + 1])

    @pl.loop(0, nz)
    def _(i):
        z = nz - 1 - i

        @pl.when(i == nz - 1)
        def _():
            @pl.when(exists(-1, 0))
            def _():
                mat_copy(0).wait_recv()

            @pl.when(exists(-1, -1))
            def _():
                mat_copy(1).wait_recv()

            fields(0, MZ[...], MR[0])

        near = {}
        for ez in (-1, 0):
            for f in (0, 1):
                for iy in (0, 1):
                    for ix in (0, 1):
                        near[ez, f, iy, ix] = F[z + 1 + ez, f, iy, ix]
        for ca in range(3):
            for n, (oz, oy, ox) in enumerate(OFFSETS):
                for cb in range(3):
                    total = None
                    for ez in CELLS[oz]:
                        for ey in CELLS[oy]:
                            for ex in CELLS[ox]:
                                a = 3 * (-4 * ez - 2 * ey - ex) + ca
                                b = 3 * (4 * (oz - ez) + 2 * (oy - ey) + ox - ex) + cb
                                for f in (0, 1):
                                    term = near[ez, f, ey + 1, ex - ox + 1] * k_ref[f, a, b]
                                    total = term if total is None else total + term
                    C[z, (n * 3 + cb) * 3 + ca] = total

    half = nx // 2
    at_bottom = (d == nd - 1).astype(jnp.float32)

    @pl.loop(0, steps)
    def _(t):
        @pl.when(t > 0)
        def _():
            send(t)

        for c in range(3):
            TR[c] = (at_bottom * imp_ref[c]) * (
                2.0 * mask_ref[...].astype(jnp.float32) * inc_ref[t, c] - v_out[c, nz - 1])
        arrive(t)
        for z in range(nz + 2):
            for c in range(3):
                value = U[t, z, c]
                VS[0, z, c] = jnp.where(
                    row == 0, jnp.broadcast_to(R[t, 0, z, c], (ny, nx)), pltpu.roll(value, 1, 0))
                VS[1, z, c] = jnp.where(
                    row == ny - 1, jnp.broadcast_to(R[t, 1, z, c], (ny, nx)),
                    pltpu.roll(value, ny - 1, 0))

        @pl.loop(0, nz)
        def _(z):
            halves = []
            for h in range(2):
                part = pl.ds(h * half, half)
                sums = {}
                for oz in (-1, 0, 1):
                    for oy in (-1, 0, 1):
                        for cb in range(3):
                            if oy == 0:
                                u = U[t, z + 1 + oz, cb, :, part]
                            else:
                                u = VS[(oy + 1) // 2, z + 1 + oz, cb, :, part]
                            for ox in (-1, 0, 1):
                                n = OFFSETS.index((oz, oy, ox))
                                for ca in range(3):
                                    term = C[z, (n * 3 + cb) * 3 + ca, :, part] * u
                                    sums[ca, ox] = term if (ca, ox) not in sums else sums[ca, ox] + term
                halves.append(sums)
            weight = (z == nz - 1).astype(jnp.float32)
            scale = DT * im_ref[z]
            for c in range(3):
                whole = {ox: jnp.concatenate([halves[0][c, ox], halves[1][c, ox]], 1) for ox in (-1, 0, 1)}
                force = (whole[0] + pltpu.roll(whole[1], nx - 1, 1)
                         + jnp.where(lane == 0, 0.0, pltpu.roll(whole[-1], 1, 1)))
                v = v_out[c, z] + scale * (weight * TR[c] - force)
                u = U[t, z + 1, c] + DT * v
                v_out[c, z] = v
                U[t + 1, z + 1, c] = u
                keep_rows(t + 1, z, c, u)

    for z in range(nz):
        for c in range(3):
            u_out[c, z] = U[steps, z + 1, c]

    for k, (dz, dy) in enumerate(((1, 0), (1, 1), (0, 1))):
        @pl.when(exists(dz, dy))
        def _():
            mat_copy(k).wait_send()

    @pl.loop(0, steps)
    def _(t):
        for k, (dz, dy) in enumerate(DIRECTIONS):
            @pl.when(exists(dz, dy))
            def _():
                copy(t, k).wait_send()


def per_device(nd, nl, displacement, velocity, inverse_mass, material, dilation_table, shear_table,
               stiffness_pair, impedance, bedrock_mask, incident):
    _, nz, ny, nx = displacement.shape
    steps = incident.shape[0]
    f32, i32 = jnp.float32, jnp.int32
    vmem = pl.BlockSpec(memory_space=pltpu.VMEM)
    smem = pl.BlockSpec(memory_space=pltpu.SMEM)
    return pl.pallas_call(
        functools.partial(kernel, nd, nl),
        out_shape=[jax.ShapeDtypeStruct(displacement.shape, f32)] * 2,
        in_specs=[vmem, vmem, vmem, vmem, smem, smem, smem, smem, vmem, vmem],
        out_specs=[vmem, vmem],
        scratch_shapes=[
            pltpu.VMEM((steps + 1, nz + 2, 3, ny, nx), f32),
            pltpu.VMEM((steps + 1, 2, nz, 3, 1, nx), f32),
            pltpu.VMEM((steps, 2, nz + 2, 3, 1, nx), f32),
            pltpu.VMEM((2, nz + 2, 3, ny, nx), f32),
            pltpu.VMEM((nz, 243, ny, nx), f32),
            pltpu.VMEM((nz + 1, 2, 2, 2, ny, nx), f32),
            pltpu.VMEM((ny, nx), i32),
            pltpu.VMEM((nz + 1, 1, nx), i32),
            pltpu.VMEM((nz, 1, nx), i32),
            pltpu.VMEM((3, ny, nx), f32),
            pltpu.SemaphoreType.DMA((steps, len(DIRECTIONS))),
            pltpu.SemaphoreType.DMA((steps, len(DIRECTIONS))),
            pltpu.SemaphoreType.DMA((3,)),
            pltpu.SemaphoreType.DMA((3,)),
        ],
        compiler_params=pltpu.CompilerParams(
            collective_id=0, has_side_effects=True, vmem_limit_bytes=48 * 1024 * 1024),
    )(displacement, velocity, inverse_mass, material, dilation_table, shear_table,
      stiffness_pair, impedance, bedrock_mask, incident)


def solution(mesh):
    in_specs = (
        P(None, "depth", "lat", None),
        P(None, "depth", "lat", None),
        P("depth", "lat", None),
        P("depth", "lat", None),
        P(),
        P(),
        P(),
        P(),
        P("lat", None),
        P(None, None, "lat", None),
    )
    out_specs = (P(None, "depth", "lat", None), P(None, "depth", "lat", None))
    return jax.shard_map(
        functools.partial(per_device, mesh.shape["depth"], mesh.shape["lat"]),
        mesh=mesh, in_specs=in_specs, out_specs=out_specs, check_vma=False)
```

```python
import functools

import jax
import jax.numpy as jnp
from jax import lax
from jax.experimental import pallas as pl
from jax.experimental.pallas import tpu as pltpu
from jax.sharding import PartitionSpec as P

MESH = pl.DeviceIdType.MESH
DT = 0.1
f32, bf16, i32 = jnp.float32, jnp.bfloat16, jnp.int32
DIRECTIONS = ((1, 0), (-1, 0), (1, 1), (1, -1), (-1, 1), (-1, -1), (0, 1), (0, -1))

KL = 80
KB = 2 * KL
KP = 512
MO = 384
MH = 512


def kernel(
    nd, nl,
    u_in, v_in, im_in, mat_in, dil_in, she_in, k_in, imp_in, mask_in, inc_in,
    u_out, v_out,
    W, HW, Q, HQ, BI, HB, MI, KV, MV, IV, E, WM, XH, XL, PR, FD, FH, HIM,
    dil, she, imp,
    in_sem, send_sem, recv_sem, qsend_sem, qrecv_sem, bsend_sem, brecv_sem,
):
    steps = inc_in.shape[0]
    rounds = steps // 2
    nz, ny, nx = im_in.shape
    d = lax.axis_index("depth")
    l = lax.axis_index("lat")

    def exists(dz, dy):
        return ((d + dz >= 0) & (d + dz < nd)) & ((l + dy >= 0) & (l + dy < nl))

    own = pl.ds(2, nz)
    loads = [(im_in, Q.at[own, 0]), (mat_in, MI)]
    for c in range(3):
        loads.append((u_in.at[c], W.at[0, own, 1, c]))
        loads.append((v_in.at[c], W.at[0, own, 0, c]))
    first = len(loads)
    loads += [(k_in, KV), (mask_in, MV), (inc_in, IV), (dil_in, dil), (she_in, she), (imp_in, imp)]
    loads = [pltpu.make_async_copy(a, b, in_sem.at[i]) for i, (a, b) in enumerate(loads)]
    for load in loads:
        load.start()

    barrier = pltpu.get_barrier_semaphore()
    partners = 0
    for dz, dy in DIRECTIONS:
        @pl.when(exists(dz, dy))
        def _():
            pl.semaphore_signal(barrier, inc=1, device_id=(d + dz, l + dy), device_id_type=MESH)
        partners = partners + exists(dz, dy).astype(i32)
    for load in loads[:first]:
        load.wait()
    for z in range(nz):
        Q[z + 2, 1] = MI[z].astype(f32)
    pl.semaphore_wait(barrier, partners)

    def remote(src, dst, ss, rs, dz, dy):
        return pltpu.make_async_remote_copy(
            src_ref=src, dst_ref=dst, send_sem=ss, recv_sem=rs,
            device_id=(d + dz, l + dy), device_id_type=MESH)

    def layers(dz):
        if dz == 0:
            return own, own
        return (pl.ds(nz, 2), pl.ds(0, 2)) if dz == 1 else (pl.ds(2, 2), pl.ds(nz + 2, 2))

    def copies(t, k):
        dz, dy = DIRECTIONS[k]
        a, b = layers(dz)
        if dy == 0:
            near, far = (nz + 1, nz) if dz == 1 else (2, 3)
            to_near, to_far = (1, 0) if dz == 1 else (nz + 2, nz + 3)
            pairs = [(W.at[t, near], W.at[t, to_near]), (W.at[t, far, 1], W.at[t, to_far, 1])]
        else:
            rows, to = ((ny - 1, ny - 2), pl.ds(0, 3)) if dy == 1 else ((0, 1), pl.ds(3, 3))
            pairs = [(W.at[t, a, :, :, rows[0]], HW.at[t, b, pl.ds(0, 2), to]),
                     (W.at[t, a, 1, :, rows[1]], HW.at[t, b, 2, to])]
        return [remote(src, dst, send_sem.at[t // 2, 2 * k + i], recv_sem.at[t // 2, 2 * k + i], dz, dy)
                for i, (src, dst) in enumerate(pairs)]

    def q_copies(k):
        dz, dy = DIRECTIONS[k]
        a, b = layers(dz)
        if dy == 0:
            pairs = [(Q.at[a], Q.at[b])]
        elif dy == 1:
            pairs = [(Q.at[a, :, ny - 1], HQ.at[b, :, 0]), (Q.at[a, :, ny - 2], HQ.at[b, :, 1])]
        else:
            pairs = [(Q.at[a, :, 0], HQ.at[b, :, 2])]
        return [remote(src, dst, qsend_sem.at[2 * k + i], qrecv_sem.at[2 * k + i], dz, dy)
                for i, (src, dst) in enumerate(pairs)]

    def b_copy(dy):
        row, to, i = (ny - 1, pl.ds(0, 3), 0) if dy == 1 else (0, pl.ds(3, 3), 1)
        return remote(BI.at[:, 0, :, row], HB.at[:, to], bsend_sem.at[i], brecv_sem.at[i], 0, dy)

    def for_all(make, backward, act):
        for k, (dz, dy) in enumerate(DIRECTIONS):
            sign = -1 if backward else 1

            @pl.when(exists(sign * dz, sign * dy))
            def _():
                for copy in make(k):
                    act(copy)

    def for_bottom(backward, act):
        for dy in (1, -1):
            @pl.when((d == nd - 1) & exists(0, -dy if backward else dy))
            def _():
                act(b_copy(dy))

    start = lambda copy: copy.start()
    for_all(lambda k: copies(0, k) + q_copies(k), False, start)

    for load in loads[first:]:
        load.wait()
    for r in range(rounds):
        for i in range(2):
            for c in range(3):
                BI[r, i, c] = 2.0 * MV[...].astype(f32) * IV[2 * r + i, c]
    for_bottom(False, start)

    def clear(n):
        for t in range(0, steps, 2):
            W[t, n] = jnp.zeros_like(W[t, n])
            HW[t, n] = jnp.zeros_like(HW[t, n])
        Q[n, 0] = jnp.zeros_like(Q[n, 0])
        Q[n, 1] = jnp.full_like(Q[n, 1], -1.0)
        HQ[n, 0] = jnp.zeros_like(HQ[n, 0])
        HQ[n, 1] = jnp.full_like(HQ[n, 1], -1.0)

    @pl.when(d == 0)
    def _():
        clear(0)
        clear(1)

    @pl.when(d == nd - 1)
    def _():
        clear(nz + 2)
        clear(nz + 3)

    def clear_side(rows, q_rows):
        for n in range(nz + 4):
            for t in range(0, steps, 2):
                for i in range(3):
                    HW[t, n, i, rows[0]:rows[1]] = jnp.zeros((3, nx), f32)
            HQ[n, 0, q_rows[0]:q_rows[1]] = jnp.zeros((q_rows[1] - q_rows[0], nx), f32)
            HQ[n, 1, q_rows[0]:q_rows[1]] = jnp.full((q_rows[1] - q_rows[0], nx), -1.0, f32)
        for r in range(rounds):
            HB[r, rows[0]:rows[1]] = jnp.zeros((3, nx), f32)

    @pl.when(l == 0)
    def _():
        clear_side((0, 3), (0, 2))

    @pl.when(l == nl - 1)
    def _():
        clear_side((3, 6), (2, 3))

    row = lax.broadcasted_iota(i32, (ny, nx), 0)
    lane = lax.broadcasted_iota(i32, (ny, nx), 1)

    def column_dofs(shape):
        j = lax.broadcasted_iota(i32, shape, 1)
        block = (j >= KB).astype(i32) + (j >= 2 * KB).astype(i32) + (j >= 3 * KB).astype(i32)
        j = j - KB * block
        bz = (j >= KL).astype(i32)
        j = j - KL * bz
        inner = j < 48
        bx_i = (j >= 24).astype(i32)
        c_i = (j - 24 * bx_i) >> 3
        y_i = j & 7
        h = j - 48
        far = (h >= 16).astype(i32)
        bx_h = (h >> 3) & 1
        r = h & 7
        s = (r >= 3).astype(i32)
        c_h = r - 3 * s
        y_h = jnp.where(r >= 6, 99, jnp.where(s == 0, -1 - far, 8 + far))
        y = jnp.where(inner, y_i, y_h)
        bx = jnp.where(inner, bx_i, bx_h)
        c = jnp.where(inner, c_i, c_h)
        return block, jnp.where(block < 3, y, 99), 12 * bz + 3 * bx + c

    block, _, dof = column_dofs((24, KP))
    i24 = lax.broadcasted_iota(i32, (24, KP), 0)
    stiff = jnp.concatenate([KV[0], KV[1]], 0)
    block48, _, _ = column_dofs((48, KP))
    for by in (0, 1):
        one_hot = (i24 == dof + 6 * by).astype(f32)
        e = jnp.dot(stiff, one_hot, precision=lax.Precision.HIGHEST, preferred_element_type=f32)
        e_hi = e.astype(bf16).astype(f32)
        E[by] = jnp.where(block48 == 2, e - e_hi, e_hi)
    _, y_col, _ = column_dofs((8, KP))
    r8 = lax.broadcasted_iota(i32, (8, KP), 0)
    y_halo = jnp.where(r8 < 3, -1, jnp.where(r8 < 6, 8, 199))

    def band(y_row, ay, picks):
        e0, e1 = picks
        delta = y_col - y_row + ay
        return jnp.where(delta == 0, e0, jnp.where(delta == 1, e1, 0.0))

    def wide(by, q):
        return jnp.broadcast_to(E[by, q:q + 1], (8, KP))

    for q in range(0, 48, 2):
        tiles = [band(r8, (p // 6) % 2, (wide(0, p), wide(1, p))) for p in (q, q + 1)]
        WM[8 * q:8 * q + 16] = jnp.concatenate(tiles, 0).astype(bf16)
    for g in range(0, 16, 2):
        tiles = []
        for p in (g, g + 1):
            picks = []
            for by in (0, 1):
                a, b, c = (wide(by, 3 * p + i) for i in range(3))
                picks.append(jnp.where((r8 == 0) | (r8 == 3), a, jnp.where((r8 == 1) | (r8 == 4), b, c)))
            tiles.append(band(y_halo, (p // 2) % 2, picks))
        WM[MO + 8 * g:MO + 8 * g + 16] = jnp.concatenate(tiles, 0).astype(bf16)

    def fields(n):
        def full(x):
            return jnp.broadcast_to(x, (ny, nx))
        mat = Q[n, 1]
        m1, m2, m8 = full(HQ[n, 1, 0:1]), full(HQ[n, 1, 1:2]), full(HQ[n, 1, 2:3])
        m7 = full(Q[n, 1, ny - 1:ny])
        before = jnp.where(row == 0, m1, pltpu.roll(mat, 1, 0))
        for ref, ay, m in ((FD, 0, mat), (FD, 1, before), (FH, 0, jnp.where(row < 3, m1, m8)),
                           (FH, 1, jnp.where(row < 3, m2, m7))):
            for f, table in ((0, dil), (1, she)):
                value = jnp.zeros((ny, nx), f32)
                for level in range(table.shape[0]):
                    value = jnp.where(m == float(level), table[level], value)
                ref[n, f, ay] = value

    def masses(n):
        low, high = HQ[n, 0, 0:1], HQ[n, 0, 2:3]
        HIM[n] = DT * jnp.where(row < 3, jnp.broadcast_to(low, (ny, nx)), jnp.broadcast_to(high, (ny, nx)))

    for_all(q_copies, True, lambda copy: copy.wait_recv())
    for_bottom(True, lambda copy: copy.wait_recv())

    @pl.loop(0, nz + 3)
    def _(n):
        fields(n)
        masses(n)

    at_bottom = (d == nd - 1).astype(f32)
    imp_rows = jnp.where((row == 0) | (row == 3), imp[0], jnp.where((row == 1) | (row == 4), imp[1], imp[2]))

    def ahead(x):
        return jnp.where(lane == nx - 1, 0.0, pltpu.roll(x, nx - 1, 1))

    def behind(x):
        return jnp.where(lane == 0, 0.0, pltpu.roll(x, 1, 1))

    def operand(t, n, extended):
        tiles = [W[t, n, 1, c] for c in range(3)]
        halo = [jnp.where(row < 6, HW[t, n, 1], 0.0)]
        if extended:
            halo.append(jnp.where(row < 6, HW[t, n, 2], 0.0))
        parts = tiles + [ahead(x) for x in tiles]
        for x in halo:
            parts += [x, ahead(x)]
        if not extended:
            parts += [jnp.zeros((ny, nx), f32)] * 2
        x = jnp.concatenate(parts, 0)
        hi = x.astype(bf16)
        XH[n] = hi
        XL[n] = (x - hi.astype(f32)).astype(bf16)

    def step(t, r, extended):
        first_e, last_e = (0, nz + 3) if extended else (1, nz + 2)
        m = MH if extended else MO
        for n in range(first_e, last_e + 1):
            operand(t, n, extended)
        carry = None
        for e in range(first_e, last_e):
            x = jnp.concatenate([XH[e], XH[e + 1], XL[e], XL[e + 1], XH[e], XH[e + 1],
                                 jnp.zeros((KP - 3 * KB, nx), bf16)], 0)
            slot = e % 2
            PR[slot, 0:m] = jnp.dot(WM[0:m], x, preferred_element_type=f32)

            def gather(az):
                sums = {}
                for ax in (0, 1):
                    for c in range(4 if extended else 3):
                        total = None
                        for f in (0, 1):
                            for ay in (0, 1):
                                g = 8 * f + 4 * az + 2 * ay + ax
                                if c < 3:
                                    at = 8 * (3 * g + c)
                                    term = FD[e, f, ay] * PR[slot, at:at + 8]
                                else:
                                    at = MO + 8 * g
                                    term = FH[e, f, ay] * PR[slot, at:at + 8]
                                total = term if total is None else total + term
                        sums[ax, c] = total
                return sums

            if carry is not None:
                sums = gather(0)
                force = [sums[0, c] + carry[0, c] + behind(sums[1, c] + carry[1, c])
                         for c in range(4 if extended else 3)]
                scale = DT * Q[e, 0]
                for c in range(3):
                    net = -force[c]
                    v = W[t, e, 0, c]
                    if e == nz + 1:
                        net = net + at_bottom * imp[c] * (BI[t // 2, r, c] - v)
                    v = v + scale * net
                    W[t + 1, e, 0, c] = v
                    W[t + 1, e, 1, c] = W[t, e, 1, c] + DT * v
                if extended:
                    net = -force[3]
                    v = HW[t, e, 0]
                    if e == nz + 1:
                        net = net + at_bottom * imp_rows * (HB[t // 2] - v)
                    v = v + HIM[e] * net
                    HW[t + 1, e, 1] = HW[t, e, 1] + DT * v
            carry = gather(1)

    @pl.loop(0, rounds)
    def _(i):
        t = 2 * i

        @pl.when(i > 0)
        def _():
            for_all(lambda k: copies(t, k), False, start)

        for_all(lambda k: copies(t, k), True, lambda copy: copy.wait_recv())
        step(t, 0, True)
        step(t + 1, 1, False)

    for z in range(nz):
        for c in range(3):
            u_out[c, z] = W[steps, z + 2, 1, c]
            v_out[c, z] = W[steps, z + 2, 0, c]

    done = lambda copy: copy.wait_send()
    for_all(q_copies, False, done)
    for_bottom(False, done)

    @pl.loop(0, rounds)
    def _(i):
        for_all(lambda k: copies(2 * i, k), False, done)


def per_device(nd, nl, displacement, velocity, inverse_mass, material, dilation_table, shear_table,
               stiffness_pair, impedance, bedrock_mask, incident):
    _, nz, ny, nx = displacement.shape
    steps = incident.shape[0]
    rounds = steps // 2
    nmat = dilation_table.shape[0]
    vmem = pl.BlockSpec(memory_space=pltpu.VMEM)
    hbm = pl.BlockSpec(memory_space=pltpu.MemorySpace.HBM)
    ext = nz + 4
    dma = pltpu.SemaphoreType.DMA
    return pl.pallas_call(
        functools.partial(kernel, nd, nl),
        out_shape=[jax.ShapeDtypeStruct(displacement.shape, f32)] * 2,
        in_specs=[hbm] * 10,
        out_specs=[vmem, vmem],
        scratch_shapes=[
            pltpu.VMEM((steps + 1, ext, 2, 3, ny, nx), f32),
            pltpu.VMEM((steps, ext, 3, ny, nx), f32),
            pltpu.VMEM((ext, 2, ny, nx), f32),
            pltpu.VMEM((ext, 2, ny, nx), f32),
            pltpu.VMEM((rounds, 2, 3, ny, nx), f32),
            pltpu.VMEM((rounds, ny, nx), f32),
            pltpu.VMEM((nz, ny, nx), i32),
            pltpu.VMEM(stiffness_pair.shape, f32),
            pltpu.VMEM((ny, nx), i32),
            pltpu.VMEM((steps, 3, ny, nx), f32),
            pltpu.VMEM((2, 48, KP), f32),
            pltpu.VMEM((MH, KP), bf16),
            pltpu.VMEM((ext, KL, nx), bf16),
            pltpu.VMEM((ext, KL, nx), bf16),
            pltpu.VMEM((2, MH, nx), f32),
            pltpu.VMEM((ext, 2, 2, ny, nx), f32),
            pltpu.VMEM((ext, 2, 2, ny, nx), f32),
            pltpu.VMEM((ext, ny, nx), f32),
            pltpu.SMEM((nmat,), f32),
            pltpu.SMEM((nmat,), f32),
            pltpu.SMEM((3,), f32),
            dma((14,)),
            dma((rounds, 16)),
            dma((rounds, 16)),
            dma((16,)),
            dma((16,)),
            dma((2,)),
            dma((2,)),
        ],
        compiler_params=pltpu.CompilerParams(
            collective_id=0, has_side_effects=True, vmem_limit_bytes=67043328),
    )(displacement, velocity, inverse_mass, material, dilation_table, shear_table,
      stiffness_pair, impedance, bedrock_mask, incident)


def solution(mesh):
    in_specs = (
        P(None, "depth", "lat", None),
        P(None, "depth", "lat", None),
        P("depth", "lat", None),
        P("depth", "lat", None),
        P(),
        P(),
        P(),
        P(),
        P("lat", None),
        P(None, None, "lat", None),
    )
    out_specs = (P(None, "depth", "lat", None), P(None, "depth", "lat", None))
    return jax.shard_map(
        functools.partial(per_device, mesh.shape["depth"], mesh.shape["lat"]),
        mesh=mesh, in_specs=in_specs, out_specs=out_specs, check_vma=False)
```

```python
import functools

import jax
import jax.numpy as jnp
from jax import lax
from jax.experimental import pallas as pl
from jax.experimental.pallas import tpu as pltpu
from jax.sharding import PartitionSpec as P

MESH = pl.DeviceIdType.MESH
DT = 0.1
f32, bf16, i32 = jnp.float32, jnp.bfloat16, jnp.int32
DIRECTIONS = ((1, 0), (-1, 0), (1, 1), (1, -1), (-1, 1), (-1, -1), (0, 1), (0, -1))

KL = 80
KB = 2 * KL
KP = 512
MO = 384
MH = 512


def kernel(
    nd, nl,
    u_in, v_in, im_in, mat_in, dil_in, she_in, k_in, imp_in, mask_in, inc_in,
    u_out, v_out,
    W, HW, Q, HQ, BI, HB, MI, KV, MV, IV, E, WM, XH, XL, PR, FD, FH, HIM,
    dil, she, imp,
    in_sem, send_sem, recv_sem, qsend_sem, qrecv_sem, bsend_sem, brecv_sem,
):
    steps = inc_in.shape[0]
    rounds = steps // 2
    nz, ny, nx = im_in.shape
    d = lax.axis_index("depth")
    l = lax.axis_index("lat")

    def exists(dz, dy):
        return ((d + dz >= 0) & (d + dz < nd)) & ((l + dy >= 0) & (l + dy < nl))

    barrier = pltpu.get_barrier_semaphore()
    partners = 0
    for dz, dy in DIRECTIONS:
        @pl.when(exists(dz, dy))
        def _():
            pl.semaphore_signal(barrier, inc=1, device_id=(d + dz, l + dy), device_id_type=MESH)
        partners = partners + exists(dz, dy).astype(i32)
    own = pl.ds(2, nz)
    loads = [(im_in, Q.at[own, 0]), (mat_in, MI)]
    for c in range(3):
        loads.append((u_in.at[c], W.at[0, own, 1, c]))
        loads.append((v_in.at[c], W.at[0, own, 0, c]))
    first = len(loads)
    loads += [(k_in, KV), (mask_in, MV), (inc_in, IV), (dil_in, dil), (she_in, she), (imp_in, imp)]
    loads = [pltpu.make_async_copy(a, b, in_sem.at[i]) for i, (a, b) in enumerate(loads)]
    for load in loads:
        load.start()

    for load in loads[:first]:
        load.wait()
    for z in range(nz):
        Q[z + 2, 1] = MI[z].astype(f32)
    pl.semaphore_wait(barrier, partners)

    def remote(src, dst, ss, rs, dz, dy):
        return pltpu.make_async_remote_copy(
            src_ref=src, dst_ref=dst, send_sem=ss, recv_sem=rs,
            device_id=(d + dz, l + dy), device_id_type=MESH)

    def layers(dz):
        if dz == 0:
            return own, own
        return (pl.ds(nz, 2), pl.ds(0, 2)) if dz == 1 else (pl.ds(2, 2), pl.ds(nz + 2, 2))

    def rows_of(dy):
        return (ny - 1, ny - 2, pl.ds(0, 3)) if dy == 1 else (0, 1, pl.ds(3, 3))

    def copies(t, k):
        dz, dy = DIRECTIONS[k]
        a, b = layers(dz)
        if dy == 0:
            pairs = [(W.at[t, a, 1], W.at[t, b, 1])]
        else:
            near_row, far_row, to = rows_of(dy)
            pairs = [(W.at[t, a, 1, :, near_row], HW.at[t, b, 1, to]),
                     (W.at[t, a, 1, :, far_row], HW.at[t, b, 2, to])]
        return [remote(src, dst, send_sem.at[t // 2, 2 * k + i], recv_sem.at[t // 2, 2 * k + i], dz, dy)
                for i, (src, dst) in enumerate(pairs)]

    def first_copies(k):
        dz, dy = DIRECTIONS[k]
        a, b = layers(dz)
        near, far = (nz + 1, nz) if dz == 1 else (2, 3)
        to_near, to_far = (1, 0) if dz == 1 else (nz + 2, nz + 3)
        if dy == 0:
            pairs = [(W.at[0, near], W.at[0, to_near]), (W.at[0, far, 1], W.at[0, to_far, 1]),
                     (Q.at[near], Q.at[to_near])]
            if dz == 1:
                pairs.append((Q.at[far, 1], Q.at[to_far, 1]))
        else:
            near_row, far_row, to = rows_of(dy)
            slot = 0 if dy == 1 else 2
            pairs = [(W.at[0, a, 1, :, far_row], HW.at[0, b, 2, to])]
            if dz == 0:
                pairs += [(W.at[0, a, :, :, near_row], HW.at[0, b, pl.ds(0, 2), to]),
                          (Q.at[a, :, near_row], HQ.at[b, :, slot])]
                if dy == 1:
                    pairs.append((Q.at[a, 1, far_row], HQ.at[b, 1, 1]))
            else:
                pairs += [(W.at[0, near, :, :, near_row], HW.at[0, to_near, pl.ds(0, 2), to]),
                          (W.at[0, far, 1, :, near_row], HW.at[0, to_far, 1, to]),
                          (Q.at[near, :, near_row], HQ.at[to_near, :, slot])]
                if dz == 1:
                    pairs.append((Q.at[far, 1, near_row], HQ.at[to_far, 1, slot]))
                if dy == 1:
                    if dz == 1:
                        pairs.append((Q.at[a, 1, far_row], HQ.at[b, 1, 1]))
                    else:
                        pairs.append((Q.at[near, 1, far_row], HQ.at[to_near, 1, 1]))
        return [remote(src, dst, qsend_sem.at[6 * k + i], qrecv_sem.at[6 * k + i], dz, dy)
                for i, (src, dst) in enumerate(pairs)]

    def b_copy(dy):
        row, to, i = (ny - 1, pl.ds(0, 3), 0) if dy == 1 else (0, pl.ds(3, 3), 1)
        return remote(BI.at[:, 0, :, row], HB.at[:, to], bsend_sem.at[i], brecv_sem.at[i], 0, dy)

    def for_all(make, backward, act, which=tuple(range(len(DIRECTIONS)))):
        for k in which:
            dz, dy = DIRECTIONS[k]
            sign = -1 if backward else 1

            @pl.when(exists(sign * dz, sign * dy))
            def _():
                for copy in make(k):
                    act(copy)

    def for_bottom(backward, act):
        for dy in (1, -1):
            @pl.when((d == nd - 1) & exists(0, -dy if backward else dy))
            def _():
                act(b_copy(dy))

    start = lambda copy: copy.start()
    for_all(first_copies, False, start)

    for load in loads[first:]:
        load.wait()
    for r in range(rounds):
        for i in range(2):
            for c in range(3):
                BI[r, i, c] = 2.0 * MV[...].astype(f32) * IV[2 * r + i, c]
    for_bottom(False, start)

    def clear(n):
        for t in range(0, steps, 2):
            W[t, n] = jnp.zeros_like(W[t, n])
            HW[t, n] = jnp.zeros_like(HW[t, n])
        Q[n, 0] = jnp.zeros_like(Q[n, 0])
        Q[n, 1] = jnp.full_like(Q[n, 1], -1.0)
        HQ[n, 0] = jnp.zeros_like(HQ[n, 0])
        HQ[n, 1] = jnp.full_like(HQ[n, 1], -1.0)

    @pl.when(d == 0)
    def _():
        clear(0)
        clear(1)

    @pl.when(d == nd - 1)
    def _():
        clear(nz + 2)
        clear(nz + 3)

    def clear_side(rows, q_rows):
        for n in range(nz + 4):
            for t in range(0, steps, 2):
                for i in range(3):
                    HW[t, n, i, rows[0]:rows[1]] = jnp.zeros((3, nx), f32)
            HQ[n, 0, q_rows[0]:q_rows[1]] = jnp.zeros((q_rows[1] - q_rows[0], nx), f32)
            HQ[n, 1, q_rows[0]:q_rows[1]] = jnp.full((q_rows[1] - q_rows[0], nx), -1.0, f32)
        for r in range(rounds):
            HB[r, rows[0]:rows[1]] = jnp.zeros((3, nx), f32)

    @pl.when(d < nd - 1)
    def _():
        HB[...] = jnp.zeros_like(HB)

    @pl.when(l == 0)
    def _():
        clear_side((0, 3), (0, 2))

    @pl.when(l == nl - 1)
    def _():
        clear_side((3, 6), (2, 3))

    row = lax.broadcasted_iota(i32, (ny, nx), 0)
    lane = lax.broadcasted_iota(i32, (ny, nx), 1)

    def column_dofs(shape):
        j = lax.broadcasted_iota(i32, shape, 1)
        block = (j >= KB).astype(i32) + (j >= 2 * KB).astype(i32) + (j >= 3 * KB).astype(i32)
        j = j - KB * block
        bz = (j >= KL).astype(i32)
        j = j - KL * bz
        inner = j < 48
        bx_i = (j >= 24).astype(i32)
        c_i = (j - 24 * bx_i) >> 3
        y_i = j & 7
        h = j - 48
        far = (h >= 16).astype(i32)
        bx_h = (h >> 3) & 1
        r = h & 7
        s = (r >= 3).astype(i32)
        c_h = r - 3 * s
        y_h = jnp.where(r >= 6, 99, jnp.where(s == 0, -1 - far, 8 + far))
        y = jnp.where(inner, y_i, y_h)
        bx = jnp.where(inner, bx_i, bx_h)
        c = jnp.where(inner, c_i, c_h)
        return block, jnp.where(block < 3, y, 99), 12 * bz + 3 * bx + c

    block, _, dof = column_dofs((24, KP))
    i24 = lax.broadcasted_iota(i32, (24, KP), 0)
    stiff = jnp.concatenate([KV[0], KV[1]], 0)
    block48, _, _ = column_dofs((48, KP))
    for by in (0, 1):
        one_hot = (i24 == dof + 6 * by).astype(f32)
        e = jnp.dot(stiff, one_hot, precision=lax.Precision.HIGHEST, preferred_element_type=f32)
        e_hi = e.astype(bf16).astype(f32)
        E[by] = jnp.where(block48 == 2, e - e_hi, e_hi)
    _, y_col, _ = column_dofs((8, KP))
    r8 = lax.broadcasted_iota(i32, (8, KP), 0)
    y_halo = jnp.where(r8 < 3, -1, jnp.where(r8 < 6, 8, 199))

    def band(y_row, ay, picks):
        e0, e1 = picks
        delta = y_col - y_row + ay
        return jnp.where(delta == 0, e0, jnp.where(delta == 1, e1, 0.0))

    def wide(by, q):
        return jnp.broadcast_to(E[by, q:q + 1], (8, KP))

    for q in range(0, 48, 2):
        tiles = [band(r8, (p // 6) % 2, (wide(0, p), wide(1, p))) for p in (q, q + 1)]
        WM[8 * q:8 * q + 16] = jnp.concatenate(tiles, 0).astype(bf16)
    for g in range(0, 16, 2):
        tiles = []
        for p in (g, g + 1):
            picks = []
            for by in (0, 1):
                a, b, c = (wide(by, 3 * p + i) for i in range(3))
                picks.append(jnp.where((r8 == 0) | (r8 == 3), a, jnp.where((r8 == 1) | (r8 == 4), b, c)))
            tiles.append(band(y_halo, (p // 2) % 2, picks))
        WM[MO + 8 * g:MO + 8 * g + 16] = jnp.concatenate(tiles, 0).astype(bf16)

    def fields(n):
        def full(x):
            return jnp.broadcast_to(x, (ny, nx))
        mat = Q[n, 1]
        m1, m2, m8 = full(HQ[n, 1, 0:1]), full(HQ[n, 1, 1:2]), full(HQ[n, 1, 2:3])
        m7 = full(Q[n, 1, ny - 1:ny])
        before = jnp.where(row == 0, m1, pltpu.roll(mat, 1, 0))
        for ref, ay, m in ((FD, 0, mat), (FD, 1, before), (FH, 0, jnp.where(row < 3, m1, m8)),
                           (FH, 1, jnp.where(row < 3, m2, m7))):
            for f, table in ((0, dil), (1, she)):
                value = jnp.zeros((ny, nx), f32)
                for level in range(table.shape[0]):
                    value = jnp.where(m == float(level), table[level], value)
                ref[n, f, ay] = value

    def masses(n):
        low, high = HQ[n, 0, 0:1], HQ[n, 0, 2:3]
        HIM[n] = DT * jnp.where(row < 3, jnp.broadcast_to(low, (ny, nx)), jnp.broadcast_to(high, (ny, nx)))

    here = lambda copy: copy.wait_recv()
    lat_k, depth_k = (6, 7), (0, 1, 2, 3, 4, 5)
    for_all(first_copies, True, here, lat_k)
    for_bottom(True, here)

    @pl.loop(2, nz + 2)
    def _(n):
        fields(n)
        masses(n)

    at_bottom = (d == nd - 1).astype(f32)
    imp_rows = jnp.where((row == 0) | (row == 3), imp[0], jnp.where((row == 1) | (row == 4), imp[1], imp[2]))

    def ahead(x):
        return jnp.where(lane == nx - 1, 0.0, pltpu.roll(x, nx - 1, 1))

    def behind(x):
        return jnp.where(lane == 0, 0.0, pltpu.roll(x, 1, 1))

    def operand(t, n, extended):
        tiles = [W[t, n, 1, c] for c in range(3)]
        halo = [jnp.where(row < 6, HW[t, n, 1], 0.0)]
        if extended:
            halo.append(jnp.where(row < 6, HW[t, n, 2], 0.0))
        parts = tiles + [ahead(x) for x in tiles]
        for x in halo:
            parts += [x, ahead(x)]
        if not extended:
            parts += [jnp.zeros((ny, nx), f32)] * 2
        x = jnp.concatenate(parts, 0)
        hi = x.astype(bf16)
        XH[n] = hi
        XL[n] = (x - hi.astype(f32)).astype(bf16)

    def element(e, extended):
        m = MH if extended else MO
        x = jnp.concatenate([XH[e], XH[e + 1], XL[e], XL[e + 1], XH[e], XH[e + 1],
                             jnp.zeros((KP - 3 * KB, nx), bf16)], 0)
        slot = e % 2
        PR[slot, 0:m] = jnp.dot(WM[0:m], x, preferred_element_type=f32)
        sides = []
        for az in (0, 1):
            sums = {}
            for ax in (0, 1):
                for c in range(4 if extended else 3):
                    total = None
                    for f in (0, 1):
                        for ay in (0, 1):
                            g = 8 * f + 4 * az + 2 * ay + ax
                            if c < 3:
                                at = 8 * (3 * g + c)
                                term = FD[e, f, ay] * PR[slot, at:at + 8]
                            else:
                                at = MO + 8 * g
                                term = FH[e, f, ay] * PR[slot, at:at + 8]
                            total = term if total is None else total + term
                    sums[ax, c] = total
            sides.append(sums)
        return sides

    def advance(t, r, n, before, after, extended):
        force = [after[0, c] + before[0, c] + behind(after[1, c] + before[1, c])
                 for c in range(4 if extended else 3)]
        scale = DT * Q[n, 0]
        for c in range(3):
            net = -force[c]
            v = W[t, n, 0, c]
            if n == nz + 1:
                net = net + at_bottom * imp[c] * (BI[t // 2, r, c] - v)
            v = v + scale * net
            W[t + 1, n, 0, c] = v
            W[t + 1, n, 1, c] = W[t, n, 1, c] + DT * v
        if extended:
            net = -force[3]
            v = HW[t, n, 0]
            if n == nz + 1:
                net = net + at_bottom * imp_rows * (HB[t // 2] - v)
            v = v + HIM[n] * net
            HW[t + 1, n, 1] = HW[t, n, 1] + DT * v

    def run(t, r, extended, order, nodes, low, high):
        for e in order:
            low[e], high[e] = element(e, extended)
            for n in (e, e + 1):
                if n in nodes and n in low and n - 1 in high:
                    advance(t, r, n, high[n - 1], low[n], extended)
                    nodes.remove(n)

    def follow_tile(t, n):
        HW[t, n, 0] = (HW[t, n, 1] - HW[t - 1, n, 1]) * (1.0 / DT)

    def follow_layer(t, n):
        for c in range(3):
            W[t, n, 0, c] = (W[t, n, 1, c] - W[t - 1, n, 1, c]) * (1.0 / DT)

    top = nz + 2

    @pl.loop(0, rounds)
    def _(i):
        t = 2 * i

        @pl.when(i > 0)
        def _():
            for_all(lambda k: copies(t, k), True, here, lat_k)
            for n in range(2, top):
                follow_tile(t, n)

        low, high, nodes = {}, {}, set(range(1, top + 1))
        for n in range(2, top):
            operand(t, n, True)
        run(t, 0, True, range(2, top - 1), nodes, low, high)

        @pl.when(i == 0)
        def _():
            for_all(first_copies, True, here, depth_k)
            for n in (0, 1, top):
                fields(n)
            for n in (1, top):
                masses(n)

        @pl.when(i > 0)
        def _():
            for_all(lambda k: copies(t, k), True, here, depth_k)
            for n in (1, top):
                follow_tile(t, n)
                follow_layer(t, n)

        for n in (1, 0, top, top + 1):
            operand(t, n, True)
        run(t, 0, True, (1, 0, top - 1, top), nodes, low, high)

        def send(which):
            @pl.when(i < rounds - 1)
            def _():
                for_all(lambda k: copies(t + 2, k), False, start, which)

        low, high, nodes = {}, {}, set(range(2, top))
        for n in range(1, 5):
            operand(t + 1, n, False)
        run(t + 1, 1, False, (1, 2, 3), nodes, low, high)
        send((1, 4, 5))
        for n in range(top - 3, top + 1):
            operand(t + 1, n, False)
        run(t + 1, 1, False, (top - 3, top - 2, top - 1), nodes, low, high)
        send((0, 2, 3))
        for n in range(5, top - 3):
            operand(t + 1, n, False)
        run(t + 1, 1, False, range(4, top - 3), nodes, low, high)
        send(lat_k)

    for z in range(nz):
        for c in range(3):
            u_out[c, z] = W[steps, z + 2, 1, c]
            v_out[c, z] = W[steps, z + 2, 0, c]

    done = lambda copy: copy.wait_send()
    for_all(first_copies, False, done)
    for_bottom(False, done)

    @pl.loop(1, rounds)
    def _(i):
        for_all(lambda k: copies(2 * i, k), False, done)


def per_device(nd, nl, displacement, velocity, inverse_mass, material, dilation_table, shear_table,
               stiffness_pair, impedance, bedrock_mask, incident):
    _, nz, ny, nx = displacement.shape
    steps = incident.shape[0]
    rounds = steps // 2
    nmat = dilation_table.shape[0]
    vmem = pl.BlockSpec(memory_space=pltpu.VMEM)
    hbm = pl.BlockSpec(memory_space=pltpu.MemorySpace.HBM)
    ext = nz + 4
    dma = pltpu.SemaphoreType.DMA
    return pl.pallas_call(
        functools.partial(kernel, nd, nl),
        out_shape=[jax.ShapeDtypeStruct(displacement.shape, f32)] * 2,
        in_specs=[hbm] * 10,
        out_specs=[vmem, vmem],
        scratch_shapes=[
            pltpu.VMEM((steps + 1, ext, 2, 3, ny, nx), f32),
            pltpu.VMEM((steps, ext, 3, ny, nx), f32),
            pltpu.VMEM((ext, 2, ny, nx), f32),
            pltpu.VMEM((ext, 2, ny, nx), f32),
            pltpu.VMEM((rounds, 2, 3, ny, nx), f32),
            pltpu.VMEM((rounds, ny, nx), f32),
            pltpu.VMEM((nz, ny, nx), i32),
            pltpu.VMEM(stiffness_pair.shape, f32),
            pltpu.VMEM((ny, nx), i32),
            pltpu.VMEM((steps, 3, ny, nx), f32),
            pltpu.VMEM((2, 48, KP), f32),
            pltpu.VMEM((MH, KP), bf16),
            pltpu.VMEM((ext, KL, nx), bf16),
            pltpu.VMEM((ext, KL, nx), bf16),
            pltpu.VMEM((2, MH, nx), f32),
            pltpu.VMEM((ext, 2, 2, ny, nx), f32),
            pltpu.VMEM((ext, 2, 2, ny, nx), f32),
            pltpu.VMEM((ext, ny, nx), f32),
            pltpu.SMEM((nmat,), f32),
            pltpu.SMEM((nmat,), f32),
            pltpu.SMEM((3,), f32),
            dma((14,)),
            dma((rounds, 16)),
            dma((rounds, 16)),
            dma((48,)),
            dma((48,)),
            dma((2,)),
            dma((2,)),
        ],
        compiler_params=pltpu.CompilerParams(
            collective_id=0, has_side_effects=True, vmem_limit_bytes=48 * 1024 * 1024),
    )(*(pltpu.with_memory_space_constraint(x, pltpu.MemorySpace.HBM) for x in (
        displacement, velocity, inverse_mass, material, dilation_table, shear_table,
        stiffness_pair, impedance, bedrock_mask, incident)))


def solution(mesh):
    in_specs = (
        P(None, "depth", "lat", None),
        P(None, "depth", "lat", None),
        P("depth", "lat", None),
        P("depth", "lat", None),
        P(),
        P(),
        P(),
        P(),
        P("lat", None),
        P(None, None, "lat", None),
    )
    out_specs = (P(None, "depth", "lat", None), P(None, "depth", "lat", None))
    return jax.shard_map(
        functools.partial(per_device, mesh.shape["depth"], mesh.shape["lat"]),
        mesh=mesh, in_specs=in_specs, out_specs=out_specs, check_vma=False)
```

```python
import functools

import jax
import jax.numpy as jnp
from jax import lax
from jax.experimental import pallas as pl
from jax.experimental.pallas import tpu as pltpu
from jax.sharding import PartitionSpec as P

MESH = pl.DeviceIdType.MESH
DT = 0.1
f32, bf16, i32 = jnp.float32, jnp.bfloat16, jnp.int32
DIRECTIONS = ((1, 0), (-1, 0), (1, 1), (1, -1), (-1, 1), (-1, -1), (0, 1), (0, -1))

KL = 80
KB = 2 * KL
KP = 512
MO = 384
MH = 512


def kernel(
    nd, nl,
    u_in, v_in, im_in, mat_in, dil_in, she_in, k_in, imp_in, mask_in, inc_in,
    u_out, v_out,
    W, HW, Q, HQ, BI, HB, MI, KV, MV, IV, E, WM, XH, XL, PR, FD, FH, HIM,
    dil, she, imp,
    in_sem, send_sem, recv_sem, qsend_sem, qrecv_sem, bsend_sem, brecv_sem,
):
    steps = inc_in.shape[0]
    rounds = steps // 2
    nz, ny, nx = im_in.shape
    d = lax.axis_index("depth")
    l = lax.axis_index("lat")

    def exists(dz, dy):
        return ((d + dz >= 0) & (d + dz < nd)) & ((l + dy >= 0) & (l + dy < nl))

    barrier = pltpu.get_barrier_semaphore()
    partners = 0
    for dz, dy in DIRECTIONS:
        @pl.when(exists(dz, dy))
        def _():
            pl.semaphore_signal(barrier, inc=1, device_id=(d + dz, l + dy), device_id_type=MESH)
        partners = partners + exists(dz, dy).astype(i32)
    own = pl.ds(2, nz)
    loads = [(im_in, Q.at[own, 0]), (mat_in, MI)]
    for c in range(3):
        loads.append((u_in.at[c], W.at[0, own, 1, c]))
        loads.append((v_in.at[c], W.at[0, own, 0, c]))
    first = len(loads)
    loads += [(k_in, KV), (mask_in, MV), (inc_in, IV), (dil_in, dil), (she_in, she), (imp_in, imp)]
    loads = [pltpu.make_async_copy(a, b, in_sem.at[i]) for i, (a, b) in enumerate(loads)]
    for load in loads:
        load.start()

    for load in loads[:first]:
        load.wait()
    for z in range(nz):
        Q[z + 2, 1] = MI[z].astype(f32)
    pl.semaphore_wait(barrier, partners)

    def remote(src, dst, ss, rs, dz, dy):
        return pltpu.make_async_remote_copy(
            src_ref=src, dst_ref=dst, send_sem=ss, recv_sem=rs,
            device_id=(d + dz, l + dy), device_id_type=MESH)

    def layers(dz):
        if dz == 0:
            return own, own
        return (pl.ds(nz, 2), pl.ds(0, 2)) if dz == 1 else (pl.ds(2, 2), pl.ds(nz + 2, 2))

    def rows_of(dy):
        return (ny - 1, ny - 2, pl.ds(0, 3)) if dy == 1 else (0, 1, pl.ds(3, 3))

    def copies(t, k):
        dz, dy = DIRECTIONS[k]
        a, b = layers(dz)
        if dy == 0:
            pairs = [(W.at[t, a, 1], W.at[t, b, 1])]
        else:
            near_row, far_row, to = rows_of(dy)
            pairs = [(W.at[t, a, 1, :, near_row], HW.at[t, b, 1, to]),
                     (W.at[t, a, 1, :, far_row], HW.at[t, b, 2, to])]
        return [remote(src, dst, send_sem.at[t // 2, 2 * k + i], recv_sem.at[t // 2, 2 * k + i], dz, dy)
                for i, (src, dst) in enumerate(pairs)]

    def first_copies(k):
        dz, dy = DIRECTIONS[k]
        a, b = layers(dz)
        near, far = (nz + 1, nz) if dz == 1 else (2, 3)
        to_near, to_far = (1, 0) if dz == 1 else (nz + 2, nz + 3)
        if dy == 0:
            pairs = [(W.at[0, near], W.at[0, to_near]), (W.at[0, far, 1], W.at[0, to_far, 1]),
                     (Q.at[near], Q.at[to_near])]
            if dz == 1:
                pairs.append((Q.at[far, 1], Q.at[to_far, 1]))
        else:
            near_row, far_row, to = rows_of(dy)
            slot = 0 if dy == 1 else 2
            pairs = [(W.at[0, a, 1, :, far_row], HW.at[0, b, 2, to])]
            if dz == 0:
                pairs += [(W.at[0, a, :, :, near_row], HW.at[0, b, pl.ds(0, 2), to]),
                          (Q.at[a, :, near_row], HQ.at[b, :, slot])]
                if dy == 1:
                    pairs.append((Q.at[a, 1, far_row], HQ.at[b, 1, 1]))
            else:
                pairs += [(W.at[0, near, :, :, near_row], HW.at[0, to_near, pl.ds(0, 2), to]),
                          (W.at[0, far, 1, :, near_row], HW.at[0, to_far, 1, to]),
                          (Q.at[near, :, near_row], HQ.at[to_near, :, slot])]
                if dz == 1:
                    pairs.append((Q.at[far, 1, near_row], HQ.at[to_far, 1, slot]))
                if dy == 1:
                    if dz == 1:
                        pairs.append((Q.at[a, 1, far_row], HQ.at[b, 1, 1]))
                    else:
                        pairs.append((Q.at[near, 1, far_row], HQ.at[to_near, 1, 1]))
        return [remote(src, dst, qsend_sem.at[6 * k + i], qrecv_sem.at[6 * k + i], dz, dy)
                for i, (src, dst) in enumerate(pairs)]

    def b_copy(dy):
        row, to, i = (ny - 1, pl.ds(0, 3), 0) if dy == 1 else (0, pl.ds(3, 3), 1)
        return remote(BI.at[:, 0, :, row], HB.at[:, to], bsend_sem.at[i], brecv_sem.at[i], 0, dy)

    def for_all(make, backward, act, which=tuple(range(len(DIRECTIONS)))):
        for k in which:
            dz, dy = DIRECTIONS[k]
            sign = -1 if backward else 1

            @pl.when(exists(sign * dz, sign * dy))
            def _():
                for copy in make(k):
                    act(copy)

    def for_bottom(backward, act):
        for dy in (1, -1):
            @pl.when((d == nd - 1) & exists(0, -dy if backward else dy))
            def _():
                act(b_copy(dy))

    start = lambda copy: copy.start()
    for_all(first_copies, False, start)

    for load in loads[first:]:
        load.wait()
    for r in range(rounds):
        for i in range(2):
            for c in range(3):
                BI[r, i, c] = 2.0 * MV[...].astype(f32) * IV[2 * r + i, c]
    for_bottom(False, start)

    def clear(n):
        for t in range(0, steps, 2):
            W[t, n] = jnp.zeros_like(W[t, n])
            HW[t, n] = jnp.zeros_like(HW[t, n])
        Q[n, 0] = jnp.zeros_like(Q[n, 0])
        Q[n, 1] = jnp.full_like(Q[n, 1], -1.0)
        HQ[n, 0] = jnp.zeros_like(HQ[n, 0])
        HQ[n, 1] = jnp.full_like(HQ[n, 1], -1.0)

    @pl.when(d == 0)
    def _():
        clear(0)
        clear(1)

    @pl.when(d == nd - 1)
    def _():
        clear(nz + 2)
        clear(nz + 3)

    def clear_side(rows, q_rows):
        for n in range(nz + 4):
            for t in range(0, steps, 2):
                for i in range(3):
                    HW[t, n, i, rows[0]:rows[1]] = jnp.zeros((3, nx), f32)
            HQ[n, 0, q_rows[0]:q_rows[1]] = jnp.zeros((q_rows[1] - q_rows[0], nx), f32)
            HQ[n, 1, q_rows[0]:q_rows[1]] = jnp.full((q_rows[1] - q_rows[0], nx), -1.0, f32)
        for r in range(rounds):
            HB[r, rows[0]:rows[1]] = jnp.zeros((3, nx), f32)

    @pl.when(d < nd - 1)
    def _():
        HB[...] = jnp.zeros_like(HB)

    @pl.when(l == 0)
    def _():
        clear_side((0, 3), (0, 2))

    @pl.when(l == nl - 1)
    def _():
        clear_side((3, 6), (2, 3))

    row = lax.broadcasted_iota(i32, (ny, nx), 0)
    lane = lax.broadcasted_iota(i32, (ny, nx), 1)

    def column_dofs(shape):
        j = lax.broadcasted_iota(i32, shape, 1)
        block = (j >= KB).astype(i32) + (j >= 2 * KB).astype(i32) + (j >= 3 * KB).astype(i32)
        j = j - KB * block
        bz = (j >= KL).astype(i32)
        j = j - KL * bz
        inner = j < 48
        bx_i = (j >= 24).astype(i32)
        c_i = (j - 24 * bx_i) >> 3
        y_i = j & 7
        h = j - 48
        far = (h >= 16).astype(i32)
        bx_h = (h >> 3) & 1
        r = h & 7
        s = (r >= 3).astype(i32)
        c_h = r - 3 * s
        y_h = jnp.where(r >= 6, 99, jnp.where(s == 0, -1 - far, 8 + far))
        y = jnp.where(inner, y_i, y_h)
        bx = jnp.where(inner, bx_i, bx_h)
        c = jnp.where(inner, c_i, c_h)
        return block, jnp.where(block < 3, y, 99), 12 * bz + 3 * bx + c

    block, _, dof = column_dofs((24, KP))
    i24 = lax.broadcasted_iota(i32, (24, KP), 0)
    stiff = jnp.concatenate([KV[0], KV[1]], 0)
    block48, _, _ = column_dofs((48, KP))
    for by in (0, 1):
        one_hot = (i24 == dof + 6 * by).astype(f32)
        e = jnp.dot(stiff, one_hot, precision=lax.Precision.HIGHEST, preferred_element_type=f32)
        e_hi = e.astype(bf16).astype(f32)
        E[by] = jnp.where(block48 == 2, e - e_hi, e_hi)
    _, y_col, _ = column_dofs((8, KP))
    r8 = lax.broadcasted_iota(i32, (8, KP), 0)
    y_halo = jnp.where(r8 < 3, -1, jnp.where(r8 < 6, 8, 199))

    def band(y_row, ay, picks):
        e0, e1 = picks
        delta = y_col - y_row + ay
        return jnp.where(delta == 0, e0, jnp.where(delta == 1, e1, 0.0))

    def wide(by, q):
        return jnp.broadcast_to(E[by, q:q + 1], (8, KP))

    for q in range(0, 48, 2):
        tiles = [band(r8, (p // 6) % 2, (wide(0, p), wide(1, p))) for p in (q, q + 1)]
        WM[8 * q:8 * q + 16] = jnp.concatenate(tiles, 0).astype(bf16)
    for g in range(0, 16, 2):
        tiles = []
        for p in (g, g + 1):
            picks = []
            for by in (0, 1):
                a, b, c = (wide(by, 3 * p + i) for i in range(3))
                picks.append(jnp.where((r8 == 0) | (r8 == 3), a, jnp.where((r8 == 1) | (r8 == 4), b, c)))
            tiles.append(band(y_halo, (p // 2) % 2, picks))
        WM[MO + 8 * g:MO + 8 * g + 16] = jnp.concatenate(tiles, 0).astype(bf16)

    def fields(n):
        def full(x):
            return jnp.broadcast_to(x, (ny, nx))
        mat = Q[n, 1]
        m1, m2, m8 = full(HQ[n, 1, 0:1]), full(HQ[n, 1, 1:2]), full(HQ[n, 1, 2:3])
        m7 = full(Q[n, 1, ny - 1:ny])
        before = jnp.where(row == 0, m1, pltpu.roll(mat, 1, 0))
        for ref, ay, m in ((FD, 0, mat), (FD, 1, before), (FH, 0, jnp.where(row < 3, m1, m8)),
                           (FH, 1, jnp.where(row < 3, m2, m7))):
            for f, table in ((0, dil), (1, she)):
                value = jnp.zeros((ny, nx), f32)
                for level in range(table.shape[0]):
                    value = jnp.where(m == float(level), table[level], value)
                ref[n, f, ay] = value

    def masses(n):
        low, high = HQ[n, 0, 0:1], HQ[n, 0, 2:3]
        HIM[n] = DT * jnp.where(row < 3, jnp.broadcast_to(low, (ny, nx)), jnp.broadcast_to(high, (ny, nx)))

    here = lambda copy: copy.wait_recv()
    lat_k = (6, 7)
    for_all(first_copies, True, here, lat_k)
    for_bottom(True, here)

    @pl.loop(2, nz + 2)
    def _(n):
        fields(n)
        masses(n)

    at_bottom = (d == nd - 1).astype(f32)
    imp_rows = jnp.where((row == 0) | (row == 3), imp[0], jnp.where((row == 1) | (row == 4), imp[1], imp[2]))

    def ahead(x):
        return jnp.where(lane == nx - 1, 0.0, pltpu.roll(x, nx - 1, 1))

    def behind(x):
        return jnp.where(lane == 0, 0.0, pltpu.roll(x, 1, 1))

    def operand(t, n, extended):
        tiles = [W[t, n, 1, c] for c in range(3)]
        halo = [jnp.where(row < 6, HW[t, n, 1], 0.0)]
        if extended:
            halo.append(jnp.where(row < 6, HW[t, n, 2], 0.0))
        parts = tiles + [ahead(x) for x in tiles]
        for x in halo:
            parts += [x, ahead(x)]
        if not extended:
            parts += [jnp.zeros((ny, nx), f32)] * 2
        x = jnp.concatenate(parts, 0)
        hi = x.astype(bf16)
        XH[n] = hi
        XL[n] = (x - hi.astype(f32)).astype(bf16)

    def element(e, extended):
        m = MH if extended else MO
        x = jnp.concatenate([XH[e], XH[e + 1], XL[e], XL[e + 1], XH[e], XH[e + 1],
                             jnp.zeros((KP - 3 * KB, nx), bf16)], 0)
        slot = e % 2
        PR[slot, 0:m] = jnp.dot(WM[0:m], x, preferred_element_type=f32)
        sides = []
        for az in (0, 1):
            sums = {}
            for ax in (0, 1):
                for c in range(4 if extended else 3):
                    total = None
                    for f in (0, 1):
                        for ay in (0, 1):
                            g = 8 * f + 4 * az + 2 * ay + ax
                            if c < 3:
                                at = 8 * (3 * g + c)
                                term = FD[e, f, ay] * PR[slot, at:at + 8]
                            else:
                                at = MO + 8 * g
                                term = FH[e, f, ay] * PR[slot, at:at + 8]
                            total = term if total is None else total + term
                    sums[ax, c] = total
            sides.append(sums)
        return sides

    def advance(t, r, n, before, after, extended):
        force = [after[0, c] + before[0, c] + behind(after[1, c] + before[1, c])
                 for c in range(4 if extended else 3)]
        scale = DT * Q[n, 0]
        for c in range(3):
            net = -force[c]
            v = W[t, n, 0, c]
            if n == nz + 1:
                net = net + at_bottom * imp[c] * (BI[t // 2, r, c] - v)
            v = v + scale * net
            W[t + 1, n, 0, c] = v
            W[t + 1, n, 1, c] = W[t, n, 1, c] + DT * v
        if extended:
            net = -force[3]
            v = HW[t, n, 0]
            if n == nz + 1:
                net = net + at_bottom * imp_rows * (HB[t // 2] - v)
            v = v + HIM[n] * net
            HW[t + 1, n, 1] = HW[t, n, 1] + DT * v

    def run(t, r, extended, order, nodes, low, high):
        for e in order:
            low[e], high[e] = element(e, extended)
            for n in (e, e + 1):
                if n in nodes and n in low and n - 1 in high:
                    advance(t, r, n, high[n - 1], low[n], extended)
                    nodes.remove(n)

    def follow_tile(t, n):
        HW[t, n, 0] = (HW[t, n, 1] - HW[t - 1, n, 1]) * (1.0 / DT)

    def follow_layer(t, n):
        for c in range(3):
            W[t, n, 0, c] = (W[t, n, 1, c] - W[t - 1, n, 1, c]) * (1.0 / DT)

    top = nz + 2

    @pl.loop(0, rounds)
    def _(i):
        t = 2 * i

        @pl.when(i > 0)
        def _():
            for_all(lambda k: copies(t, k), True, here, lat_k)
            for n in range(2, top):
                follow_tile(t, n)

        low, high, nodes = {}, {}, set(range(1, top + 1))
        for n in range(2, top):
            operand(t, n, True)
        run(t, 0, True, range(2, top - 1), nodes, low, high)

        sides = {
            "low": ((0, 2, 3), (1, 0), 1, (1, 0)),
            "high": ((1, 4, 5), (top, top + 1), top, (top - 1, top)),
        }

        def finish_side(name, low, high, nodes):
            which, layers_in, edge, order = sides[name]

            @pl.when(i == 0)
            def _():
                for_all(first_copies, True, here, which)
                for n in (0, 1) if name == "low" else (top,):
                    fields(n)
                masses(edge)

            @pl.when(i > 0)
            def _():
                for_all(lambda k: copies(t, k), True, here, which)
                follow_tile(t, edge)
                follow_layer(t, edge)

            for n in layers_in:
                operand(t, n, True)
            run(t, 0, True, order, nodes, low, high)

        def send(which):
            @pl.when(i < rounds - 1)
            def _():
                for_all(lambda k: copies(t + 2, k), False, start, which)

        def rest(names):
            low_a, high_a, nodes_a = dict(low), dict(high), set(nodes)
            for name in names:
                finish_side(name, low_a, high_a, nodes_a)
            low_b, high_b, nodes_b = {}, {}, set(range(2, top))
            done = set()
            for name in names[::-1]:
                order = (1, 2, 3) if name == "low" else (top - 3, top - 2, top - 1)
                for n in range(order[0], order[-1] + 2):
                    if n not in done:
                        operand(t + 1, n, False)
                        done.add(n)
                run(t + 1, 1, False, order, nodes_b, low_b, high_b)
                send((1, 4, 5) if name == "low" else (0, 2, 3))
            for n in range(1, top + 1):
                if n not in done:
                    operand(t + 1, n, False)
            run(t + 1, 1, False, range(4, top - 3), nodes_b, low_b, high_b)
            send(lat_k)

        @pl.when(d < nd // 2)
        def _():
            rest(("low", "high"))

        @pl.when(d >= nd // 2)
        def _():
            rest(("high", "low"))

    for z in range(nz):
        for c in range(3):
            u_out[c, z] = W[steps, z + 2, 1, c]
            v_out[c, z] = W[steps, z + 2, 0, c]

    done = lambda copy: copy.wait_send()
    for_all(first_copies, False, done)
    for_bottom(False, done)

    @pl.loop(1, rounds)
    def _(i):
        for_all(lambda k: copies(2 * i, k), False, done)


def put_out(u, v, u_hbm, v_hbm, sem):
    copies = [pltpu.make_async_copy(a.at[c], b.at[c], sem.at[3 * i + c])
              for i, (a, b) in enumerate(((u, u_hbm), (v, v_hbm))) for c in range(3)]
    for copy in copies:
        copy.start()
    for copy in copies:
        copy.wait()


def per_device(nd, nl, displacement, velocity, inverse_mass, material, dilation_table, shear_table,
               stiffness_pair, impedance, bedrock_mask, incident):
    _, nz, ny, nx = displacement.shape
    steps = incident.shape[0]
    rounds = steps // 2
    nmat = dilation_table.shape[0]
    vmem = pl.BlockSpec(memory_space=pltpu.VMEM)
    hbm = pl.BlockSpec(memory_space=pltpu.MemorySpace.HBM)
    ext = nz + 4
    dma = pltpu.SemaphoreType.DMA
    state = pl.pallas_call(
        functools.partial(kernel, nd, nl),
        out_shape=[jax.ShapeDtypeStruct(displacement.shape, f32)] * 2,
        in_specs=[hbm] * 10,
        out_specs=[vmem, vmem],
        scratch_shapes=[
            pltpu.VMEM((steps + 1, ext, 2, 3, ny, nx), f32),
            pltpu.VMEM((steps, ext, 3, ny, nx), f32),
            pltpu.VMEM((ext, 2, ny, nx), f32),
            pltpu.VMEM((ext, 2, ny, nx), f32),
            pltpu.VMEM((rounds, 2, 3, ny, nx), f32),
            pltpu.VMEM((rounds, ny, nx), f32),
            pltpu.VMEM((nz, ny, nx), i32),
            pltpu.VMEM(stiffness_pair.shape, f32),
            pltpu.VMEM((ny, nx), i32),
            pltpu.VMEM((steps, 3, ny, nx), f32),
            pltpu.VMEM((2, 48, KP), f32),
            pltpu.VMEM((MH, KP), bf16),
            pltpu.VMEM((ext, KL, nx), bf16),
            pltpu.VMEM((ext, KL, nx), bf16),
            pltpu.VMEM((2, MH, nx), f32),
            pltpu.VMEM((ext, 2, 2, ny, nx), f32),
            pltpu.VMEM((ext, 2, 2, ny, nx), f32),
            pltpu.VMEM((ext, ny, nx), f32),
            pltpu.SMEM((nmat,), f32),
            pltpu.SMEM((nmat,), f32),
            pltpu.SMEM((3,), f32),
            dma((14,)),
            dma((rounds, 16)),
            dma((rounds, 16)),
            dma((48,)),
            dma((48,)),
            dma((2,)),
            dma((2,)),
        ],
        compiler_params=pltpu.CompilerParams(
            collective_id=0, has_side_effects=True, vmem_limit_bytes=48 * 1024 * 1024),
    )(*(pltpu.with_memory_space_constraint(x, pltpu.MemorySpace.HBM) for x in (
        displacement, velocity, inverse_mass, material, dilation_table, shear_table,
        stiffness_pair, impedance, bedrock_mask, incident)))
    return pl.pallas_call(
        put_out,
        out_shape=[jax.ShapeDtypeStruct(displacement.shape, f32)] * 2,
        in_specs=[vmem, vmem],
        out_specs=[pl.BlockSpec(memory_space=pltpu.MemorySpace.HBM)] * 2,
        scratch_shapes=[dma((6,))],
        compiler_params=pltpu.CompilerParams(vmem_limit_bytes=2 * 1024 * 1024),
    )(*state)


def solution(mesh):
    in_specs = (
        P(None, "depth", "lat", None),
        P(None, "depth", "lat", None),
        P("depth", "lat", None),
        P("depth", "lat", None),
        P(),
        P(),
        P(),
        P(),
        P("lat", None),
        P(None, None, "lat", None),
    )
    out_specs = (P(None, "depth", "lat", None), P(None, "depth", "lat", None))
    return jax.shard_map(
        functools.partial(per_device, mesh.shape["depth"], mesh.shape["lat"]),
        mesh=mesh, in_specs=in_specs, out_specs=out_specs, check_vma=False)
```

```python
import functools

import jax
import jax.numpy as jnp
from jax import lax
from jax.experimental import pallas as pl
from jax.experimental.pallas import tpu as pltpu
from jax.sharding import PartitionSpec as P

MESH = pl.DeviceIdType.MESH
DT = 0.1
f32, bf16, i32 = jnp.float32, jnp.bfloat16, jnp.int32
DIRECTIONS = ((1, 0), (-1, 0), (1, 1), (1, -1), (-1, 1), (-1, -1), (0, 1), (0, -1))

KL = 80
KB = 2 * KL
KP = 512
MO = 384
MH = 512


def kernel(
    nd, nl,
    u_in, v_in, im_in, mat_in, dil_in, she_in, k_in, imp_in, mask_in, inc_in,
    u_out, v_out,
    W, HW, Q, HQ, BI, HB, MI, KV, MV, IV, E, WM, XH, XL, PR, FD, FH, HIM,
    dil, she, imp,
    in_sem, send_sem, recv_sem, qsend_sem, qrecv_sem, bsend_sem, brecv_sem,
):
    steps = inc_in.shape[0]
    rounds = steps // 2
    nz, ny, nx = im_in.shape
    d = lax.axis_index("depth")
    l = lax.axis_index("lat")

    def exists(dz, dy):
        return ((d + dz >= 0) & (d + dz < nd)) & ((l + dy >= 0) & (l + dy < nl))

    barrier = pltpu.get_barrier_semaphore()
    partners = 0
    for dz, dy in DIRECTIONS:
        @pl.when(exists(dz, dy))
        def _():
            pl.semaphore_signal(barrier, inc=1, device_id=(d + dz, l + dy), device_id_type=MESH)
        partners = partners + exists(dz, dy).astype(i32)
    own = pl.ds(2, nz)
    loads = [(im_in, Q.at[own, 0]), (mat_in, MI)]
    for c in range(3):
        loads.append((u_in.at[c], W.at[0, own, 1, c]))
        loads.append((v_in.at[c], W.at[0, own, 0, c]))
    first = len(loads)
    loads += [(k_in, KV), (mask_in, MV), (inc_in, IV), (dil_in, dil), (she_in, she), (imp_in, imp)]
    loads = [pltpu.make_async_copy(a, b, in_sem.at[i]) for i, (a, b) in enumerate(loads)]
    for load in loads:
        load.start()

    for load in loads[:first]:
        load.wait()
    for z in range(nz):
        Q[z + 2, 1] = MI[z].astype(f32)
    pl.semaphore_wait(barrier, partners)

    def remote(src, dst, ss, rs, dz, dy):
        return pltpu.make_async_remote_copy(
            src_ref=src, dst_ref=dst, send_sem=ss, recv_sem=rs,
            device_id=(d + dz, l + dy), device_id_type=MESH)

    def layers(dz):
        if dz == 0:
            return own, own
        return (pl.ds(nz, 2), pl.ds(0, 2)) if dz == 1 else (pl.ds(2, 2), pl.ds(nz + 2, 2))

    def rows_of(dy):
        return (ny - 1, ny - 2, pl.ds(0, 3)) if dy == 1 else (0, 1, pl.ds(3, 3))

    def copies(t, k):
        dz, dy = DIRECTIONS[k]
        a, b = layers(dz)
        if dy == 0:
            pairs = [(W.at[t, a, 1], W.at[t, b, 1])]
        else:
            near_row, far_row, to = rows_of(dy)
            pairs = [(W.at[t, a, 1, :, near_row], HW.at[t, b, 1, to]),
                     (W.at[t, a, 1, :, far_row], HW.at[t, b, 2, to])]
        return [remote(src, dst, send_sem.at[t // 2, 2 * k + i], recv_sem.at[t // 2, 2 * k + i], dz, dy)
                for i, (src, dst) in enumerate(pairs)]

    def first_copies(k):
        dz, dy = DIRECTIONS[k]
        a, b = layers(dz)
        near, far = (nz + 1, nz) if dz == 1 else (2, 3)
        to_near, to_far = (1, 0) if dz == 1 else (nz + 2, nz + 3)
        if dy == 0:
            pairs = [(W.at[0, near], W.at[0, to_near]), (W.at[0, far, 1], W.at[0, to_far, 1]),
                     (Q.at[near], Q.at[to_near])]
            if dz == 1:
                pairs.append((Q.at[far, 1], Q.at[to_far, 1]))
        else:
            near_row, far_row, to = rows_of(dy)
            slot = 0 if dy == 1 else 2
            pairs = [(W.at[0, a, 1, :, far_row], HW.at[0, b, 2, to])]
            if dz == 0:
                pairs += [(W.at[0, a, :, :, near_row], HW.at[0, b, pl.ds(0, 2), to]),
                          (Q.at[a, :, near_row], HQ.at[b, :, slot])]
                if dy == 1:
                    pairs.append((Q.at[a, 1, far_row], HQ.at[b, 1, 1]))
            else:
                pairs += [(W.at[0, near, :, :, near_row], HW.at[0, to_near, pl.ds(0, 2), to]),
                          (W.at[0, far, 1, :, near_row], HW.at[0, to_far, 1, to]),
                          (Q.at[near, :, near_row], HQ.at[to_near, :, slot])]
                if dz == 1:
                    pairs.append((Q.at[far, 1, near_row], HQ.at[to_far, 1, slot]))
                if dy == 1:
                    if dz == 1:
                        pairs.append((Q.at[a, 1, far_row], HQ.at[b, 1, 1]))
                    else:
                        pairs.append((Q.at[near, 1, far_row], HQ.at[to_near, 1, 1]))
        return [remote(src, dst, qsend_sem.at[6 * k + i], qrecv_sem.at[6 * k + i], dz, dy)
                for i, (src, dst) in enumerate(pairs)]

    def b_copy(dy):
        row, to, i = (ny - 1, pl.ds(0, 3), 0) if dy == 1 else (0, pl.ds(3, 3), 1)
        return remote(BI.at[:, 0, :, row], HB.at[:, to], bsend_sem.at[i], brecv_sem.at[i], 0, dy)

    def for_all(make, backward, act, which=tuple(range(len(DIRECTIONS)))):
        for k in which:
            dz, dy = DIRECTIONS[k]
            sign = -1 if backward else 1

            @pl.when(exists(sign * dz, sign * dy))
            def _():
                for copy in make(k):
                    act(copy)

    def for_bottom(backward, act):
        for dy in (1, -1):
            @pl.when((d == nd - 1) & exists(0, -dy if backward else dy))
            def _():
                act(b_copy(dy))

    start = lambda copy: copy.start()
    for_all(first_copies, False, start, (6,7,0,1,2,3,4,5))

    for load in loads[first:]:
        load.wait()
    for r in range(rounds):
        for i in range(2):
            for c in range(3):
                BI[r, i, c] = 2.0 * MV[...].astype(f32) * IV[2 * r + i, c]
    for_bottom(False, start)

    def clear(n):
        for t in range(0, steps, 2):
            W[t, n] = jnp.zeros_like(W[t, n])
            HW[t, n] = jnp.zeros_like(HW[t, n])
        Q[n, 0] = jnp.zeros_like(Q[n, 0])
        Q[n, 1] = jnp.full_like(Q[n, 1], -1.0)
        HQ[n, 0] = jnp.zeros_like(HQ[n, 0])
        HQ[n, 1] = jnp.full_like(HQ[n, 1], -1.0)

    @pl.when(d == 0)
    def _():
        clear(0)
        clear(1)

    @pl.when(d == nd - 1)
    def _():
        clear(nz + 2)
        clear(nz + 3)

    def clear_side(rows, q_rows):
        for n in range(nz + 4):
            for t in range(0, steps, 2):
                for i in range(3):
                    HW[t, n, i, rows[0]:rows[1]] = jnp.zeros((3, nx), f32)
            HQ[n, 0, q_rows[0]:q_rows[1]] = jnp.zeros((q_rows[1] - q_rows[0], nx), f32)
            HQ[n, 1, q_rows[0]:q_rows[1]] = jnp.full((q_rows[1] - q_rows[0], nx), -1.0, f32)
        for r in range(rounds):
            HB[r, rows[0]:rows[1]] = jnp.zeros((3, nx), f32)

    @pl.when(d < nd - 1)
    def _():
        HB[...] = jnp.zeros_like(HB)

    @pl.when(l == 0)
    def _():
        clear_side((0, 3), (0, 2))

    @pl.when(l == nl - 1)
    def _():
        clear_side((3, 6), (2, 3))

    row = lax.broadcasted_iota(i32, (ny, nx), 0)
    lane = lax.broadcasted_iota(i32, (ny, nx), 1)

    def column_dofs(shape):
        j = lax.broadcasted_iota(i32, shape, 1)
        block = (j >= KB).astype(i32) + (j >= 2 * KB).astype(i32) + (j >= 3 * KB).astype(i32)
        j = j - KB * block
        bz = (j >= KL).astype(i32)
        j = j - KL * bz
        inner = j < 48
        bx_i = (j >= 24).astype(i32)
        c_i = (j - 24 * bx_i) >> 3
        y_i = j & 7
        h = j - 48
        far = (h >= 16).astype(i32)
        bx_h = (h >> 3) & 1
        r = h & 7
        s = (r >= 3).astype(i32)
        c_h = r - 3 * s
        y_h = jnp.where(r >= 6, 99, jnp.where(s == 0, -1 - far, 8 + far))
        y = jnp.where(inner, y_i, y_h)
        bx = jnp.where(inner, bx_i, bx_h)
        c = jnp.where(inner, c_i, c_h)
        return block, jnp.where(block < 3, y, 99), 12 * bz + 3 * bx + c

    block, _, dof = column_dofs((24, KP))
    i24 = lax.broadcasted_iota(i32, (24, KP), 0)
    stiff = jnp.concatenate([KV[0], KV[1]], 0)
    block48, _, _ = column_dofs((48, KP))
    for by in (0, 1):
        one_hot = (i24 == dof + 6 * by).astype(f32)
        e = jnp.dot(stiff, one_hot, precision=lax.Precision.HIGHEST, preferred_element_type=f32)
        e_hi = e.astype(bf16).astype(f32)
        E[by] = jnp.where(block48 == 2, e - e_hi, e_hi)
    _, y_col, _ = column_dofs((8, KP))
    r8 = lax.broadcasted_iota(i32, (8, KP), 0)
    y_halo = jnp.where(r8 < 3, -1, jnp.where(r8 < 6, 8, 199))

    def band(y_row, ay, picks):
        e0, e1 = picks
        delta = y_col - y_row + ay
        return jnp.where(delta == 0, e0, jnp.where(delta == 1, e1, 0.0))

    def wide(by, q):
        return jnp.broadcast_to(E[by, q:q + 1], (8, KP))

    for q in range(0, 48, 2):
        tiles = [band(r8, (p // 6) % 2, (wide(0, p), wide(1, p))) for p in (q, q + 1)]
        WM[8 * q:8 * q + 16] = jnp.concatenate(tiles, 0).astype(bf16)
    for g in range(0, 16, 2):
        tiles = []
        for p in (g, g + 1):
            picks = []
            for by in (0, 1):
                a, b, c = (wide(by, 3 * p + i) for i in range(3))
                picks.append(jnp.where((r8 == 0) | (r8 == 3), a, jnp.where((r8 == 1) | (r8 == 4), b, c)))
            tiles.append(band(y_halo, (p // 2) % 2, picks))
        WM[MO + 8 * g:MO + 8 * g + 16] = jnp.concatenate(tiles, 0).astype(bf16)

    def fields(n):
        def full(x):
            return jnp.broadcast_to(x, (ny, nx))
        mat = Q[n, 1]
        m1, m2, m8 = full(HQ[n, 1, 0:1]), full(HQ[n, 1, 1:2]), full(HQ[n, 1, 2:3])
        m7 = full(Q[n, 1, ny - 1:ny])
        before = jnp.where(row == 0, m1, pltpu.roll(mat, 1, 0))
        for ref, ay, m in ((FD, 0, mat), (FD, 1, before), (FH, 0, jnp.where(row < 3, m1, m8)),
                           (FH, 1, jnp.where(row < 3, m2, m7))):
            for f, table in ((0, dil), (1, she)):
                value = jnp.zeros((ny, nx), f32)
                for level in range(table.shape[0]):
                    value = jnp.where(m == float(level), table[level], value)
                ref[n, f, ay] = value

    def masses(n):
        low, high = HQ[n, 0, 0:1], HQ[n, 0, 2:3]
        HIM[n] = DT * jnp.where(row < 3, jnp.broadcast_to(low, (ny, nx)), jnp.broadcast_to(high, (ny, nx)))

    here = lambda copy: copy.wait_recv()
    lat_k = (6, 7)
    for_all(first_copies, True, here, lat_k)
    for_bottom(True, here)

    @pl.loop(2, nz + 2)
    def _(n):
        fields(n)
        masses(n)

    at_bottom = (d == nd - 1).astype(f32)
    imp_rows = jnp.where((row == 0) | (row == 3), imp[0], jnp.where((row == 1) | (row == 4), imp[1], imp[2]))

    def ahead(x):
        return jnp.where(lane == nx - 1, 0.0, pltpu.roll(x, nx - 1, 1))

    def behind(x):
        return jnp.where(lane == 0, 0.0, pltpu.roll(x, 1, 1))

    def operand(t, n, extended):
        tiles = [W[t, n, 1, c] for c in range(3)]
        halo = [jnp.where(row < 6, HW[t, n, 1], 0.0)]
        if extended:
            halo.append(jnp.where(row < 6, HW[t, n, 2], 0.0))
        parts = tiles + [ahead(x) for x in tiles]
        for x in halo:
            parts += [x, ahead(x)]
        if not extended:
            parts += [jnp.zeros((ny, nx), f32)] * 2
        x = jnp.concatenate(parts, 0)
        hi = x.astype(bf16)
        XH[n] = hi
        XL[n] = (x - hi.astype(f32)).astype(bf16)

    def element(e, extended):
        m = MH if extended else MO
        x = jnp.concatenate([XH[e], XH[e + 1], XL[e], XL[e + 1], XH[e], XH[e + 1],
                             jnp.zeros((KP - 3 * KB, nx), bf16)], 0)
        slot = e % 2
        PR[slot, 0:m] = jnp.dot(WM[0:m], x, preferred_element_type=f32)
        sides = []
        for az in (0, 1):
            sums = {}
            for ax in (0, 1):
                for c in range(4 if extended else 3):
                    total = None
                    for f in (0, 1):
                        for ay in (0, 1):
                            g = 8 * f + 4 * az + 2 * ay + ax
                            if c < 3:
                                at = 8 * (3 * g + c)
                                term = FD[e, f, ay] * PR[slot, at:at + 8]
                            else:
                                at = MO + 8 * g
                                term = FH[e, f, ay] * PR[slot, at:at + 8]
                            total = term if total is None else total + term
                    sums[ax, c] = total
            sides.append(sums)
        return sides

    def advance(t, r, n, before, after, extended):
        force = [after[0, c] + before[0, c] + behind(after[1, c] + before[1, c])
                 for c in range(4 if extended else 3)]
        scale = DT * Q[n, 0]
        for c in range(3):
            net = -force[c]
            v = W[t, n, 0, c]
            if n == nz + 1:
                net = net + at_bottom * imp[c] * (BI[t // 2, r, c] - v)
            v = v + scale * net
            W[t + 1, n, 0, c] = v
            W[t + 1, n, 1, c] = W[t, n, 1, c] + DT * v
        if extended:
            net = -force[3]
            v = HW[t, n, 0]
            if n == nz + 1:
                net = net + at_bottom * imp_rows * (HB[t // 2] - v)
            v = v + HIM[n] * net
            HW[t + 1, n, 1] = HW[t, n, 1] + DT * v

    def run(t, r, extended, order, nodes, low, high):
        for e in order:
            low[e], high[e] = element(e, extended)
            for n in (e, e + 1):
                if n in nodes and n in low and n - 1 in high:
                    advance(t, r, n, high[n - 1], low[n], extended)
                    nodes.remove(n)

    def follow_tile(t, n):
        HW[t, n, 0] = (HW[t, n, 1] - HW[t - 1, n, 1]) * (1.0 / DT)

    def follow_layer(t, n):
        for c in range(3):
            W[t, n, 0, c] = (W[t, n, 1, c] - W[t - 1, n, 1, c]) * (1.0 / DT)

    top = nz + 2

    @pl.loop(0, rounds)
    def _(i):
        t = 2 * i

        @pl.when(i > 0)
        def _():
            for_all(lambda k: copies(t, k), True, here, lat_k)
            for n in range(2, top):
                follow_tile(t, n)

        low, high, nodes = {}, {}, set(range(1, top + 1))
        for n in range(2, top):
            operand(t, n, True)
        run(t, 0, True, range(2, top - 1), nodes, low, high)

        sides = {
            "low": ((0, 2, 3), (1, 0), 1, (1, 0)),
            "high": ((1, 4, 5), (top, top + 1), top, (top - 1, top)),
        }

        def finish_side(name, low, high, nodes):
            which, layers_in, edge, order = sides[name]

            @pl.when(i == 0)
            def _():
                for_all(first_copies, True, here, which)
                for n in (0, 1) if name == "low" else (top,):
                    fields(n)
                masses(edge)

            @pl.when(i > 0)
            def _():
                for_all(lambda k: copies(t, k), True, here, which)
                follow_tile(t, edge)
                follow_layer(t, edge)

            for n in layers_in:
                operand(t, n, True)
            run(t, 0, True, order, nodes, low, high)

        def send(which):
            @pl.when(i < rounds - 1)
            def _():
                for_all(lambda k: copies(t + 2, k), False, start, which)

        def rest(names):
            low_a, high_a, nodes_a = dict(low), dict(high), set(nodes)
            for name in names:
                finish_side(name, low_a, high_a, nodes_a)
            low_b, high_b, nodes_b = {}, {}, set(range(2, top))
            done = set()
            for name in names[::-1]:
                order = (1, 2, 3) if name == "low" else (top - 3, top - 2, top - 1)
                for n in range(order[0], order[-1] + 2):
                    if n not in done:
                        operand(t + 1, n, False)
                        done.add(n)
                run(t + 1, 1, False, order, nodes_b, low_b, high_b)
                send((1, 4, 5) if name == "low" else (0, 2, 3))
            for n in range(1, top + 1):
                if n not in done:
                    operand(t + 1, n, False)
            run(t + 1, 1, False, range(4, top - 3), nodes_b, low_b, high_b)
            send(lat_k)

        @pl.when(d < nd // 2)
        def _():
            rest(("low", "high"))

        @pl.when(d >= nd // 2)
        def _():
            rest(("high", "low"))

    for z in range(nz):
        for c in range(3):
            u_out[c, z] = W[steps, z + 2, 1, c]
            v_out[c, z] = W[steps, z + 2, 0, c]

    done = lambda copy: copy.wait_send()
    for_all(first_copies, False, done)
    for_bottom(False, done)

    @pl.loop(1, rounds)
    def _(i):
        for_all(lambda k: copies(2 * i, k), False, done)


def put_out(u, v, u_hbm, v_hbm, sem):
    copies = [pltpu.make_async_copy(a.at[c], b.at[c], sem.at[3 * i + c])
              for i, (a, b) in enumerate(((u, u_hbm), (v, v_hbm))) for c in range(3)]
    for copy in copies:
        copy.start()
    for copy in copies:
        copy.wait()


def per_device(nd, nl, displacement, velocity, inverse_mass, material, dilation_table, shear_table,
               stiffness_pair, impedance, bedrock_mask, incident):
    _, nz, ny, nx = displacement.shape
    steps = incident.shape[0]
    rounds = steps // 2
    nmat = dilation_table.shape[0]
    vmem = pl.BlockSpec(memory_space=pltpu.VMEM)
    hbm = pl.BlockSpec(memory_space=pltpu.MemorySpace.HBM)
    ext = nz + 4
    dma = pltpu.SemaphoreType.DMA
    state = pl.pallas_call(
        functools.partial(kernel, nd, nl),
        out_shape=[jax.ShapeDtypeStruct(displacement.shape, f32)] * 2,
        in_specs=[hbm] * 10,
        out_specs=[vmem, vmem],
        scratch_shapes=[
            pltpu.VMEM((steps + 1, ext, 2, 3, ny, nx), f32),
            pltpu.VMEM((steps, ext, 3, ny, nx), f32),
            pltpu.VMEM((ext, 2, ny, nx), f32),
            pltpu.VMEM((ext, 2, ny, nx), f32),
            pltpu.VMEM((rounds, 2, 3, ny, nx), f32),
            pltpu.VMEM((rounds, ny, nx), f32),
            pltpu.VMEM((nz, ny, nx), i32),
            pltpu.VMEM(stiffness_pair.shape, f32),
            pltpu.VMEM((ny, nx), i32),
            pltpu.VMEM((steps, 3, ny, nx), f32),
            pltpu.VMEM((2, 48, KP), f32),
            pltpu.VMEM((MH, KP), bf16),
            pltpu.VMEM((ext, KL, nx), bf16),
            pltpu.VMEM((ext, KL, nx), bf16),
            pltpu.VMEM((2, MH, nx), f32),
            pltpu.VMEM((ext, 2, 2, ny, nx), f32),
            pltpu.VMEM((ext, 2, 2, ny, nx), f32),
            pltpu.VMEM((ext, ny, nx), f32),
            pltpu.SMEM((nmat,), f32),
            pltpu.SMEM((nmat,), f32),
            pltpu.SMEM((3,), f32),
            dma((14,)),
            dma((rounds, 16)),
            dma((rounds, 16)),
            dma((48,)),
            dma((48,)),
            dma((2,)),
            dma((2,)),
        ],
        compiler_params=pltpu.CompilerParams(
            collective_id=0, has_side_effects=True, vmem_limit_bytes=48 * 1024 * 1024),
    )(*(pltpu.with_memory_space_constraint(x, pltpu.MemorySpace.HBM) for x in (
        displacement, velocity, inverse_mass, material, dilation_table, shear_table,
        stiffness_pair, impedance, bedrock_mask, incident)))
    return pl.pallas_call(
        put_out,
        out_shape=[jax.ShapeDtypeStruct(displacement.shape, f32)] * 2,
        in_specs=[vmem, vmem],
        out_specs=[pl.BlockSpec(memory_space=pltpu.MemorySpace.HBM)] * 2,
        scratch_shapes=[dma((6,))],
        compiler_params=pltpu.CompilerParams(vmem_limit_bytes=2 * 1024 * 1024),
    )(*state)


def solution(mesh):
    in_specs = (
        P(None, "depth", "lat", None),
        P(None, "depth", "lat", None),
        P("depth", "lat", None),
        P("depth", "lat", None),
        P(),
        P(),
        P(),
        P(),
        P("lat", None),
        P(None, None, "lat", None),
    )
    out_specs = (P(None, "depth", "lat", None), P(None, "depth", "lat", None))
    return jax.shard_map(
        functools.partial(per_device, mesh.shape["depth"], mesh.shape["lat"]),
        mesh=mesh, in_specs=in_specs, out_specs=out_specs, check_vma=False)
```

```python
import functools

import jax
import jax.numpy as jnp
from jax import lax
from jax.experimental import pallas as pl
from jax.experimental.pallas import tpu as pltpu
from jax.sharding import PartitionSpec as P

MESH = pl.DeviceIdType.MESH
DT = 0.1
f32, bf16, i32 = jnp.float32, jnp.bfloat16, jnp.int32
DIRECTIONS = ((1, 0), (-1, 0), (1, 1), (1, -1), (-1, 1), (-1, -1), (0, 1), (0, -1))

KL = 80
KB = 2 * KL
KP = 512
MO = 384
MH = 512


def kernel(
    nd, nl,
    u_in, v_in, im_in, mat_in, dil_in, she_in, k_in, imp_in, mask_in, inc_in,
    u_out, v_out,
    W, HW, Q, HQ, BI, HB, MI, KV, MV, IV, E, WM, XH, XL, PR, FD, FH, HIM,
    dil, she, imp,
    in_sem, send_sem, recv_sem, qsend_sem, qrecv_sem, bsend_sem, brecv_sem,
):
    steps = inc_in.shape[0]
    rounds = steps // 2
    nz, ny, nx = im_in.shape
    d = lax.axis_index("depth")
    l = lax.axis_index("lat")

    def exists(dz, dy):
        return ((d + dz >= 0) & (d + dz < nd)) & ((l + dy >= 0) & (l + dy < nl))

    barrier = pltpu.get_barrier_semaphore()
    partners = 0
    for dz, dy in DIRECTIONS:
        @pl.when(exists(dz, dy))
        def _():
            pl.semaphore_signal(barrier, inc=1, device_id=(d + dz, l + dy), device_id_type=MESH)
        partners = partners + exists(dz, dy).astype(i32)
    own = pl.ds(2, nz)
    loads = [(im_in, Q.at[own, 0]), (mat_in, MI)]
    for c in range(3):
        loads.append((u_in.at[c], W.at[0, own, 1, c]))
        loads.append((v_in.at[c], W.at[0, own, 0, c]))
    first = len(loads)
    loads += [(k_in, KV), (mask_in, MV), (inc_in, IV), (dil_in, dil), (she_in, she), (imp_in, imp)]
    loads = [pltpu.make_async_copy(a, b, in_sem.at[i]) for i, (a, b) in enumerate(loads)]
    for load in loads:
        load.start()

    for load in loads[:first]:
        load.wait()
    for z in range(nz):
        Q[z + 2, 1] = MI[z].astype(f32)
    pl.semaphore_wait(barrier, partners)

    def remote(src, dst, ss, rs, dz, dy):
        return pltpu.make_async_remote_copy(
            src_ref=src, dst_ref=dst, send_sem=ss, recv_sem=rs,
            device_id=(d + dz, l + dy), device_id_type=MESH)

    def layers(dz):
        if dz == 0:
            return own, own
        return (pl.ds(nz, 2), pl.ds(0, 2)) if dz == 1 else (pl.ds(2, 2), pl.ds(nz + 2, 2))

    def rows_of(dy):
        return (ny - 1, ny - 2, pl.ds(0, 3)) if dy == 1 else (0, 1, pl.ds(3, 3))

    def copies(t, k):
        dz, dy = DIRECTIONS[k]
        a, b = layers(dz)
        if dy == 0:
            pairs = [(W.at[t, a, 1], W.at[t, b, 1])]
        else:
            near_row, far_row, to = rows_of(dy)
            pairs = [(W.at[t, a, 1, :, near_row], HW.at[t, b, 1, to]),
                     (W.at[t, a, 1, :, far_row], HW.at[t, b, 2, to])]
        return [remote(src, dst, send_sem.at[t // 2, 2 * k + i], recv_sem.at[t // 2, 2 * k + i], dz, dy)
                for i, (src, dst) in enumerate(pairs)]

    def first_copies(k, part="all"):
        dz, dy = DIRECTIONS[k]
        a, b = layers(dz)
        near, far = (nz + 1, nz) if dz == 1 else (2, 3)
        to_near, to_far = (1, 0) if dz == 1 else (nz + 2, nz + 3)
        if dy == 0:
            pairs = [(W.at[0, a, 1], W.at[0, b, 1])]
            pairs.append((Q.at[a, 1], Q.at[b, 1]) if dz == 1 else (Q.at[near, 1], Q.at[to_near, 1]))
            late = [(W.at[0, near, 0], W.at[0, to_near, 0]), (Q.at[near, 0], Q.at[to_near, 0])]
        else:
            near_row, far_row, to = rows_of(dy)
            slot = 0 if dy == 1 else 2
            pairs = [(W.at[0, a, 1, :, near_row], HW.at[0, b, 1, to]),
                     (W.at[0, a, 1, :, far_row], HW.at[0, b, 2, to])]
            m, to_m = (near, to_near) if dz == -1 else (a, b)
            pairs.append((Q.at[m, 1, near_row], HQ.at[to_m, 1, slot]))
            if dy == 1:
                pairs.append((Q.at[m, 1, far_row], HQ.at[to_m, 1, 1]))
            n, to_n = (a, b) if dz == 0 else (near, to_near)
            late = [(W.at[0, n, 0, :, near_row], HW.at[0, to_n, 0, to]),
                    (Q.at[n, 0, near_row], HQ.at[to_n, 0, slot])]
        offset = len(pairs) if part == "late" else 0
        pairs = {"all": pairs + late, "early": pairs, "late": late}[part]
        return [remote(src, dst, qsend_sem.at[6 * k + offset + i], qrecv_sem.at[6 * k + offset + i], dz, dy)
                for i, (src, dst) in enumerate(pairs)]

    def b_copy(dy):
        row, to, i = (ny - 1, pl.ds(0, 3), 0) if dy == 1 else (0, pl.ds(3, 3), 1)
        return remote(BI.at[:, 0, :, row], HB.at[:, to], bsend_sem.at[i], brecv_sem.at[i], 0, dy)

    def for_all(make, backward, act, which=tuple(range(len(DIRECTIONS)))):
        for k in which:
            dz, dy = DIRECTIONS[k]
            sign = -1 if backward else 1

            @pl.when(exists(sign * dz, sign * dy))
            def _():
                for copy in make(k):
                    act(copy)

    def for_bottom(backward, act):
        for dy in (1, -1):
            @pl.when((d == nd - 1) & exists(0, -dy if backward else dy))
            def _():
                act(b_copy(dy))

    start = lambda copy: copy.start()
    for_all(first_copies, False, start, (6, 7))
    for part in ("early", "late"):
        for_all(lambda k: first_copies(k, part), False, start, (0, 1, 2, 3, 4, 5))

    for load in loads[first:]:
        load.wait()
    for r in range(rounds):
        for i in range(2):
            for c in range(3):
                BI[r, i, c] = 2.0 * MV[...].astype(f32) * IV[2 * r + i, c]
    for_bottom(False, start)

    def clear(n):
        for t in range(0, steps, 2):
            W[t, n] = jnp.zeros_like(W[t, n])
            HW[t, n] = jnp.zeros_like(HW[t, n])
        Q[n, 0] = jnp.zeros_like(Q[n, 0])
        Q[n, 1] = jnp.full_like(Q[n, 1], -1.0)
        HQ[n, 0] = jnp.zeros_like(HQ[n, 0])
        HQ[n, 1] = jnp.full_like(HQ[n, 1], -1.0)

    @pl.when(d == 0)
    def _():
        clear(0)
        clear(1)

    @pl.when(d == nd - 1)
    def _():
        clear(nz + 2)
        clear(nz + 3)

    def clear_side(rows, q_rows):
        for n in range(nz + 4):
            for t in range(0, steps, 2):
                for i in range(3):
                    HW[t, n, i, rows[0]:rows[1]] = jnp.zeros((3, nx), f32)
            HQ[n, 0, q_rows[0]:q_rows[1]] = jnp.zeros((q_rows[1] - q_rows[0], nx), f32)
            HQ[n, 1, q_rows[0]:q_rows[1]] = jnp.full((q_rows[1] - q_rows[0], nx), -1.0, f32)
        for r in range(rounds):
            HB[r, rows[0]:rows[1]] = jnp.zeros((3, nx), f32)

    @pl.when(d < nd - 1)
    def _():
        HB[...] = jnp.zeros_like(HB)

    @pl.when(l == 0)
    def _():
        clear_side((0, 3), (0, 2))

    @pl.when(l == nl - 1)
    def _():
        clear_side((3, 6), (2, 3))

    row = lax.broadcasted_iota(i32, (ny, nx), 0)
    lane = lax.broadcasted_iota(i32, (ny, nx), 1)

    def column_dofs(shape):
        j = lax.broadcasted_iota(i32, shape, 1)
        block = (j >= KB).astype(i32) + (j >= 2 * KB).astype(i32) + (j >= 3 * KB).astype(i32)
        j = j - KB * block
        bz = (j >= KL).astype(i32)
        j = j - KL * bz
        inner = j < 48
        bx_i = (j >= 24).astype(i32)
        c_i = (j - 24 * bx_i) >> 3
        y_i = j & 7
        h = j - 48
        far = (h >= 16).astype(i32)
        bx_h = (h >> 3) & 1
        r = h & 7
        s = (r >= 3).astype(i32)
        c_h = r - 3 * s
        y_h = jnp.where(r >= 6, 99, jnp.where(s == 0, -1 - far, 8 + far))
        y = jnp.where(inner, y_i, y_h)
        bx = jnp.where(inner, bx_i, bx_h)
        c = jnp.where(inner, c_i, c_h)
        return block, jnp.where(block < 3, y, 99), 12 * bz + 3 * bx + c

    block, _, dof = column_dofs((24, KP))
    i24 = lax.broadcasted_iota(i32, (24, KP), 0)
    stiff = jnp.concatenate([KV[0], KV[1]], 0)
    block48, _, _ = column_dofs((48, KP))
    for by in (0, 1):
        one_hot = (i24 == dof + 6 * by).astype(f32)
        e = jnp.dot(stiff, one_hot, precision=lax.Precision.HIGHEST, preferred_element_type=f32)
        e_hi = e.astype(bf16).astype(f32)
        E[by] = jnp.where(block48 == 2, e - e_hi, e_hi)
    _, y_col, _ = column_dofs((8, KP))
    r8 = lax.broadcasted_iota(i32, (8, KP), 0)
    y_halo = jnp.where(r8 < 3, -1, jnp.where(r8 < 6, 8, 199))

    def band(y_row, ay, picks):
        e0, e1 = picks
        delta = y_col - y_row + ay
        return jnp.where(delta == 0, e0, jnp.where(delta == 1, e1, 0.0))

    def wide(by, q):
        return jnp.broadcast_to(E[by, q:q + 1], (8, KP))

    for q in range(0, 48, 2):
        tiles = [band(r8, (p // 6) % 2, (wide(0, p), wide(1, p))) for p in (q, q + 1)]
        WM[8 * q:8 * q + 16] = jnp.concatenate(tiles, 0).astype(bf16)
    for g in range(0, 16, 2):
        tiles = []
        for p in (g, g + 1):
            picks = []
            for by in (0, 1):
                a, b, c = (wide(by, 3 * p + i) for i in range(3))
                picks.append(jnp.where((r8 == 0) | (r8 == 3), a, jnp.where((r8 == 1) | (r8 == 4), b, c)))
            tiles.append(band(y_halo, (p // 2) % 2, picks))
        WM[MO + 8 * g:MO + 8 * g + 16] = jnp.concatenate(tiles, 0).astype(bf16)

    def fields(n):
        def full(x):
            return jnp.broadcast_to(x, (ny, nx))
        mat = Q[n, 1]
        m1, m2, m8 = full(HQ[n, 1, 0:1]), full(HQ[n, 1, 1:2]), full(HQ[n, 1, 2:3])
        m7 = full(Q[n, 1, ny - 1:ny])
        before = jnp.where(row == 0, m1, pltpu.roll(mat, 1, 0))
        for ref, ay, m in ((FD, 0, mat), (FD, 1, before), (FH, 0, jnp.where(row < 3, m1, m8)),
                           (FH, 1, jnp.where(row < 3, m2, m7))):
            for f, table in ((0, dil), (1, she)):
                value = jnp.zeros((ny, nx), f32)
                for level in range(table.shape[0]):
                    value = jnp.where(m == float(level), table[level], value)
                ref[n, f, ay] = value

    def masses(n):
        low, high = HQ[n, 0, 0:1], HQ[n, 0, 2:3]
        HIM[n] = DT * jnp.where(row < 3, jnp.broadcast_to(low, (ny, nx)), jnp.broadcast_to(high, (ny, nx)))

    here = lambda copy: copy.wait_recv()
    lat_k = (6, 7)
    for_all(first_copies, True, here, lat_k)
    for_bottom(True, here)

    @pl.loop(2, nz + 2)
    def _(n):
        fields(n)
        masses(n)

    at_bottom = (d == nd - 1).astype(f32)
    imp_rows = jnp.where((row == 0) | (row == 3), imp[0], jnp.where((row == 1) | (row == 4), imp[1], imp[2]))

    def ahead(x):
        return jnp.where(lane == nx - 1, 0.0, pltpu.roll(x, nx - 1, 1))

    def behind(x):
        return jnp.where(lane == 0, 0.0, pltpu.roll(x, 1, 1))

    def operand(t, n, extended):
        tiles = [W[t, n, 1, c] for c in range(3)]
        halo = [jnp.where(row < 6, HW[t, n, 1], 0.0)]
        if extended:
            halo.append(jnp.where(row < 6, HW[t, n, 2], 0.0))
        parts = tiles + [ahead(x) for x in tiles]
        for x in halo:
            parts += [x, ahead(x)]
        if not extended:
            parts += [jnp.zeros((ny, nx), f32)] * 2
        x = jnp.concatenate(parts, 0)
        hi = x.astype(bf16)
        XH[n] = hi
        XL[n] = (x - hi.astype(f32)).astype(bf16)

    def element(e, extended):
        m = MH if extended else MO
        x = jnp.concatenate([XH[e], XH[e + 1], XL[e], XL[e + 1], XH[e], XH[e + 1],
                             jnp.zeros((KP - 3 * KB, nx), bf16)], 0)
        slot = e % 2
        PR[slot, 0:m] = jnp.dot(WM[0:m], x, preferred_element_type=f32)
        sides = []
        for az in (0, 1):
            sums = {}
            for ax in (0, 1):
                for c in range(4 if extended else 3):
                    total = None
                    for f in (0, 1):
                        for ay in (0, 1):
                            g = 8 * f + 4 * az + 2 * ay + ax
                            if c < 3:
                                at = 8 * (3 * g + c)
                                term = FD[e, f, ay] * PR[slot, at:at + 8]
                            else:
                                at = MO + 8 * g
                                term = FH[e, f, ay] * PR[slot, at:at + 8]
                            total = term if total is None else total + term
                    sums[ax, c] = total
            sides.append(sums)
        return sides

    def advance(t, r, n, before, after, extended):
        force = [after[0, c] + before[0, c] + behind(after[1, c] + before[1, c])
                 for c in range(4 if extended else 3)]
        scale = DT * Q[n, 0]
        for c in range(3):
            net = -force[c]
            v = W[t, n, 0, c]
            if n == nz + 1:
                net = net + at_bottom * imp[c] * (BI[t // 2, r, c] - v)
            v = v + scale * net
            W[t + 1, n, 0, c] = v
            W[t + 1, n, 1, c] = W[t, n, 1, c] + DT * v
        if extended:
            net = -force[3]
            v = HW[t, n, 0]
            if n == nz + 1:
                net = net + at_bottom * imp_rows * (HB[t // 2] - v)
            v = v + HIM[n] * net
            HW[t + 1, n, 1] = HW[t, n, 1] + DT * v

    def run(t, r, extended, order, nodes, low, high):
        for e in order:
            low[e], high[e] = element(e, extended)
            for n in (e, e + 1):
                if n in nodes and n in low and n - 1 in high:
                    advance(t, r, n, high[n - 1], low[n], extended)
                    nodes.remove(n)

    def follow_tile(t, n):
        HW[t, n, 0] = (HW[t, n, 1] - HW[t - 1, n, 1]) * (1.0 / DT)

    def follow_layer(t, n):
        for c in range(3):
            W[t, n, 0, c] = (W[t, n, 1, c] - W[t - 1, n, 1, c]) * (1.0 / DT)

    top = nz + 2

    @pl.loop(0, rounds)
    def _(i):
        t = 2 * i

        @pl.when(i > 0)
        def _():
            for_all(lambda k: copies(t, k), True, here, lat_k)
            for n in range(2, top):
                follow_tile(t, n)

        low, high, nodes = {}, {}, set(range(1, top + 1))
        for n in range(2, top):
            operand(t, n, True)
        run(t, 0, True, range(2, top - 1), nodes, low, high)

        sides = {
            "low": ((0, 2, 3), (1, 0), 1, (1, 0)),
            "high": ((1, 4, 5), (top, top + 1), top, (top - 1, top)),
        }

        def finish_side(name, low, high, nodes):
            which, layers_in, edge, order = sides[name]

            @pl.when(i == 0)
            def _():
                for_all(lambda k: first_copies(k, "early"), True, here, which)
                for n in (0, 1) if name == "low" else (top,):
                    fields(n)

            @pl.when(i > 0)
            def _():
                for_all(lambda k: copies(t, k), True, here, which)
                follow_tile(t, edge)
                follow_layer(t, edge)

            for n in layers_in:
                operand(t, n, True)
            nodes.remove(edge)
            run(t, 0, True, order, nodes, low, high)

            @pl.when(i == 0)
            def _():
                for_all(lambda k: first_copies(k, "late"), True, here, which)
                masses(edge)

            advance(t, 0, edge, high[edge - 1], low[edge], True)

        def send(which):
            @pl.when(i < rounds - 1)
            def _():
                for_all(lambda k: copies(t + 2, k), False, start, which)

        def rest(names):
            low_a, high_a, nodes_a = dict(low), dict(high), set(nodes)
            low_b, high_b, nodes_b = {}, {}, set(range(2, top))
            up = names[0] == "low"
            layers_b = range(1, top + 1) if up else range(top, 0, -1)
            order = range(1, top) if up else range(top - 1, 0, -1)
            parts = ((layers_b[:-2], order[:-2]), (layers_b[-2:], order[-2:]))
            for name, (ns, es) in zip(names, parts):
                finish_side(name, low_a, high_a, nodes_a)
                for n in ns:
                    operand(t + 1, n, False)
                run(t + 1, 1, False, es, nodes_b, low_b, high_b)
                send((1, 4, 5) if name == "low" else (0, 2, 3))
            send(lat_k)

        @pl.when(d < nd // 2)
        def _():
            rest(("low", "high"))

        @pl.when(d >= nd // 2)
        def _():
            rest(("high", "low"))

    for z in range(nz):
        for c in range(3):
            u_out[c, z] = W[steps, z + 2, 1, c]
            v_out[c, z] = W[steps, z + 2, 0, c]

    done = lambda copy: copy.wait_send()
    for_all(first_copies, False, done)
    for_bottom(False, done)

    @pl.loop(1, rounds)
    def _(i):
        for_all(lambda k: copies(2 * i, k), False, done)


def put_out(u, v, u_hbm, v_hbm, sem):
    copies = [pltpu.make_async_copy(a.at[c], b.at[c], sem.at[3 * i + c])
              for i, (a, b) in enumerate(((u, u_hbm), (v, v_hbm))) for c in range(3)]
    for copy in copies:
        copy.start()
    for copy in copies:
        copy.wait()


def per_device(nd, nl, displacement, velocity, inverse_mass, material, dilation_table, shear_table,
               stiffness_pair, impedance, bedrock_mask, incident):
    _, nz, ny, nx = displacement.shape
    steps = incident.shape[0]
    rounds = steps // 2
    nmat = dilation_table.shape[0]
    vmem = pl.BlockSpec(memory_space=pltpu.VMEM)
    hbm = pl.BlockSpec(memory_space=pltpu.MemorySpace.HBM)
    ext = nz + 4
    dma = pltpu.SemaphoreType.DMA
    state = pl.pallas_call(
        functools.partial(kernel, nd, nl),
        out_shape=[jax.ShapeDtypeStruct(displacement.shape, f32)] * 2,
        in_specs=[hbm] * 10,
        out_specs=[vmem, vmem],
        scratch_shapes=[
            pltpu.VMEM((steps + 1, ext, 2, 3, ny, nx), f32),
            pltpu.VMEM((steps, ext, 3, ny, nx), f32),
            pltpu.VMEM((ext, 2, ny, nx), f32),
            pltpu.VMEM((ext, 2, ny, nx), f32),
            pltpu.VMEM((rounds, 2, 3, ny, nx), f32),
            pltpu.VMEM((rounds, ny, nx), f32),
            pltpu.VMEM((nz, ny, nx), i32),
            pltpu.VMEM(stiffness_pair.shape, f32),
            pltpu.VMEM((ny, nx), i32),
            pltpu.VMEM((steps, 3, ny, nx), f32),
            pltpu.VMEM((2, 48, KP), f32),
            pltpu.VMEM((MH, KP), bf16),
            pltpu.VMEM((ext, KL, nx), bf16),
            pltpu.VMEM((ext, KL, nx), bf16),
            pltpu.VMEM((2, MH, nx), f32),
            pltpu.VMEM((ext, 2, 2, ny, nx), f32),
            pltpu.VMEM((ext, 2, 2, ny, nx), f32),
            pltpu.VMEM((ext, ny, nx), f32),
            pltpu.SMEM((nmat,), f32),
            pltpu.SMEM((nmat,), f32),
            pltpu.SMEM((3,), f32),
            dma((14,)),
            dma((rounds, 16)),
            dma((rounds, 16)),
            dma((48,)),
            dma((48,)),
            dma((2,)),
            dma((2,)),
        ],
        compiler_params=pltpu.CompilerParams(
            collective_id=0, has_side_effects=True, vmem_limit_bytes=48 * 1024 * 1024),
    )(*(pltpu.with_memory_space_constraint(x, pltpu.MemorySpace.HBM) for x in (
        displacement, velocity, inverse_mass, material, dilation_table, shear_table,
        stiffness_pair, impedance, bedrock_mask, incident)))
    return pl.pallas_call(
        put_out,
        out_shape=[jax.ShapeDtypeStruct(displacement.shape, f32)] * 2,
        in_specs=[vmem, vmem],
        out_specs=[pl.BlockSpec(memory_space=pltpu.MemorySpace.HBM)] * 2,
        scratch_shapes=[dma((6,))],
        compiler_params=pltpu.CompilerParams(vmem_limit_bytes=2 * 1024 * 1024),
    )(*state)


def solution(mesh):
    in_specs = (
        P(None, "depth", "lat", None),
        P(None, "depth", "lat", None),
        P("depth", "lat", None),
        P("depth", "lat", None),
        P(),
        P(),
        P(),
        P(),
        P("lat", None),
        P(None, None, "lat", None),
    )
    out_specs = (P(None, "depth", "lat", None), P(None, "depth", "lat", None))
    return jax.shard_map(
        functools.partial(per_device, mesh.shape["depth"], mesh.shape["lat"]),
        mesh=mesh, in_specs=in_specs, out_specs=out_specs, check_vma=False)
```

```python
import functools

import jax
import jax.numpy as jnp
from jax import lax
from jax.experimental import pallas as pl
from jax.experimental.pallas import tpu as pltpu
from jax.sharding import PartitionSpec as P

MESH = pl.DeviceIdType.MESH
DT = 0.1
f32, bf16, i32 = jnp.float32, jnp.bfloat16, jnp.int32
DIRECTIONS = ((1, 0), (-1, 0), (1, 1), (1, -1), (-1, 1), (-1, -1), (0, 1), (0, -1))

KL = 80
KB = 2 * KL
KP = 512
MO = 384
MH = 512


def kernel(
    nd, nl,
    u_in, v_in, im_in, mat_in, dil_in, she_in, k_in, imp_in, mask_in, inc_in,
    u_out, v_out,
    W, HW, Q, HQ, BI, HB, MI, KV, MV, IV, E, WM, XH, XL, PR, FD, FH, HIM,
    dil, she, imp,
    in_sem, send_sem, recv_sem, qsend_sem, qrecv_sem, bsend_sem, brecv_sem,
):
    steps = inc_in.shape[0]
    rounds = steps // 2
    nz, ny, nx = im_in.shape
    d = lax.axis_index("depth")
    l = lax.axis_index("lat")

    def exists(dz, dy):
        return ((d + dz >= 0) & (d + dz < nd)) & ((l + dy >= 0) & (l + dy < nl))

    barrier = pltpu.get_barrier_semaphore()
    partners = 0
    for dz, dy in DIRECTIONS:
        @pl.when(exists(dz, dy))
        def _():
            pl.semaphore_signal(barrier, inc=1, device_id=(d + dz, l + dy), device_id_type=MESH)
        partners = partners + exists(dz, dy).astype(i32)
    own = pl.ds(2, nz)
    loads = [(im_in, Q.at[own, 0]), (mat_in, MI)]
    for c in range(3):
        loads.append((u_in.at[c], W.at[0, own, 1, c]))
        loads.append((v_in.at[c], W.at[0, own, 0, c]))
    first = len(loads)
    loads += [(k_in, KV), (mask_in, MV), (inc_in, IV), (dil_in, dil), (she_in, she), (imp_in, imp)]
    loads = [pltpu.make_async_copy(a, b, in_sem.at[i]) for i, (a, b) in enumerate(loads)]
    for load in loads:
        load.start()

    for load in loads[:first]:
        load.wait()
    for z in range(nz):
        Q[z + 2, 1] = MI[z].astype(f32)
    pl.semaphore_wait(barrier, partners)

    def remote(src, dst, ss, rs, dz, dy):
        return pltpu.make_async_remote_copy(
            src_ref=src, dst_ref=dst, send_sem=ss, recv_sem=rs,
            device_id=(d + dz, l + dy), device_id_type=MESH)

    def layers(dz):
        if dz == 0:
            return own, own
        return (pl.ds(nz, 2), pl.ds(0, 2)) if dz == 1 else (pl.ds(2, 2), pl.ds(nz + 2, 2))

    def rows_of(dy):
        return (ny - 1, ny - 2, pl.ds(0, 3)) if dy == 1 else (0, 1, pl.ds(3, 3))

    def copies(t, k, up, part="all"):
        dz, dy = DIRECTIONS[k]
        a, b = layers(dz)
        sem = 4 * k
        if dy == 0:
            pairs = [(W.at[t, a, 1], W.at[t, b, 1])]
        else:
            near_row, far_row, to = rows_of(dy)
            if dz == 0:
                early, late = (pl.ds(2, 6), pl.ds(8, 2)) if up else (pl.ds(4, 6), pl.ds(2, 2))
                spans = {"all": (early, late), "early": (early,), "late": (late,)}[part]
                pairs = []
                for span in spans:
                    pairs += [(W.at[t, span, 1, :, near_row], HW.at[t, span, 1, to]),
                              (W.at[t, span, 1, :, far_row], HW.at[t, span, 2, to])]
                sem += 2 if part == "late" else 0
            else:
                pairs = [(W.at[t, a, 1, :, near_row], HW.at[t, b, 1, to]),
                         (W.at[t, a, 1, :, far_row], HW.at[t, b, 2, to])]
        return [remote(src, dst, send_sem.at[t // 2, sem + i], recv_sem.at[t // 2, sem + i], dz, dy)
                for i, (src, dst) in enumerate(pairs)]

    def first_copies(k, part="all"):
        dz, dy = DIRECTIONS[k]
        a, b = layers(dz)
        near, far = (nz + 1, nz) if dz == 1 else (2, 3)
        to_near, to_far = (1, 0) if dz == 1 else (nz + 2, nz + 3)
        if dy == 0:
            pairs = [(W.at[0, a, 1], W.at[0, b, 1])]
            pairs.append((Q.at[a, 1], Q.at[b, 1]) if dz == 1 else (Q.at[near, 1], Q.at[to_near, 1]))
            late = [(W.at[0, near, 0], W.at[0, to_near, 0]), (Q.at[near, 0], Q.at[to_near, 0])]
        else:
            near_row, far_row, to = rows_of(dy)
            slot = 0 if dy == 1 else 2
            pairs = [(W.at[0, a, 1, :, near_row], HW.at[0, b, 1, to]),
                     (W.at[0, a, 1, :, far_row], HW.at[0, b, 2, to])]
            m, to_m = (near, to_near) if dz == -1 else (a, b)
            pairs.append((Q.at[m, 1, near_row], HQ.at[to_m, 1, slot]))
            if dy == 1:
                pairs.append((Q.at[m, 1, far_row], HQ.at[to_m, 1, 1]))
            n, to_n = (a, b) if dz == 0 else (near, to_near)
            late = [(W.at[0, n, 0, :, near_row], HW.at[0, to_n, 0, to]),
                    (Q.at[n, 0, near_row], HQ.at[to_n, 0, slot])]
        offset = len(pairs) if part == "late" else 0
        pairs = {"all": pairs + late, "early": pairs, "late": late}[part]
        return [remote(src, dst, qsend_sem.at[6 * k + offset + i], qrecv_sem.at[6 * k + offset + i], dz, dy)
                for i, (src, dst) in enumerate(pairs)]

    def b_copy(dy):
        row, to, i = (ny - 1, pl.ds(0, 3), 0) if dy == 1 else (0, pl.ds(3, 3), 1)
        return remote(BI.at[:, 0, :, row], HB.at[:, to], bsend_sem.at[i], brecv_sem.at[i], 0, dy)

    def for_all(make, backward, act, which=tuple(range(len(DIRECTIONS)))):
        for k in which:
            dz, dy = DIRECTIONS[k]
            sign = -1 if backward else 1

            @pl.when(exists(sign * dz, sign * dy))
            def _():
                for copy in make(k):
                    act(copy)

    def for_bottom(backward, act):
        for dy in (1, -1):
            @pl.when((d == nd - 1) & exists(0, -dy if backward else dy))
            def _():
                act(b_copy(dy))

    start = lambda copy: copy.start()
    for_all(first_copies, False, start, (6, 7))
    for part in ("early", "late"):
        for_all(lambda k: first_copies(k, part), False, start, (0, 1, 2, 3, 4, 5))

    for load in loads[first:]:
        load.wait()
    for r in range(rounds):
        for i in range(2):
            for c in range(3):
                BI[r, i, c] = 2.0 * MV[...].astype(f32) * IV[2 * r + i, c]
    for_bottom(False, start)

    def clear(n):
        for t in range(0, steps, 2):
            W[t, n] = jnp.zeros_like(W[t, n])
            HW[t, n] = jnp.zeros_like(HW[t, n])
        Q[n, 0] = jnp.zeros_like(Q[n, 0])
        Q[n, 1] = jnp.full_like(Q[n, 1], -1.0)
        HQ[n, 0] = jnp.zeros_like(HQ[n, 0])
        HQ[n, 1] = jnp.full_like(HQ[n, 1], -1.0)

    @pl.when(d == 0)
    def _():
        clear(0)
        clear(1)

    @pl.when(d == nd - 1)
    def _():
        clear(nz + 2)
        clear(nz + 3)

    def clear_side(rows, q_rows):
        for n in range(nz + 4):
            for t in range(0, steps, 2):
                for i in range(3):
                    HW[t, n, i, rows[0]:rows[1]] = jnp.zeros((3, nx), f32)
            HQ[n, 0, q_rows[0]:q_rows[1]] = jnp.zeros((q_rows[1] - q_rows[0], nx), f32)
            HQ[n, 1, q_rows[0]:q_rows[1]] = jnp.full((q_rows[1] - q_rows[0], nx), -1.0, f32)
        for r in range(rounds):
            HB[r, rows[0]:rows[1]] = jnp.zeros((3, nx), f32)

    @pl.when(d < nd - 1)
    def _():
        HB[...] = jnp.zeros_like(HB)

    @pl.when(l == 0)
    def _():
        clear_side((0, 3), (0, 2))

    @pl.when(l == nl - 1)
    def _():
        clear_side((3, 6), (2, 3))

    row = lax.broadcasted_iota(i32, (ny, nx), 0)
    lane = lax.broadcasted_iota(i32, (ny, nx), 1)

    def column_dofs(shape):
        j = lax.broadcasted_iota(i32, shape, 1)
        block = (j >= KB).astype(i32) + (j >= 2 * KB).astype(i32) + (j >= 3 * KB).astype(i32)
        j = j - KB * block
        bz = (j >= KL).astype(i32)
        j = j - KL * bz
        inner = j < 48
        bx_i = (j >= 24).astype(i32)
        c_i = (j - 24 * bx_i) >> 3
        y_i = j & 7
        h = j - 48
        far = (h >= 16).astype(i32)
        bx_h = (h >> 3) & 1
        r = h & 7
        s = (r >= 3).astype(i32)
        c_h = r - 3 * s
        y_h = jnp.where(r >= 6, 99, jnp.where(s == 0, -1 - far, 8 + far))
        y = jnp.where(inner, y_i, y_h)
        bx = jnp.where(inner, bx_i, bx_h)
        c = jnp.where(inner, c_i, c_h)
        return block, jnp.where(block < 3, y, 99), 12 * bz + 3 * bx + c

    block, _, dof = column_dofs((24, KP))
    i24 = lax.broadcasted_iota(i32, (24, KP), 0)
    stiff = jnp.concatenate([KV[0], KV[1]], 0)
    block48, _, _ = column_dofs((48, KP))
    for by in (0, 1):
        one_hot = (i24 == dof + 6 * by).astype(f32)
        e = jnp.dot(stiff, one_hot, precision=lax.Precision.HIGHEST, preferred_element_type=f32)
        e_hi = e.astype(bf16).astype(f32)
        E[by] = jnp.where(block48 == 2, e - e_hi, e_hi)
    _, y_col, _ = column_dofs((8, KP))
    r8 = lax.broadcasted_iota(i32, (8, KP), 0)
    y_halo = jnp.where(r8 < 3, -1, jnp.where(r8 < 6, 8, 199))

    def band(y_row, ay, picks):
        e0, e1 = picks
        delta = y_col - y_row + ay
        return jnp.where(delta == 0, e0, jnp.where(delta == 1, e1, 0.0))

    def wide(by, q):
        return jnp.broadcast_to(E[by, q:q + 1], (8, KP))

    for q in range(0, 48, 2):
        tiles = [band(r8, (p // 6) % 2, (wide(0, p), wide(1, p))) for p in (q, q + 1)]
        WM[8 * q:8 * q + 16] = jnp.concatenate(tiles, 0).astype(bf16)
    for g in range(0, 16, 2):
        tiles = []
        for p in (g, g + 1):
            picks = []
            for by in (0, 1):
                a, b, c = (wide(by, 3 * p + i) for i in range(3))
                picks.append(jnp.where((r8 == 0) | (r8 == 3), a, jnp.where((r8 == 1) | (r8 == 4), b, c)))
            tiles.append(band(y_halo, (p // 2) % 2, picks))
        WM[MO + 8 * g:MO + 8 * g + 16] = jnp.concatenate(tiles, 0).astype(bf16)

    def fields(n):
        def full(x):
            return jnp.broadcast_to(x, (ny, nx))
        mat = Q[n, 1]
        m1, m2, m8 = full(HQ[n, 1, 0:1]), full(HQ[n, 1, 1:2]), full(HQ[n, 1, 2:3])
        m7 = full(Q[n, 1, ny - 1:ny])
        before = jnp.where(row == 0, m1, pltpu.roll(mat, 1, 0))
        for ref, ay, m in ((FD, 0, mat), (FD, 1, before), (FH, 0, jnp.where(row < 3, m1, m8)),
                           (FH, 1, jnp.where(row < 3, m2, m7))):
            for f, table in ((0, dil), (1, she)):
                value = jnp.zeros((ny, nx), f32)
                for level in range(table.shape[0]):
                    value = jnp.where(m == float(level), table[level], value)
                ref[n, f, ay] = value

    def masses(n):
        low, high = HQ[n, 0, 0:1], HQ[n, 0, 2:3]
        HIM[n] = DT * jnp.where(row < 3, jnp.broadcast_to(low, (ny, nx)), jnp.broadcast_to(high, (ny, nx)))

    here = lambda copy: copy.wait_recv()
    lat_k = (6, 7)
    for_all(first_copies, True, here, lat_k)
    for_bottom(True, here)

    @pl.loop(2, nz + 2)
    def _(n):
        fields(n)
        masses(n)

    at_bottom = (d == nd - 1).astype(f32)
    imp_rows = jnp.where((row == 0) | (row == 3), imp[0], jnp.where((row == 1) | (row == 4), imp[1], imp[2]))

    def ahead(x):
        return jnp.where(lane == nx - 1, 0.0, pltpu.roll(x, nx - 1, 1))

    def behind(x):
        return jnp.where(lane == 0, 0.0, pltpu.roll(x, 1, 1))

    def operand(t, n, extended):
        tiles = [W[t, n, 1, c] for c in range(3)]
        halo = [jnp.where(row < 6, HW[t, n, 1], 0.0)]
        if extended:
            halo.append(jnp.where(row < 6, HW[t, n, 2], 0.0))
        parts = tiles + [ahead(x) for x in tiles]
        for x in halo:
            parts += [x, ahead(x)]
        if not extended:
            parts += [jnp.zeros((ny, nx), f32)] * 2
        x = jnp.concatenate(parts, 0)
        hi = x.astype(bf16)
        XH[n] = hi
        XL[n] = (x - hi.astype(f32)).astype(bf16)

    def element(e, extended):
        m = MH if extended else MO
        x = jnp.concatenate([XH[e], XH[e + 1], XL[e], XL[e + 1], XH[e], XH[e + 1],
                             jnp.zeros((KP - 3 * KB, nx), bf16)], 0)
        slot = e % 2
        PR[slot, 0:m] = jnp.dot(WM[0:m], x, preferred_element_type=f32)
        sides = []
        for az in (0, 1):
            sums = {}
            for ax in (0, 1):
                for c in range(4 if extended else 3):
                    total = None
                    for f in (0, 1):
                        for ay in (0, 1):
                            g = 8 * f + 4 * az + 2 * ay + ax
                            if c < 3:
                                at = 8 * (3 * g + c)
                                term = FD[e, f, ay] * PR[slot, at:at + 8]
                            else:
                                at = MO + 8 * g
                                term = FH[e, f, ay] * PR[slot, at:at + 8]
                            total = term if total is None else total + term
                    sums[ax, c] = total
            sides.append(sums)
        return sides

    def advance(t, r, n, before, after, extended):
        force = [after[0, c] + before[0, c] + behind(after[1, c] + before[1, c])
                 for c in range(4 if extended else 3)]
        scale = DT * Q[n, 0]
        for c in range(3):
            net = -force[c]
            v = W[t, n, 0, c]
            if n == nz + 1:
                net = net + at_bottom * imp[c] * (BI[t // 2, r, c] - v)
            v = v + scale * net
            W[t + 1, n, 0, c] = v
            W[t + 1, n, 1, c] = W[t, n, 1, c] + DT * v
        if extended:
            net = -force[3]
            v = HW[t, n, 0]
            if n == nz + 1:
                net = net + at_bottom * imp_rows * (HB[t // 2] - v)
            v = v + HIM[n] * net
            HW[t + 1, n, 1] = HW[t, n, 1] + DT * v

    def run(t, r, extended, order, nodes, low, high):
        for e in order:
            low[e], high[e] = element(e, extended)
            for n in (e, e + 1):
                if n in nodes and n in low and n - 1 in high:
                    advance(t, r, n, high[n - 1], low[n], extended)
                    nodes.remove(n)

    def follow_tile(t, n):
        HW[t, n, 0] = (HW[t, n, 1] - HW[t - 1, n, 1]) * (1.0 / DT)

    def follow_layer(t, n):
        for c in range(3):
            W[t, n, 0, c] = (W[t, n, 1, c] - W[t - 1, n, 1, c]) * (1.0 / DT)

    top = nz + 2

    @pl.loop(0, rounds)
    def _(i):
        t = 2 * i

        sides = {
            "low": ((0, 2, 3), (1, 0), 1, (1, 0)),
            "high": ((1, 4, 5), (top, top + 1), top, (top - 1, top)),
        }

        def finish_side(name, up, low, high, nodes):
            which, layers_in, edge, order = sides[name]

            @pl.when(i == 0)
            def _():
                for_all(lambda k: first_copies(k, "early"), True, here, which)
                for n in (0, 1) if name == "low" else (top,):
                    fields(n)

            @pl.when(i > 0)
            def _():
                for_all(lambda k: copies(t, k, up), True, here, which)
                follow_tile(t, edge)
                follow_layer(t, edge)

            for n in layers_in:
                operand(t, n, True)
            nodes.remove(edge)
            run(t, 0, True, order, nodes, low, high)

            @pl.when(i == 0)
            def _():
                for_all(lambda k: first_copies(k, "late"), True, here, which)
                masses(edge)

            advance(t, 0, edge, high[edge - 1], low[edge], True)

        def work(up):
            near, far = ("low", "high") if up else ("high", "low")
            turn = (lambda x: list(x)) if up else (lambda x: list(x)[::-1])
            own_layers = turn(range(2, top))
            own_elements = turn(range(2, top - 1))
            layers_b = turn(range(1, top + 1))
            elements_b = turn(range(1, top))
            low_a, high_a, nodes_a = {}, {}, set(range(1, top + 1))
            low_b, high_b, nodes_b = {}, {}, set(range(2, top))

            def send(which, part="all"):
                @pl.when(i < rounds - 1)
                def _():
                    for_all(lambda k: copies(t + 2, k, up, part), False, start, which)

            def lat_rows(part, ns):
                @pl.when(i > 0)
                def _():
                    for_all(lambda k: copies(t, k, up, part), True, here, lat_k)
                    for n in ns:
                        follow_tile(t, n)

            def step_a(ns, es):
                for n in ns:
                    operand(t, n, True)
                run(t, 0, True, es, nodes_a, low_a, high_a)

            def step_b(ns, es):
                for n in ns:
                    operand(t + 1, n, False)
                run(t + 1, 1, False, es, nodes_b, low_b, high_b)

            def side_k(name):
                return (1, 4, 5) if name == "low" else (0, 2, 3)

            lat_rows("early", own_layers[:6])
            step_a(own_layers[:6], own_elements[:5])
            finish_side(near, up, low_a, high_a, nodes_a)
            step_b(layers_b[:6], elements_b[:5])
            send(side_k(near))
            lat_rows("late", own_layers[6:])
            step_a(own_layers[6:], own_elements[5:])
            step_b(layers_b[6:8], elements_b[5:7])
            send(lat_k, "early")
            finish_side(far, up, low_a, high_a, nodes_a)
            step_b(layers_b[8:], elements_b[7:])
            send(side_k(far))
            send(lat_k, "late")

        @pl.when(d < nd // 2)
        def _():
            work(True)

        @pl.when(d >= nd // 2)
        def _():
            work(False)

    for z in range(nz):
        for c in range(3):
            u_out[c, z] = W[steps, z + 2, 1, c]
            v_out[c, z] = W[steps, z + 2, 0, c]

    done = lambda copy: copy.wait_send()
    for_all(first_copies, False, done)
    for_bottom(False, done)

    @pl.loop(1, rounds)
    def _(i):
        @pl.when(d < nd // 2)
        def _():
            for_all(lambda k: copies(2 * i, k, True), False, done)

        @pl.when(d >= nd // 2)
        def _():
            for_all(lambda k: copies(2 * i, k, False), False, done)


def put_out(u, v, u_hbm, v_hbm, sem):
    copies = [pltpu.make_async_copy(a.at[c], b.at[c], sem.at[3 * i + c])
              for i, (a, b) in enumerate(((u, u_hbm), (v, v_hbm))) for c in range(3)]
    for copy in copies:
        copy.start()
    for copy in copies:
        copy.wait()


def per_device(nd, nl, displacement, velocity, inverse_mass, material, dilation_table, shear_table,
               stiffness_pair, impedance, bedrock_mask, incident):
    _, nz, ny, nx = displacement.shape
    steps = incident.shape[0]
    rounds = steps // 2
    nmat = dilation_table.shape[0]
    vmem = pl.BlockSpec(memory_space=pltpu.VMEM)
    hbm = pl.BlockSpec(memory_space=pltpu.MemorySpace.HBM)
    ext = nz + 4
    dma = pltpu.SemaphoreType.DMA
    state = pl.pallas_call(
        functools.partial(kernel, nd, nl),
        out_shape=[jax.ShapeDtypeStruct(displacement.shape, f32)] * 2,
        in_specs=[hbm] * 10,
        out_specs=[vmem, vmem],
        scratch_shapes=[
            pltpu.VMEM((steps + 1, ext, 2, 3, ny, nx), f32),
            pltpu.VMEM((steps, ext, 3, ny, nx), f32),
            pltpu.VMEM((ext, 2, ny, nx), f32),
            pltpu.VMEM((ext, 2, ny, nx), f32),
            pltpu.VMEM((rounds, 2, 3, ny, nx), f32),
            pltpu.VMEM((rounds, ny, nx), f32),
            pltpu.VMEM((nz, ny, nx), i32),
            pltpu.VMEM(stiffness_pair.shape, f32),
            pltpu.VMEM((ny, nx), i32),
            pltpu.VMEM((steps, 3, ny, nx), f32),
            pltpu.VMEM((2, 48, KP), f32),
            pltpu.VMEM((MH, KP), bf16),
            pltpu.VMEM((ext, KL, nx), bf16),
            pltpu.VMEM((ext, KL, nx), bf16),
            pltpu.VMEM((2, MH, nx), f32),
            pltpu.VMEM((ext, 2, 2, ny, nx), f32),
            pltpu.VMEM((ext, 2, 2, ny, nx), f32),
            pltpu.VMEM((ext, ny, nx), f32),
            pltpu.SMEM((nmat,), f32),
            pltpu.SMEM((nmat,), f32),
            pltpu.SMEM((3,), f32),
            dma((14,)),
            dma((rounds, 32)),
            dma((rounds, 32)),
            dma((48,)),
            dma((48,)),
            dma((2,)),
            dma((2,)),
        ],
        compiler_params=pltpu.CompilerParams(
            collective_id=0, has_side_effects=True, vmem_limit_bytes=48 * 1024 * 1024),
    )(*(pltpu.with_memory_space_constraint(x, pltpu.MemorySpace.HBM) for x in (
        displacement, velocity, inverse_mass, material, dilation_table, shear_table,
        stiffness_pair, impedance, bedrock_mask, incident)))
    return pl.pallas_call(
        put_out,
        out_shape=[jax.ShapeDtypeStruct(displacement.shape, f32)] * 2,
        in_specs=[vmem, vmem],
        out_specs=[pl.BlockSpec(memory_space=pltpu.MemorySpace.HBM)] * 2,
        scratch_shapes=[dma((6,))],
        compiler_params=pltpu.CompilerParams(vmem_limit_bytes=2 * 1024 * 1024),
    )(*state)


def solution(mesh):
    in_specs = (
        P(None, "depth", "lat", None),
        P(None, "depth", "lat", None),
        P("depth", "lat", None),
        P("depth", "lat", None),
        P(),
        P(),
        P(),
        P(),
        P("lat", None),
        P(None, None, "lat", None),
    )
    out_specs = (P(None, "depth", "lat", None), P(None, "depth", "lat", None))
    return jax.shard_map(
        functools.partial(per_device, mesh.shape["depth"], mesh.shape["lat"]),
        mesh=mesh, in_specs=in_specs, out_specs=out_specs, check_vma=False)
```

```python
import functools

import jax
import jax.numpy as jnp
from jax import lax
from jax.experimental import pallas as pl
from jax.experimental.pallas import tpu as pltpu
from jax.sharding import PartitionSpec as P

MESH = pl.DeviceIdType.MESH
DT = 0.1
f32, bf16, i32 = jnp.float32, jnp.bfloat16, jnp.int32
DIRECTIONS = ((1, 0), (-1, 0), (1, 1), (1, -1), (-1, 1), (-1, -1), (0, 1), (0, -1))

KL = 80
KB = 2 * KL
KP = 512
MH = 512


def own_row(g):
    f, az, rest = g // 8, (g // 4) % 2, g % 4
    return (64, 256)[az] + 96 * f + 24 * rest


def halo_row(g):
    f, az, rest = g // 8, (g // 4) % 2, g % 4
    return (0, 448)[az] + 32 * f + 8 * rest


def kernel(
    nd, nl,
    u_in, v_in, im_in, mat_in, dil_in, she_in, k_in, imp_in, mask_in, inc_in,
    u_out, v_out,
    W, HW, Q, HQ, BI, HB, MI, KV, MV, IV, E, WM, XH, XL, PR, FD, FH, HIM,
    dil, she, imp,
    in_sem, send_sem, recv_sem, qsend_sem, qrecv_sem, bsend_sem, brecv_sem,
):
    steps = inc_in.shape[0]
    rounds = steps // 2
    nz, ny, nx = im_in.shape
    d = lax.axis_index("depth")
    l = lax.axis_index("lat")

    def exists(dz, dy):
        return ((d + dz >= 0) & (d + dz < nd)) & ((l + dy >= 0) & (l + dy < nl))

    barrier = pltpu.get_barrier_semaphore()
    partners = 0
    for dz, dy in DIRECTIONS:
        @pl.when(exists(dz, dy))
        def _():
            pl.semaphore_signal(barrier, inc=1, device_id=(d + dz, l + dy), device_id_type=MESH)
        partners = partners + exists(dz, dy).astype(i32)
    own = pl.ds(2, nz)
    loads = [(im_in, Q.at[own, 0]), (mat_in, MI)]
    for c in range(3):
        loads.append((u_in.at[c], W.at[0, own, 1, c]))
        loads.append((v_in.at[c], W.at[0, own, 0, c]))
    first = len(loads)
    loads += [(k_in, KV), (mask_in, MV), (inc_in, IV), (dil_in, dil), (she_in, she), (imp_in, imp)]
    loads = [pltpu.make_async_copy(a, b, in_sem.at[i]) for i, (a, b) in enumerate(loads)]
    for load in loads:
        load.start()

    for load in loads[:first]:
        load.wait()
    for z in range(nz):
        Q[z + 2, 1] = MI[z].astype(f32)
    pl.semaphore_wait(barrier, partners)

    def remote(src, dst, ss, rs, dz, dy):
        return pltpu.make_async_remote_copy(
            src_ref=src, dst_ref=dst, send_sem=ss, recv_sem=rs,
            device_id=(d + dz, l + dy), device_id_type=MESH)

    def layers(dz):
        if dz == 0:
            return own, own
        return (pl.ds(nz, 2), pl.ds(0, 2)) if dz == 1 else (pl.ds(2, 2), pl.ds(nz + 2, 2))

    def rows_of(dy):
        return (ny - 1, ny - 2, pl.ds(0, 3)) if dy == 1 else (0, 1, pl.ds(3, 3))

    def copies(t, k, up, part="all"):
        dz, dy = DIRECTIONS[k]
        a, b = layers(dz)
        sem = 4 * k
        if dy == 0:
            pairs = [(W.at[t, a, 1], W.at[t, b, 1])]
        else:
            near_row, far_row, to = rows_of(dy)
            if dz == 0:
                early, late = (pl.ds(2, 6), pl.ds(8, 2)) if up else (pl.ds(4, 6), pl.ds(2, 2))
                spans = {"all": (early, late), "early": (early,), "late": (late,)}[part]
                pairs = []
                for span in spans:
                    pairs += [(W.at[t, span, 1, :, near_row], HW.at[t, span, 1, to]),
                              (W.at[t, span, 1, :, far_row], HW.at[t, span, 2, to])]
                sem += 2 if part == "late" else 0
            else:
                pairs = [(W.at[t, a, 1, :, near_row], HW.at[t, b, 1, to]),
                         (W.at[t, a, 1, :, far_row], HW.at[t, b, 2, to])]
        return [remote(src, dst, send_sem.at[t // 2, sem + i], recv_sem.at[t // 2, sem + i], dz, dy)
                for i, (src, dst) in enumerate(pairs)]

    def first_copies(k, part="all"):
        dz, dy = DIRECTIONS[k]
        a, b = layers(dz)
        near, far = (nz + 1, nz) if dz == 1 else (2, 3)
        to_near, to_far = (1, 0) if dz == 1 else (nz + 2, nz + 3)
        if dy == 0:
            pairs = [(W.at[0, a, 1], W.at[0, b, 1])]
            pairs.append((Q.at[a, 1], Q.at[b, 1]) if dz == 1 else (Q.at[near, 1], Q.at[to_near, 1]))
            late = [(W.at[0, near, 0], W.at[0, to_near, 0]), (Q.at[near, 0], Q.at[to_near, 0])]
        else:
            near_row, far_row, to = rows_of(dy)
            slot = 0 if dy == 1 else 2
            pairs = [(W.at[0, a, 1, :, near_row], HW.at[0, b, 1, to]),
                     (W.at[0, a, 1, :, far_row], HW.at[0, b, 2, to])]
            m, to_m = (near, to_near) if dz == -1 else (a, b)
            pairs.append((Q.at[m, 1, near_row], HQ.at[to_m, 1, slot]))
            if dy == 1:
                pairs.append((Q.at[m, 1, far_row], HQ.at[to_m, 1, 1]))
            n, to_n = (a, b) if dz == 0 else (near, to_near)
            late = [(W.at[0, n, 0, :, near_row], HW.at[0, to_n, 0, to]),
                    (Q.at[n, 0, near_row], HQ.at[to_n, 0, slot])]
        offset = len(pairs) if part == "late" else 0
        pairs = {"all": pairs + late, "early": pairs, "late": late}[part]
        return [remote(src, dst, qsend_sem.at[6 * k + offset + i], qrecv_sem.at[6 * k + offset + i], dz, dy)
                for i, (src, dst) in enumerate(pairs)]

    def b_copy(dy):
        row, to, i = (ny - 1, pl.ds(0, 3), 0) if dy == 1 else (0, pl.ds(3, 3), 1)
        return remote(BI.at[:, 0, :, row], HB.at[:, to], bsend_sem.at[i], brecv_sem.at[i], 0, dy)

    def for_all(make, backward, act, which=tuple(range(len(DIRECTIONS)))):
        for k in which:
            dz, dy = DIRECTIONS[k]
            sign = -1 if backward else 1

            @pl.when(exists(sign * dz, sign * dy))
            def _():
                for copy in make(k):
                    act(copy)

    def for_bottom(backward, act):
        for dy in (1, -1):
            @pl.when((d == nd - 1) & exists(0, -dy if backward else dy))
            def _():
                act(b_copy(dy))

    start = lambda copy: copy.start()
    for_all(first_copies, False, start, (6, 7))
    for part in ("early", "late"):
        for_all(lambda k: first_copies(k, part), False, start, (0, 1, 2, 3, 4, 5))

    for load in loads[first:]:
        load.wait()
    for r in range(rounds):
        for i in range(2):
            for c in range(3):
                BI[r, i, c] = 2.0 * MV[...].astype(f32) * IV[2 * r + i, c]
    for_bottom(False, start)

    def clear(n):
        for t in range(0, steps, 2):
            W[t, n] = jnp.zeros_like(W[t, n])
            HW[t, n] = jnp.zeros_like(HW[t, n])
        Q[n, 0] = jnp.zeros_like(Q[n, 0])
        Q[n, 1] = jnp.full_like(Q[n, 1], -1.0)
        HQ[n, 0] = jnp.zeros_like(HQ[n, 0])
        HQ[n, 1] = jnp.full_like(HQ[n, 1], -1.0)

    @pl.when(d == 0)
    def _():
        clear(0)
        clear(1)

    @pl.when(d == nd - 1)
    def _():
        clear(nz + 2)
        clear(nz + 3)

    def clear_side(rows, q_rows):
        for n in range(nz + 4):
            for t in range(0, steps, 2):
                for i in range(3):
                    HW[t, n, i, rows[0]:rows[1]] = jnp.zeros((3, nx), f32)
            HQ[n, 0, q_rows[0]:q_rows[1]] = jnp.zeros((q_rows[1] - q_rows[0], nx), f32)
            HQ[n, 1, q_rows[0]:q_rows[1]] = jnp.full((q_rows[1] - q_rows[0], nx), -1.0, f32)
        for r in range(rounds):
            HB[r, rows[0]:rows[1]] = jnp.zeros((3, nx), f32)

    @pl.when(d < nd - 1)
    def _():
        HB[...] = jnp.zeros_like(HB)

    @pl.when(l == 0)
    def _():
        clear_side((0, 3), (0, 2))

    @pl.when(l == nl - 1)
    def _():
        clear_side((3, 6), (2, 3))

    row = lax.broadcasted_iota(i32, (ny, nx), 0)
    lane = lax.broadcasted_iota(i32, (ny, nx), 1)

    def column_dofs(shape):
        j = lax.broadcasted_iota(i32, shape, 1)
        block = (j >= KB).astype(i32) + (j >= 2 * KB).astype(i32) + (j >= 3 * KB).astype(i32)
        j = j - KB * block
        bz = (j >= KL).astype(i32)
        j = j - KL * bz
        inner = j < 48
        bx_i = (j >= 24).astype(i32)
        c_i = (j - 24 * bx_i) >> 3
        y_i = j & 7
        h = j - 48
        far = (h >= 16).astype(i32)
        bx_h = (h >> 3) & 1
        r = h & 7
        s = (r >= 3).astype(i32)
        c_h = r - 3 * s
        y_h = jnp.where(r >= 6, 99, jnp.where(s == 0, -1 - far, 8 + far))
        y = jnp.where(inner, y_i, y_h)
        bx = jnp.where(inner, bx_i, bx_h)
        c = jnp.where(inner, c_i, c_h)
        return block, jnp.where(block < 3, y, 99), 12 * bz + 3 * bx + c

    block, _, dof = column_dofs((24, KP))
    i24 = lax.broadcasted_iota(i32, (24, KP), 0)
    stiff = jnp.concatenate([KV[0], KV[1]], 0)
    block48, _, _ = column_dofs((48, KP))
    for by in (0, 1):
        one_hot = (i24 == dof + 6 * by).astype(f32)
        e = jnp.dot(stiff, one_hot, precision=lax.Precision.HIGHEST, preferred_element_type=f32)
        e_hi = e.astype(bf16).astype(f32)
        E[by] = jnp.where(block48 == 2, e - e_hi, e_hi)
    _, y_col, _ = column_dofs((8, KP))
    r8 = lax.broadcasted_iota(i32, (8, KP), 0)
    y_halo = jnp.where(r8 < 3, -1, jnp.where(r8 < 6, 8, 199))

    def band(y_row, ay, picks):
        e0, e1 = picks
        delta = y_col - y_row + ay
        return jnp.where(delta == 0, e0, jnp.where(delta == 1, e1, 0.0))

    def wide(by, q):
        return jnp.broadcast_to(E[by, q:q + 1], (8, KP))

    for q in range(0, 48, 2):
        tiles = [band(r8, (p // 6) % 2, (wide(0, p), wide(1, p))) for p in (q, q + 1)]
        at = [own_row(p // 3) + 8 * (p % 3) for p in (q, q + 1)]
        assert at[1] == at[0] + 8 and at[0] % 16 == 0
        WM[at[0]:at[0] + 16] = jnp.concatenate(tiles, 0).astype(bf16)
    for g in range(0, 16, 2):
        tiles = []
        for p in (g, g + 1):
            picks = []
            for by in (0, 1):
                a, b, c = (wide(by, 3 * p + i) for i in range(3))
                picks.append(jnp.where((r8 == 0) | (r8 == 3), a, jnp.where((r8 == 1) | (r8 == 4), b, c)))
            tiles.append(band(y_halo, (p // 2) % 2, picks))
        WM[halo_row(g):halo_row(g) + 16] = jnp.concatenate(tiles, 0).astype(bf16)

    def fields(n):
        def full(x):
            return jnp.broadcast_to(x, (ny, nx))
        mat = Q[n, 1]
        m1, m2, m8 = full(HQ[n, 1, 0:1]), full(HQ[n, 1, 1:2]), full(HQ[n, 1, 2:3])
        m7 = full(Q[n, 1, ny - 1:ny])
        before = jnp.where(row == 0, m1, pltpu.roll(mat, 1, 0))
        for ref, ay, m in ((FD, 0, mat), (FD, 1, before), (FH, 0, jnp.where(row < 3, m1, m8)),
                           (FH, 1, jnp.where(row < 3, m2, m7))):
            for f, table in ((0, dil), (1, she)):
                value = jnp.zeros((ny, nx), f32)
                for level in range(table.shape[0]):
                    value = jnp.where(m == float(level), table[level], value)
                ref[n, f, ay] = value

    def masses(n):
        low, high = HQ[n, 0, 0:1], HQ[n, 0, 2:3]
        HIM[n] = DT * jnp.where(row < 3, jnp.broadcast_to(low, (ny, nx)), jnp.broadcast_to(high, (ny, nx)))

    here = lambda copy: copy.wait_recv()
    lat_k = (6, 7)
    for_all(first_copies, True, here, lat_k)
    for_bottom(True, here)

    @pl.loop(2, nz + 2)
    def _(n):
        fields(n)
        masses(n)

    at_bottom = (d == nd - 1).astype(f32)
    imp_rows = jnp.where((row == 0) | (row == 3), imp[0], jnp.where((row == 1) | (row == 4), imp[1], imp[2]))

    def ahead(x):
        return jnp.where(lane == nx - 1, 0.0, pltpu.roll(x, nx - 1, 1))

    def behind(x):
        return jnp.where(lane == 0, 0.0, pltpu.roll(x, 1, 1))

    def operand(t, n, extended):
        tiles = [W[t, n, 1, c] for c in range(3)]
        halo = [jnp.where(row < 6, HW[t, n, 1], 0.0)]
        if extended:
            halo.append(jnp.where(row < 6, HW[t, n, 2], 0.0))
        parts = tiles + [ahead(x) for x in tiles]
        for x in halo:
            parts += [x, ahead(x)]
        if not extended:
            parts += [jnp.zeros((ny, nx), f32)] * 2
        x = jnp.concatenate(parts, 0)
        hi = x.astype(bf16)
        XH[n] = hi
        XL[n] = (x - hi.astype(f32)).astype(bf16)

    def element(e, extended, which):
        a = (0 if extended else 64) if 0 in which else 256
        b = (MH if extended else 448) if 1 in which else 256
        x = jnp.concatenate([XH[e], XH[e + 1], XL[e], XL[e + 1], XH[e], XH[e + 1],
                             jnp.zeros((KP - 3 * KB, nx), bf16)], 0)
        slot = e % 2
        PR[slot, a:b] = jnp.dot(WM[a:b], x, preferred_element_type=f32)
        sides = {}
        for az in which:
            sums = {}
            for ax in (0, 1):
                for c in range(4 if extended else 3):
                    total = None
                    for f in (0, 1):
                        for ay in (0, 1):
                            g = 8 * f + 4 * az + 2 * ay + ax
                            if c < 3:
                                at = own_row(g) + 8 * c
                                term = FD[e, f, ay] * PR[slot, at:at + 8]
                            else:
                                at = halo_row(g)
                                term = FH[e, f, ay] * PR[slot, at:at + 8]
                            total = term if total is None else total + term
                    sums[ax, c] = total
            sides[az] = sums
        return sides

    def advance(t, r, n, before, after, extended):
        force = [after[0, c] + before[0, c] + behind(after[1, c] + before[1, c])
                 for c in range(4 if extended else 3)]
        scale = DT * Q[n, 0]
        for c in range(3):
            net = -force[c]
            v = W[t, n, 0, c]
            if n == nz + 1:
                net = net + at_bottom * imp[c] * (BI[t // 2, r, c] - v)
            v = v + scale * net
            W[t + 1, n, 0, c] = v
            W[t + 1, n, 1, c] = W[t, n, 1, c] + DT * v
        if extended:
            net = -force[3]
            v = HW[t, n, 0]
            if n == nz + 1:
                net = net + at_bottom * imp_rows * (HB[t // 2] - v)
            v = v + HIM[n] * net
            HW[t + 1, n, 1] = HW[t, n, 1] + DT * v

    def run(t, r, extended, order, nodes, low, high):
        for e in order:
            first_e, last_e = (0, nz + 2) if extended else (1, nz + 1)
            which = (1,) if e == first_e else (0,) if e == last_e else (0, 1)
            sides = element(e, extended, which)
            if 0 in which:
                low[e] = sides[0]
            if 1 in which:
                high[e] = sides[1]
            for n in (e, e + 1):
                if n in nodes and n in low and n - 1 in high:
                    advance(t, r, n, high[n - 1], low[n], extended)
                    nodes.remove(n)

    def follow_tile(t, n):
        HW[t, n, 0] = (HW[t, n, 1] - HW[t - 1, n, 1]) * (1.0 / DT)

    def follow_layer(t, n):
        for c in range(3):
            W[t, n, 0, c] = (W[t, n, 1, c] - W[t - 1, n, 1, c]) * (1.0 / DT)

    top = nz + 2

    @pl.loop(0, rounds)
    def _(i):
        t = 2 * i

        sides = {
            "low": ((0, 2, 3), (1, 0), 1, (1, 0)),
            "high": ((1, 4, 5), (top, top + 1), top, (top - 1, top)),
        }

        def finish_side(name, up, low, high, nodes):
            which, layers_in, edge, order = sides[name]

            @pl.when(i == 0)
            def _():
                for_all(first_copies, True, here, which)
                for n in (0, 1) if name == "low" else (top,):
                    fields(n)
                masses(edge)

            @pl.when(i > 0)
            def _():
                for_all(lambda k: copies(t, k, up), True, here, which)
                follow_tile(t, edge)
                follow_layer(t, edge)

            for n in layers_in:
                operand(t, n, True)
            run(t, 0, True, order, nodes, low, high)

        def work(up):
            near, far = ("low", "high") if up else ("high", "low")
            turn = (lambda x: list(x)) if up else (lambda x: list(x)[::-1])
            own_layers = turn(range(2, top))
            own_elements = turn(range(2, top - 1))
            layers_b = turn(range(1, top + 1))
            elements_b = turn(range(1, top))
            low_a, high_a, nodes_a = {}, {}, set(range(1, top + 1))
            low_b, high_b, nodes_b = {}, {}, set(range(2, top))

            def send(which, part="all"):
                @pl.when(i < rounds - 1)
                def _():
                    for_all(lambda k: copies(t + 2, k, up, part), False, start, which)

            def lat_rows(part, ns):
                @pl.when(i > 0)
                def _():
                    for_all(lambda k: copies(t, k, up, part), True, here, lat_k)
                    for n in ns:
                        follow_tile(t, n)

            def step_a(ns, es):
                for n in ns:
                    operand(t, n, True)
                run(t, 0, True, es, nodes_a, low_a, high_a)

            def step_b(ns, es):
                for n in ns:
                    operand(t + 1, n, False)
                run(t + 1, 1, False, es, nodes_b, low_b, high_b)

            def side_k(name):
                return (1, 4, 5) if name == "low" else (0, 2, 3)

            lat_rows("early", own_layers[:6])
            step_a(own_layers[:6], own_elements[:5])
            finish_side(near, up, low_a, high_a, nodes_a)
            step_b(layers_b[:6], elements_b[:5])
            send(side_k(near))
            lat_rows("late", own_layers[6:])
            step_a(own_layers[6:], own_elements[5:])
            step_b(layers_b[6:8], elements_b[5:7])
            send(lat_k, "early")
            finish_side(far, up, low_a, high_a, nodes_a)
            step_b(layers_b[8:], elements_b[7:])
            send(side_k(far))
            send(lat_k, "late")

        @pl.when(d < nd // 2)
        def _():
            work(True)

        @pl.when(d >= nd // 2)
        def _():
            work(False)

    for z in range(nz):
        for c in range(3):
            u_out[c, z] = W[steps, z + 2, 1, c]
            v_out[c, z] = W[steps, z + 2, 0, c]

    done = lambda copy: copy.wait_send()
    for_all(first_copies, False, done)
    for_bottom(False, done)

    @pl.loop(1, rounds)
    def _(i):
        @pl.when(d < nd // 2)
        def _():
            for_all(lambda k: copies(2 * i, k, True), False, done)

        @pl.when(d >= nd // 2)
        def _():
            for_all(lambda k: copies(2 * i, k, False), False, done)


def put_out(u, v, u_hbm, v_hbm, sem):
    copies = [pltpu.make_async_copy(a.at[c], b.at[c], sem.at[3 * i + c])
              for i, (a, b) in enumerate(((u, u_hbm), (v, v_hbm))) for c in range(3)]
    for copy in copies:
        copy.start()
    for copy in copies:
        copy.wait()


def per_device(nd, nl, displacement, velocity, inverse_mass, material, dilation_table, shear_table,
               stiffness_pair, impedance, bedrock_mask, incident):
    _, nz, ny, nx = displacement.shape
    steps = incident.shape[0]
    rounds = steps // 2
    nmat = dilation_table.shape[0]
    vmem = pl.BlockSpec(memory_space=pltpu.VMEM)
    hbm = pl.BlockSpec(memory_space=pltpu.MemorySpace.HBM)
    ext = nz + 4
    dma = pltpu.SemaphoreType.DMA
    state = pl.pallas_call(
        functools.partial(kernel, nd, nl),
        out_shape=[jax.ShapeDtypeStruct(displacement.shape, f32)] * 2,
        in_specs=[hbm] * 10,
        out_specs=[vmem, vmem],
        scratch_shapes=[
            pltpu.VMEM((steps + 1, ext, 2, 3, ny, nx), f32),
            pltpu.VMEM((steps, ext, 3, ny, nx), f32),
            pltpu.VMEM((ext, 2, ny, nx), f32),
            pltpu.VMEM((ext, 2, ny, nx), f32),
            pltpu.VMEM((rounds, 2, 3, ny, nx), f32),
            pltpu.VMEM((rounds, ny, nx), f32),
            pltpu.VMEM((nz, ny, nx), i32),
            pltpu.VMEM(stiffness_pair.shape, f32),
            pltpu.VMEM((ny, nx), i32),
            pltpu.VMEM((steps, 3, ny, nx), f32),
            pltpu.VMEM((2, 48, KP), f32),
            pltpu.VMEM((MH, KP), bf16),
            pltpu.VMEM((ext, KL, nx), bf16),
            pltpu.VMEM((ext, KL, nx), bf16),
            pltpu.VMEM((2, MH, nx), f32),
            pltpu.VMEM((ext, 2, 2, ny, nx), f32),
            pltpu.VMEM((ext, 2, 2, ny, nx), f32),
            pltpu.VMEM((ext, ny, nx), f32),
            pltpu.SMEM((nmat,), f32),
            pltpu.SMEM((nmat,), f32),
            pltpu.SMEM((3,), f32),
            dma((14,)),
            dma((rounds, 32)),
            dma((rounds, 32)),
            dma((48,)),
            dma((48,)),
            dma((2,)),
            dma((2,)),
        ],
        compiler_params=pltpu.CompilerParams(
            collective_id=0, has_side_effects=True, vmem_limit_bytes=48 * 1024 * 1024),
    )(*(pltpu.with_memory_space_constraint(x, pltpu.MemorySpace.HBM) for x in (
        displacement, velocity, inverse_mass, material, dilation_table, shear_table,
        stiffness_pair, impedance, bedrock_mask, incident)))
    return pl.pallas_call(
        put_out,
        out_shape=[jax.ShapeDtypeStruct(displacement.shape, f32)] * 2,
        in_specs=[vmem, vmem],
        out_specs=[pl.BlockSpec(memory_space=pltpu.MemorySpace.HBM)] * 2,
        scratch_shapes=[dma((6,))],
        compiler_params=pltpu.CompilerParams(vmem_limit_bytes=2 * 1024 * 1024),
    )(*state)


def solution(mesh):
    in_specs = (
        P(None, "depth", "lat", None),
        P(None, "depth", "lat", None),
        P("depth", "lat", None),
        P("depth", "lat", None),
        P(),
        P(),
        P(),
        P(),
        P("lat", None),
        P(None, None, "lat", None),
    )
    out_specs = (P(None, "depth", "lat", None), P(None, "depth", "lat", None))
    return jax.shard_map(
        functools.partial(per_device, mesh.shape["depth"], mesh.shape["lat"]),
        mesh=mesh, in_specs=in_specs, out_specs=out_specs, check_vma=False)
```

```python
import functools

import jax
import jax.numpy as jnp
from jax import lax
from jax.experimental import pallas as pl
from jax.experimental.pallas import tpu as pltpu
from jax.sharding import PartitionSpec as P

MESH = pl.DeviceIdType.MESH
DT = 0.1
f32, bf16, i32 = jnp.float32, jnp.bfloat16, jnp.int32
DIRECTIONS = ((1, 0), (-1, 0), (1, 1), (1, -1), (-1, 1), (-1, -1), (0, 1), (0, -1))

KL = 80
KB = 2 * KL
KP = 512
MH = 512


def own_row(g):
    f, az, rest = g // 8, (g // 4) % 2, g % 4
    return (64, 256)[az] + 96 * f + 24 * rest


def halo_row(g):
    f, az, rest = g // 8, (g // 4) % 2, g % 4
    return (0, 448)[az] + 32 * f + 8 * rest


def kernel(
    nd, nl,
    u_in, v_in, im_in, mat_in, dil_in, she_in, k_in, imp_in, mask_in, inc_in,
    u_out, v_out,
    W, HW, Q, HQ, BI, HB, MI, KV, MV, IV, E, WM, XH, XL, PR, FD, FH, HIM,
    dil, she, imp,
    in_sem, send_sem, recv_sem, qsend_sem, qrecv_sem, bsend_sem, brecv_sem,
):
    steps = inc_in.shape[0]
    rounds = steps // 2
    nz, ny, nx = im_in.shape
    d = lax.axis_index("depth")
    l = lax.axis_index("lat")

    def exists(dz, dy):
        return ((d + dz >= 0) & (d + dz < nd)) & ((l + dy >= 0) & (l + dy < nl))

    barrier = pltpu.get_barrier_semaphore()
    partners = 0
    for dz, dy in DIRECTIONS:
        @pl.when(exists(dz, dy))
        def _():
            pl.semaphore_signal(barrier, inc=1, device_id=(d + dz, l + dy), device_id_type=MESH)
        partners = partners + exists(dz, dy).astype(i32)
    own = pl.ds(2, nz)
    loads = [(im_in, Q.at[own, 0]), (mat_in, MI)]
    for c in range(3):
        loads.append((u_in.at[c], W.at[0, own, 1, c]))
        loads.append((v_in.at[c], W.at[0, own, 0, c]))
    first = len(loads)
    loads += [(k_in, KV), (mask_in, MV), (inc_in, IV), (dil_in, dil), (she_in, she), (imp_in, imp)]
    loads = [pltpu.make_async_copy(a, b, in_sem.at[i]) for i, (a, b) in enumerate(loads)]
    for load in loads:
        load.start()

    for load in loads[:first]:
        load.wait()
    for z in range(nz):
        Q[z + 2, 1] = MI[z].astype(f32)
    pl.semaphore_wait(barrier, partners)

    def remote(src, dst, ss, rs, dz, dy):
        return pltpu.make_async_remote_copy(
            src_ref=src, dst_ref=dst, send_sem=ss, recv_sem=rs,
            device_id=(d + dz, l + dy), device_id_type=MESH)

    def layers(dz):
        if dz == 0:
            return own, own
        return (pl.ds(nz, 2), pl.ds(0, 2)) if dz == 1 else (pl.ds(2, 2), pl.ds(nz + 2, 2))

    def rows_of(dy):
        return (ny - 1, ny - 2, pl.ds(0, 3)) if dy == 1 else (0, 1, pl.ds(3, 3))

    def copies(t, k, up, part="all"):
        dz, dy = DIRECTIONS[k]
        a, b = layers(dz)
        sem = 4 * k
        if dy == 0:
            pairs = [(W.at[t, a, 1], W.at[t, b, 1])]
        else:
            near_row, far_row, to = rows_of(dy)
            if dz == 0:
                early, late = (pl.ds(2, 6), pl.ds(8, 2)) if up else (pl.ds(4, 6), pl.ds(2, 2))
                spans = {"all": (early, late), "early": (early,), "late": (late,)}[part]
                pairs = []
                for span in spans:
                    pairs += [(W.at[t, span, 1, :, near_row], HW.at[t, span, 1, to]),
                              (W.at[t, span, 1, :, far_row], HW.at[t, span, 2, to])]
                sem += 2 if part == "late" else 0
            else:
                pairs = [(W.at[t, a, 1, :, near_row], HW.at[t, b, 1, to]),
                         (W.at[t, a, 1, :, far_row], HW.at[t, b, 2, to])]
        return [remote(src, dst, send_sem.at[t // 2, sem + i], recv_sem.at[t // 2, sem + i], dz, dy)
                for i, (src, dst) in enumerate(pairs)]

    def first_copies(k, part="all"):
        dz, dy = DIRECTIONS[k]
        a, b = layers(dz)
        near, far = (nz + 1, nz) if dz == 1 else (2, 3)
        to_near, to_far = (1, 0) if dz == 1 else (nz + 2, nz + 3)
        if dy == 0:
            pairs = [(W.at[0, a, 1], W.at[0, b, 1])]
            pairs.append((Q.at[a, 1], Q.at[b, 1]) if dz == 1 else (Q.at[near, 1], Q.at[to_near, 1]))
            late = [(W.at[0, near, 0], W.at[0, to_near, 0]), (Q.at[near, 0], Q.at[to_near, 0])]
        else:
            near_row, far_row, to = rows_of(dy)
            slot = 0 if dy == 1 else 2
            pairs = [(W.at[0, a, 1, :, near_row], HW.at[0, b, 1, to]),
                     (W.at[0, a, 1, :, far_row], HW.at[0, b, 2, to])]
            m, to_m = (near, to_near) if dz == -1 else (a, b)
            pairs.append((Q.at[m, 1, near_row], HQ.at[to_m, 1, slot]))
            if dy == 1:
                pairs.append((Q.at[m, 1, far_row], HQ.at[to_m, 1, 1]))
            n, to_n = (a, b) if dz == 0 else (near, to_near)
            late = [(W.at[0, n, 0, :, near_row], HW.at[0, to_n, 0, to]),
                    (Q.at[n, 0, near_row], HQ.at[to_n, 0, slot])]
        offset = len(pairs) if part == "late" else 0
        pairs = {"all": pairs + late, "early": pairs, "late": late}[part]
        return [remote(src, dst, qsend_sem.at[6 * k + offset + i], qrecv_sem.at[6 * k + offset + i], dz, dy)
                for i, (src, dst) in enumerate(pairs)]

    def b_copy(dy):
        row, to, i = (ny - 1, pl.ds(0, 3), 0) if dy == 1 else (0, pl.ds(3, 3), 1)
        return remote(BI.at[:, 0, :, row], HB.at[:, to], bsend_sem.at[i], brecv_sem.at[i], 0, dy)

    def for_all(make, backward, act, which=tuple(range(len(DIRECTIONS)))):
        for k in which:
            dz, dy = DIRECTIONS[k]
            sign = -1 if backward else 1

            @pl.when(exists(sign * dz, sign * dy))
            def _():
                for copy in make(k):
                    act(copy)

    def for_bottom(backward, act):
        for dy in (1, -1):
            @pl.when((d == nd - 1) & exists(0, -dy if backward else dy))
            def _():
                act(b_copy(dy))

    start = lambda copy: copy.start()
    for_all(first_copies, False, start, (6, 7))

    @pl.when(d < nd // 2)
    def _():
        for_all(first_copies, False, start, (0, 2, 3, 1, 4, 5))

    @pl.when(d >= nd // 2)
    def _():
        for_all(first_copies, False, start, (1, 4, 5, 0, 2, 3))

    for load in loads[first:]:
        load.wait()
    for r in range(rounds):
        for i in range(2):
            for c in range(3):
                BI[r, i, c] = 2.0 * MV[...].astype(f32) * IV[2 * r + i, c]
    for_bottom(False, start)

    def clear(n):
        for t in range(0, steps, 2):
            W[t, n] = jnp.zeros_like(W[t, n])
            HW[t, n] = jnp.zeros_like(HW[t, n])
        Q[n, 0] = jnp.zeros_like(Q[n, 0])
        Q[n, 1] = jnp.full_like(Q[n, 1], -1.0)
        HQ[n, 0] = jnp.zeros_like(HQ[n, 0])
        HQ[n, 1] = jnp.full_like(HQ[n, 1], -1.0)

    @pl.when(d == 0)
    def _():
        clear(0)
        clear(1)

    @pl.when(d == nd - 1)
    def _():
        clear(nz + 2)
        clear(nz + 3)

    def clear_side(rows, q_rows):
        for n in range(nz + 4):
            for t in range(0, steps, 2):
                for i in range(3):
                    HW[t, n, i, rows[0]:rows[1]] = jnp.zeros((3, nx), f32)
            HQ[n, 0, q_rows[0]:q_rows[1]] = jnp.zeros((q_rows[1] - q_rows[0], nx), f32)
            HQ[n, 1, q_rows[0]:q_rows[1]] = jnp.full((q_rows[1] - q_rows[0], nx), -1.0, f32)
        for r in range(rounds):
            HB[r, rows[0]:rows[1]] = jnp.zeros((3, nx), f32)

    @pl.when(d < nd - 1)
    def _():
        HB[...] = jnp.zeros_like(HB)

    @pl.when(l == 0)
    def _():
        clear_side((0, 3), (0, 2))

    @pl.when(l == nl - 1)
    def _():
        clear_side((3, 6), (2, 3))

    row = lax.broadcasted_iota(i32, (ny, nx), 0)
    lane = lax.broadcasted_iota(i32, (ny, nx), 1)

    def column_dofs(shape):
        j = lax.broadcasted_iota(i32, shape, 1)
        block = (j >= KB).astype(i32) + (j >= 2 * KB).astype(i32) + (j >= 3 * KB).astype(i32)
        j = j - KB * block
        bz = (j >= KL).astype(i32)
        j = j - KL * bz
        inner = j < 48
        bx_i = (j >= 24).astype(i32)
        c_i = (j - 24 * bx_i) >> 3
        y_i = j & 7
        h = j - 48
        far = (h >= 16).astype(i32)
        bx_h = (h >> 3) & 1
        r = h & 7
        s = (r >= 3).astype(i32)
        c_h = r - 3 * s
        y_h = jnp.where(r >= 6, 99, jnp.where(s == 0, -1 - far, 8 + far))
        y = jnp.where(inner, y_i, y_h)
        bx = jnp.where(inner, bx_i, bx_h)
        c = jnp.where(inner, c_i, c_h)
        return block, jnp.where(block < 3, y, 99), 12 * bz + 3 * bx + c

    block, _, dof = column_dofs((24, KP))
    i24 = lax.broadcasted_iota(i32, (24, KP), 0)
    stiff = jnp.concatenate([KV[0], KV[1]], 0)
    block48, _, _ = column_dofs((48, KP))
    for by in (0, 1):
        one_hot = (i24 == dof + 6 * by).astype(f32)
        e = jnp.dot(stiff, one_hot, precision=lax.Precision.HIGHEST, preferred_element_type=f32)
        e_hi = e.astype(bf16).astype(f32)
        E[by] = jnp.where(block48 == 2, e - e_hi, e_hi)
    _, y_col, _ = column_dofs((8, KP))
    r8 = lax.broadcasted_iota(i32, (8, KP), 0)
    y_halo = jnp.where(r8 < 3, -1, jnp.where(r8 < 6, 8, 199))

    def band(y_row, ay, picks):
        e0, e1 = picks
        delta = y_col - y_row + ay
        return jnp.where(delta == 0, e0, jnp.where(delta == 1, e1, 0.0))

    def wide(by, q):
        return jnp.broadcast_to(E[by, q:q + 1], (8, KP))

    for q in range(0, 48, 2):
        tiles = [band(r8, (p // 6) % 2, (wide(0, p), wide(1, p))) for p in (q, q + 1)]
        at = [own_row(p // 3) + 8 * (p % 3) for p in (q, q + 1)]
        assert at[1] == at[0] + 8 and at[0] % 16 == 0
        WM[at[0]:at[0] + 16] = jnp.concatenate(tiles, 0).astype(bf16)
    for g in range(0, 16, 2):
        tiles = []
        for p in (g, g + 1):
            picks = []
            for by in (0, 1):
                a, b, c = (wide(by, 3 * p + i) for i in range(3))
                picks.append(jnp.where((r8 == 0) | (r8 == 3), a, jnp.where((r8 == 1) | (r8 == 4), b, c)))
            tiles.append(band(y_halo, (p // 2) % 2, picks))
        WM[halo_row(g):halo_row(g) + 16] = jnp.concatenate(tiles, 0).astype(bf16)

    def fields(n):
        def full(x):
            return jnp.broadcast_to(x, (ny, nx))
        mat = Q[n, 1]
        m1, m2, m8 = full(HQ[n, 1, 0:1]), full(HQ[n, 1, 1:2]), full(HQ[n, 1, 2:3])
        m7 = full(Q[n, 1, ny - 1:ny])
        before = jnp.where(row == 0, m1, pltpu.roll(mat, 1, 0))
        for ref, ay, m in ((FD, 0, mat), (FD, 1, before), (FH, 0, jnp.where(row < 3, m1, m8)),
                           (FH, 1, jnp.where(row < 3, m2, m7))):
            for f, table in ((0, dil), (1, she)):
                value = jnp.zeros((ny, nx), f32)
                for level in range(table.shape[0]):
                    value = jnp.where(m == float(level), table[level], value)
                ref[n, f, ay] = value

    def masses(n):
        low, high = HQ[n, 0, 0:1], HQ[n, 0, 2:3]
        HIM[n] = DT * jnp.where(row < 3, jnp.broadcast_to(low, (ny, nx)), jnp.broadcast_to(high, (ny, nx)))

    here = lambda copy: copy.wait_recv()
    lat_k = (6, 7)
    for_all(first_copies, True, here, lat_k)
    for_bottom(True, here)

    @pl.loop(2, nz + 2)
    def _(n):
        fields(n)
        masses(n)

    at_bottom = (d == nd - 1).astype(f32)
    imp_rows = jnp.where((row == 0) | (row == 3), imp[0], jnp.where((row == 1) | (row == 4), imp[1], imp[2]))

    def ahead(x):
        return jnp.where(lane == nx - 1, 0.0, pltpu.roll(x, nx - 1, 1))

    def behind(x):
        return jnp.where(lane == 0, 0.0, pltpu.roll(x, 1, 1))

    def operand(t, n, extended):
        tiles = [W[t, n, 1, c] for c in range(3)]
        halo = [jnp.where(row < 6, HW[t, n, 1], 0.0)]
        if extended:
            halo.append(jnp.where(row < 6, HW[t, n, 2], 0.0))
        parts = tiles + [ahead(x) for x in tiles]
        for x in halo:
            parts += [x, ahead(x)]
        if not extended:
            parts += [jnp.zeros((ny, nx), f32)] * 2
        x = jnp.concatenate(parts, 0)
        hi = x.astype(bf16)
        XH[n] = hi
        XL[n] = (x - hi.astype(f32)).astype(bf16)

    def element(e, extended, which):
        a = (0 if extended else 64) if 0 in which else 256
        b = (MH if extended else 448) if 1 in which else 256
        x = jnp.concatenate([XH[e], XH[e + 1], XL[e], XL[e + 1], XH[e], XH[e + 1],
                             jnp.zeros((KP - 3 * KB, nx), bf16)], 0)
        slot = e % 4
        PR[slot, a:b] = jnp.dot(WM[a:b], x, preferred_element_type=f32)
        sides = {}
        for az in which:
            sums = {}
            for ax in (0, 1):
                for c in range(4 if extended else 3):
                    total = None
                    for f in (0, 1):
                        for ay in (0, 1):
                            g = 8 * f + 4 * az + 2 * ay + ax
                            if c < 3:
                                at = own_row(g) + 8 * c
                                term = FD[e, f, ay] * PR[slot, at:at + 8]
                            else:
                                at = halo_row(g)
                                term = FH[e, f, ay] * PR[slot, at:at + 8]
                            total = term if total is None else total + term
                    sums[ax, c] = total
            sides[az] = sums
        return sides

    def advance(t, r, n, before, after, extended):
        force = [after[0, c] + before[0, c] + behind(after[1, c] + before[1, c])
                 for c in range(4 if extended else 3)]
        scale = DT * Q[n, 0]
        for c in range(3):
            net = -force[c]
            v = W[t, n, 0, c]
            if n == nz + 1:
                net = net + at_bottom * imp[c] * (BI[t // 2, r, c] - v)
            v = v + scale * net
            W[t + 1, n, 0, c] = v
            W[t + 1, n, 1, c] = W[t, n, 1, c] + DT * v
        if extended:
            net = -force[3]
            v = HW[t, n, 0]
            if n == nz + 1:
                net = net + at_bottom * imp_rows * (HB[t // 2] - v)
            v = v + HIM[n] * net
            HW[t + 1, n, 1] = HW[t, n, 1] + DT * v

    def run(t, r, extended, order, nodes, low, high):
        for e in order:
            first_e, last_e = (0, nz + 2) if extended else (1, nz + 1)
            which = (1,) if e == first_e else (0,) if e == last_e else (0, 1)
            sides = element(e, extended, which)
            if 0 in which:
                low[e] = sides[0]
            if 1 in which:
                high[e] = sides[1]
            for n in (e, e + 1):
                if n in nodes and n in low and n - 1 in high:
                    advance(t, r, n, high[n - 1], low[n], extended)
                    nodes.remove(n)

    def follow_tile(t, n):
        HW[t, n, 0] = (HW[t, n, 1] - HW[t - 1, n, 1]) * (1.0 / DT)

    def follow_layer(t, n):
        for c in range(3):
            W[t, n, 0, c] = (W[t, n, 1, c] - W[t - 1, n, 1, c]) * (1.0 / DT)

    top = nz + 2

    @pl.loop(0, rounds)
    def _(i):
        t = 2 * i

        sides = {
            "low": ((0, 2, 3), (1, 0), 1, (1, 0)),
            "high": ((1, 4, 5), (top, top + 1), top, (top - 1, top)),
        }

        def finish_side(name, up, low, high, nodes):
            which, layers_in, edge, order = sides[name]

            @pl.when(i == 0)
            def _():
                for_all(first_copies, True, here, which)
                for n in (0, 1) if name == "low" else (top,):
                    fields(n)
                masses(edge)

            @pl.when(i > 0)
            def _():
                for_all(lambda k: copies(t, k, up), True, here, which)
                follow_tile(t, edge)
                follow_layer(t, edge)

            for n in layers_in:
                operand(t, n, True)
            run(t, 0, True, order, nodes, low, high)

        def work(up):
            near, far = ("low", "high") if up else ("high", "low")
            turn = (lambda x: list(x)) if up else (lambda x: list(x)[::-1])
            own_layers = turn(range(2, top))
            own_elements = turn(range(2, top - 1))
            layers_b = turn(range(1, top + 1))
            elements_b = turn(range(1, top))
            low_a, high_a, nodes_a = {}, {}, set(range(1, top + 1))
            low_b, high_b, nodes_b = {}, {}, set(range(2, top))

            def send(which, part="all"):
                @pl.when(i < rounds - 1)
                def _():
                    for_all(lambda k: copies(t + 2, k, up, part), False, start, which)

            def lat_rows(part, ns):
                @pl.when(i > 0)
                def _():
                    for_all(lambda k: copies(t, k, up, part), True, here, lat_k)
                    for n in ns:
                        follow_tile(t, n)

            def step_a(ns, es):
                for n in ns:
                    operand(t, n, True)
                run(t, 0, True, es, nodes_a, low_a, high_a)

            def step_b(ns, es):
                for n in ns:
                    operand(t + 1, n, False)
                run(t + 1, 1, False, es, nodes_b, low_b, high_b)

            def side_k(name):
                return (1, 4, 5) if name == "low" else (0, 2, 3)

            lat_rows("early", own_layers[:6])
            step_a(own_layers[:6], own_elements[:5])
            finish_side(near, up, low_a, high_a, nodes_a)
            step_b(layers_b[:6], elements_b[:5])
            send(side_k(near))
            lat_rows("late", own_layers[6:])
            step_a(own_layers[6:], own_elements[5:])
            step_b(layers_b[6:8], elements_b[5:7])
            send(lat_k, "early")
            finish_side(far, up, low_a, high_a, nodes_a)
            step_b(layers_b[8:], elements_b[7:])
            send(side_k(far))
            send(lat_k, "late")

        @pl.when(d < nd // 2)
        def _():
            work(True)

        @pl.when(d >= nd // 2)
        def _():
            work(False)

    for z in range(nz):
        for c in range(3):
            u_out[c, z] = W[steps, z + 2, 1, c]
            v_out[c, z] = W[steps, z + 2, 0, c]

    done = lambda copy: copy.wait_send()
    for_all(first_copies, False, done)
    for_bottom(False, done)

    @pl.loop(1, rounds)
    def _(i):
        @pl.when(d < nd // 2)
        def _():
            for_all(lambda k: copies(2 * i, k, True), False, done)

        @pl.when(d >= nd // 2)
        def _():
            for_all(lambda k: copies(2 * i, k, False), False, done)


def put_out(u, v, u_hbm, v_hbm, sem):
    copies = [pltpu.make_async_copy(a.at[c], b.at[c], sem.at[3 * i + c])
              for i, (a, b) in enumerate(((u, u_hbm), (v, v_hbm))) for c in range(3)]
    for copy in copies:
        copy.start()
    for copy in copies:
        copy.wait()


def per_device(nd, nl, displacement, velocity, inverse_mass, material, dilation_table, shear_table,
               stiffness_pair, impedance, bedrock_mask, incident):
    _, nz, ny, nx = displacement.shape
    steps = incident.shape[0]
    rounds = steps // 2
    nmat = dilation_table.shape[0]
    vmem = pl.BlockSpec(memory_space=pltpu.VMEM)
    hbm = pl.BlockSpec(memory_space=pltpu.MemorySpace.HBM)
    ext = nz + 4
    dma = pltpu.SemaphoreType.DMA
    state = pl.pallas_call(
        functools.partial(kernel, nd, nl),
        out_shape=[jax.ShapeDtypeStruct(displacement.shape, f32)] * 2,
        in_specs=[hbm] * 10,
        out_specs=[vmem, vmem],
        scratch_shapes=[
            pltpu.VMEM((steps + 1, ext, 2, 3, ny, nx), f32),
            pltpu.VMEM((steps, ext, 3, ny, nx), f32),
            pltpu.VMEM((ext, 2, ny, nx), f32),
            pltpu.VMEM((ext, 2, ny, nx), f32),
            pltpu.VMEM((rounds, 2, 3, ny, nx), f32),
            pltpu.VMEM((rounds, ny, nx), f32),
            pltpu.VMEM((nz, ny, nx), i32),
            pltpu.VMEM(stiffness_pair.shape, f32),
            pltpu.VMEM((ny, nx), i32),
            pltpu.VMEM((steps, 3, ny, nx), f32),
            pltpu.VMEM((2, 48, KP), f32),
            pltpu.VMEM((MH, KP), bf16),
            pltpu.VMEM((ext, KL, nx), bf16),
            pltpu.VMEM((ext, KL, nx), bf16),
            pltpu.VMEM((4, MH, nx), f32),
            pltpu.VMEM((ext, 2, 2, ny, nx), f32),
            pltpu.VMEM((ext, 2, 2, ny, nx), f32),
            pltpu.VMEM((ext, ny, nx), f32),
            pltpu.SMEM((nmat,), f32),
            pltpu.SMEM((nmat,), f32),
            pltpu.SMEM((3,), f32),
            dma((14,)),
            dma((rounds, 32)),
            dma((rounds, 32)),
            dma((48,)),
            dma((48,)),
            dma((2,)),
            dma((2,)),
        ],
        compiler_params=pltpu.CompilerParams(
            collective_id=0, has_side_effects=True, vmem_limit_bytes=48 * 1024 * 1024),
    )(*(pltpu.with_memory_space_constraint(x, pltpu.MemorySpace.HBM) for x in (
        displacement, velocity, inverse_mass, material, dilation_table, shear_table,
        stiffness_pair, impedance, bedrock_mask, incident)))
    return pl.pallas_call(
        put_out,
        out_shape=[jax.ShapeDtypeStruct(displacement.shape, f32)] * 2,
        in_specs=[vmem, vmem],
        out_specs=[pl.BlockSpec(memory_space=pltpu.MemorySpace.HBM)] * 2,
        scratch_shapes=[dma((6,))],
        compiler_params=pltpu.CompilerParams(vmem_limit_bytes=2 * 1024 * 1024),
    )(*state)


def solution(mesh):
    in_specs = (
        P(None, "depth", "lat", None),
        P(None, "depth", "lat", None),
        P("depth", "lat", None),
        P("depth", "lat", None),
        P(),
        P(),
        P(),
        P(),
        P("lat", None),
        P(None, None, "lat", None),
    )
    out_specs = (P(None, "depth", "lat", None), P(None, "depth", "lat", None))
    return jax.shard_map(
        functools.partial(per_device, mesh.shape["depth"], mesh.shape["lat"]),
        mesh=mesh, in_specs=in_specs, out_specs=out_specs, check_vma=False)
```

```python
import functools

import jax
import jax.numpy as jnp
from jax import lax
from jax.experimental import pallas as pl
from jax.experimental.pallas import tpu as pltpu
from jax.sharding import PartitionSpec as P

MESH = pl.DeviceIdType.MESH
DT = 0.1
f32, bf16, i32 = jnp.float32, jnp.bfloat16, jnp.int32
DIRECTIONS = ((1, 0), (-1, 0), (1, 1), (1, -1), (-1, 1), (-1, -1), (0, 1), (0, -1))

KL = 80
KB = 2 * KL
KP = 512
MH = 512


def own_row(g):
    f, az, rest = g // 8, (g // 4) % 2, g % 4
    return (64, 256)[az] + 96 * f + 24 * rest


def halo_row(g):
    f, az, rest = g // 8, (g // 4) % 2, g % 4
    return (0, 448)[az] + 32 * f + 8 * rest


def kernel(
    nd, nl,
    u_in, v_in, im_in, mat_in, dil_in, she_in, k_in, imp_in, mask_in, inc_in,
    u_out, v_out,
    W, HW, Q, HQ, BI, HB, MI, KV, MV, IV, E, WM, XH, XL, PR, FD, FH, HIM,
    dil, she, imp,
    in_sem, send_sem, recv_sem, qsend_sem, qrecv_sem, bsend_sem, brecv_sem,
):
    steps = inc_in.shape[0]
    rounds = steps // 2
    nz, ny, nx = im_in.shape
    d = lax.axis_index("depth")
    l = lax.axis_index("lat")

    def exists(dz, dy):
        return ((d + dz >= 0) & (d + dz < nd)) & ((l + dy >= 0) & (l + dy < nl))

    barrier = pltpu.get_barrier_semaphore()
    partners = 0
    for dz, dy in DIRECTIONS:
        @pl.when(exists(dz, dy))
        def _():
            pl.semaphore_signal(barrier, inc=1, device_id=(d + dz, l + dy), device_id_type=MESH)
        partners = partners + exists(dz, dy).astype(i32)
    own = pl.ds(2, nz)
    loads = [(im_in, Q.at[own, 0]), (mat_in, MI)]
    for c in range(3):
        loads.append((u_in.at[c], W.at[0, own, 1, c]))
        loads.append((v_in.at[c], W.at[0, own, 0, c]))
    first = len(loads)
    loads += [(k_in, KV), (mask_in, MV), (inc_in, IV), (dil_in, dil), (she_in, she), (imp_in, imp)]
    loads = [pltpu.make_async_copy(a, b, in_sem.at[i]) for i, (a, b) in enumerate(loads)]
    for load in loads:
        load.start()

    for load in loads[:first]:
        load.wait()
    for z in range(nz):
        Q[z + 2, 1] = MI[z].astype(f32)
    pl.semaphore_wait(barrier, partners)

    def remote(src, dst, ss, rs, dz, dy):
        return pltpu.make_async_remote_copy(
            src_ref=src, dst_ref=dst, send_sem=ss, recv_sem=rs,
            device_id=(d + dz, l + dy), device_id_type=MESH)

    def layers(dz):
        if dz == 0:
            return own, own
        return (pl.ds(nz, 2), pl.ds(0, 2)) if dz == 1 else (pl.ds(2, 2), pl.ds(nz + 2, 2))

    def rows_of(dy):
        return (ny - 1, ny - 2, pl.ds(0, 3)) if dy == 1 else (0, 1, pl.ds(3, 3))

    def copies(t, k, up, part="all"):
        dz, dy = DIRECTIONS[k]
        a, b = layers(dz)
        sem = 4 * k
        if dy == 0:
            pairs = [(W.at[t, a, 1], W.at[t, b, 1])]
        else:
            near_row, far_row, to = rows_of(dy)
            if dz == 0:
                early, late = (pl.ds(2, 6), pl.ds(8, 2)) if up else (pl.ds(4, 6), pl.ds(2, 2))
                spans = {"all": (early, late), "early": (early,), "late": (late,)}[part]
                pairs = []
                for span in spans:
                    pairs += [(W.at[t, span, 1, :, near_row], HW.at[t, span, 1, to]),
                              (W.at[t, span, 1, :, far_row], HW.at[t, span, 2, to])]
                sem += 2 if part == "late" else 0
            else:
                pairs = [(W.at[t, a, 1, :, near_row], HW.at[t, b, 1, to]),
                         (W.at[t, a, 1, :, far_row], HW.at[t, b, 2, to])]
        return [remote(src, dst, send_sem.at[t // 2, sem + i], recv_sem.at[t // 2, sem + i], dz, dy)
                for i, (src, dst) in enumerate(pairs)]

    def first_copies(k, part="all"):
        dz, dy = DIRECTIONS[k]
        a, b = layers(dz)
        near, far = (nz + 1, nz) if dz == 1 else (2, 3)
        to_near, to_far = (1, 0) if dz == 1 else (nz + 2, nz + 3)
        if dy == 0:
            pairs = [(W.at[0, a, 1], W.at[0, b, 1])]
            pairs.append((Q.at[a, 1], Q.at[b, 1]) if dz == 1 else (Q.at[near, 1], Q.at[to_near, 1]))
            late = [(W.at[0, near, 0], W.at[0, to_near, 0]), (Q.at[near, 0], Q.at[to_near, 0])]
        else:
            near_row, far_row, to = rows_of(dy)
            slot = 0 if dy == 1 else 2
            pairs = [(W.at[0, a, 1, :, near_row], HW.at[0, b, 1, to]),
                     (W.at[0, a, 1, :, far_row], HW.at[0, b, 2, to])]
            m, to_m = (near, to_near) if dz == -1 else (a, b)
            pairs.append((Q.at[m, 1, near_row], HQ.at[to_m, 1, slot]))
            if dy == 1:
                pairs.append((Q.at[m, 1, far_row], HQ.at[to_m, 1, 1]))
            n, to_n = (a, b) if dz == 0 else (near, to_near)
            late = [(W.at[0, n, 0, :, near_row], HW.at[0, to_n, 0, to]),
                    (Q.at[n, 0, near_row], HQ.at[to_n, 0, slot])]
        offset = len(pairs) if part == "late" else 0
        pairs = {"all": pairs + late, "early": pairs, "late": late}[part]
        return [remote(src, dst, qsend_sem.at[6 * k + offset + i], qrecv_sem.at[6 * k + offset + i], dz, dy)
                for i, (src, dst) in enumerate(pairs)]

    def b_copy(dy):
        row, to, i = (ny - 1, pl.ds(0, 3), 0) if dy == 1 else (0, pl.ds(3, 3), 1)
        return remote(BI.at[:, 0, :, row], HB.at[:, to], bsend_sem.at[i], brecv_sem.at[i], 0, dy)

    def for_all(make, backward, act, which=tuple(range(len(DIRECTIONS)))):
        for k in which:
            dz, dy = DIRECTIONS[k]
            sign = -1 if backward else 1

            @pl.when(exists(sign * dz, sign * dy))
            def _():
                for copy in make(k):
                    act(copy)

    def for_bottom(backward, act):
        for dy in (1, -1):
            @pl.when((d == nd - 1) & exists(0, -dy if backward else dy))
            def _():
                act(b_copy(dy))

    start = lambda copy: copy.start()
    for_all(first_copies, False, start, (6, 7))

    @pl.when(d < nd // 2)
    def _():
        for_all(first_copies, False, start, (0, 2, 3, 1, 4, 5))

    @pl.when(d >= nd // 2)
    def _():
        for_all(first_copies, False, start, (1, 4, 5, 0, 2, 3))

    for load in loads[first:]:
        load.wait()
    for r in range(rounds):
        for i in range(2):
            for c in range(3):
                BI[r, i, c] = 2.0 * MV[...].astype(f32) * IV[2 * r + i, c]
    for_bottom(False, start)

    def clear(n):
        for t in range(0, steps, 2):
            W[t, n] = jnp.zeros_like(W[t, n])
            HW[t, n] = jnp.zeros_like(HW[t, n])
        Q[n, 0] = jnp.zeros_like(Q[n, 0])
        Q[n, 1] = jnp.full_like(Q[n, 1], -1.0)
        HQ[n, 0] = jnp.zeros_like(HQ[n, 0])
        HQ[n, 1] = jnp.full_like(HQ[n, 1], -1.0)

    @pl.when(d == 0)
    def _():
        clear(0)
        clear(1)

    @pl.when(d == nd - 1)
    def _():
        clear(nz + 2)
        clear(nz + 3)

    def clear_side(rows, q_rows):
        for n in range(nz + 4):
            for t in range(0, steps, 2):
                for i in range(3):
                    HW[t, n, i, rows[0]:rows[1]] = jnp.zeros((3, nx), f32)
            HQ[n, 0, q_rows[0]:q_rows[1]] = jnp.zeros((q_rows[1] - q_rows[0], nx), f32)
            HQ[n, 1, q_rows[0]:q_rows[1]] = jnp.full((q_rows[1] - q_rows[0], nx), -1.0, f32)
        for r in range(rounds):
            HB[r, rows[0]:rows[1]] = jnp.zeros((3, nx), f32)

    @pl.when(d < nd - 1)
    def _():
        HB[...] = jnp.zeros_like(HB)

    @pl.when(l == 0)
    def _():
        clear_side((0, 3), (0, 2))

    @pl.when(l == nl - 1)
    def _():
        clear_side((3, 6), (2, 3))

    row = lax.broadcasted_iota(i32, (ny, nx), 0)
    lane = lax.broadcasted_iota(i32, (ny, nx), 1)

    def column_dofs(shape):
        j = lax.broadcasted_iota(i32, shape, 1)
        block = (j >= KB).astype(i32) + (j >= 2 * KB).astype(i32) + (j >= 3 * KB).astype(i32)
        j = j - KB * block
        bz = (j >= KL).astype(i32)
        j = j - KL * bz
        inner = j < 48
        bx_i = (j >= 24).astype(i32)
        c_i = (j - 24 * bx_i) >> 3
        y_i = j & 7
        h = j - 48
        far = (h >= 16).astype(i32)
        bx_h = (h >> 3) & 1
        r = h & 7
        s = (r >= 3).astype(i32)
        c_h = r - 3 * s
        y_h = jnp.where(r >= 6, 99, jnp.where(s == 0, -1 - far, 8 + far))
        y = jnp.where(inner, y_i, y_h)
        bx = jnp.where(inner, bx_i, bx_h)
        c = jnp.where(inner, c_i, c_h)
        return block, jnp.where(block < 3, y, 99), 12 * bz + 3 * bx + c

    block, _, dof = column_dofs((24, KP))
    i24 = lax.broadcasted_iota(i32, (24, KP), 0)
    stiff = jnp.concatenate([KV[0], KV[1]], 0)
    block48, _, _ = column_dofs((48, KP))
    for by in (0, 1):
        one_hot = (i24 == dof + 6 * by).astype(f32)
        e = jnp.dot(stiff, one_hot, precision=lax.Precision.HIGHEST, preferred_element_type=f32)
        e_hi = e.astype(bf16).astype(f32)
        E[by] = jnp.where(block48 == 2, e - e_hi, e_hi)
    _, y_col, _ = column_dofs((8, KP))
    r8 = lax.broadcasted_iota(i32, (8, KP), 0)
    y_halo = jnp.where(r8 < 3, -1, jnp.where(r8 < 6, 8, 199))

    def band(y_row, ay, picks):
        e0, e1 = picks
        delta = y_col - y_row + ay
        return jnp.where(delta == 0, e0, jnp.where(delta == 1, e1, 0.0))

    def wide(by, q):
        return jnp.broadcast_to(E[by, q:q + 1], (8, KP))

    for q in range(0, 48, 2):
        tiles = [band(r8, (p // 6) % 2, (wide(0, p), wide(1, p))) for p in (q, q + 1)]
        at = [own_row(p // 3) + 8 * (p % 3) for p in (q, q + 1)]
        assert at[1] == at[0] + 8 and at[0] % 16 == 0
        WM[at[0]:at[0] + 16] = jnp.concatenate(tiles, 0).astype(bf16)
    for g in range(0, 16, 2):
        tiles = []
        for p in (g, g + 1):
            picks = []
            for by in (0, 1):
                a, b, c = (wide(by, 3 * p + i) for i in range(3))
                picks.append(jnp.where((r8 == 0) | (r8 == 3), a, jnp.where((r8 == 1) | (r8 == 4), b, c)))
            tiles.append(band(y_halo, (p // 2) % 2, picks))
        WM[halo_row(g):halo_row(g) + 16] = jnp.concatenate(tiles, 0).astype(bf16)

    def fields(n):
        def full(x):
            return jnp.broadcast_to(x, (ny, nx))
        mat = Q[n, 1]
        m1, m2, m8 = full(HQ[n, 1, 0:1]), full(HQ[n, 1, 1:2]), full(HQ[n, 1, 2:3])
        m7 = full(Q[n, 1, ny - 1:ny])
        before = jnp.where(row == 0, m1, pltpu.roll(mat, 1, 0))
        for ref, ay, m in ((FD, 0, mat), (FD, 1, before), (FH, 0, jnp.where(row < 3, m1, m8)),
                           (FH, 1, jnp.where(row < 3, m2, m7))):
            for f, table in ((0, dil), (1, she)):
                value = jnp.zeros((ny, nx), f32)
                for level in range(table.shape[0]):
                    value = jnp.where(m == float(level), table[level], value)
                ref[n, f, ay] = value

    def masses(n):
        low, high = HQ[n, 0, 0:1], HQ[n, 0, 2:3]
        HIM[n] = DT * jnp.where(row < 3, jnp.broadcast_to(low, (ny, nx)), jnp.broadcast_to(high, (ny, nx)))

    here = lambda copy: copy.wait_recv()
    lat_k = (6, 7)
    for_all(first_copies, True, here, lat_k)
    for_bottom(True, here)

    @pl.loop(2, nz + 2)
    def _(n):
        fields(n)
        masses(n)

    at_bottom = (d == nd - 1).astype(f32)
    imp_rows = jnp.where((row == 0) | (row == 3), imp[0], jnp.where((row == 1) | (row == 4), imp[1], imp[2]))

    def ahead(x):
        return jnp.where(lane == nx - 1, 0.0, pltpu.roll(x, nx - 1, 1))

    def behind(x):
        return jnp.where(lane == 0, 0.0, pltpu.roll(x, 1, 1))

    def operand(t, n, extended):
        tiles = [W[t, n, 1, c] for c in range(3)]
        halo = [jnp.where(row < 6, HW[t, n, 1], 0.0)]
        if extended:
            halo.append(jnp.where(row < 6, HW[t, n, 2], 0.0))
        parts = tiles + [ahead(x) for x in tiles]
        for x in halo:
            parts += [x, ahead(x)]
        if not extended:
            parts += [jnp.zeros((ny, nx), f32)] * 2
        x = jnp.concatenate(parts, 0)
        hi = x.astype(bf16)
        XH[n] = hi
        XL[n] = (x - hi.astype(f32)).astype(bf16)

    def element(e, extended, which):
        a = (0 if extended else 64) if 0 in which else 256
        b = (MH if extended else 448) if 1 in which else 256
        x = jnp.concatenate([XH[e], XH[e + 1], XL[e], XL[e + 1], XH[e], XH[e + 1],
                             jnp.zeros((KP - 3 * KB, nx), bf16)], 0)
        slot = e % 4
        PR[slot, a:b] = jnp.dot(WM[a:b], x, preferred_element_type=f32)
        sides = {}
        for az in which:
            sums = {}
            for ax in (0, 1):
                for c in range(4 if extended else 3):
                    total = None
                    for f in (0, 1):
                        for ay in (0, 1):
                            g = 8 * f + 4 * az + 2 * ay + ax
                            if c < 3:
                                at = own_row(g) + 8 * c
                                term = FD[e, f, ay] * PR[slot, at:at + 8]
                            else:
                                at = halo_row(g)
                                term = FH[e, f, ay] * PR[slot, at:at + 8]
                            total = term if total is None else total + term
                    sums[ax, c] = total
            sides[az] = sums
        return sides

    def advance(t, r, n, before, after, extended):
        force = [after[0, c] + before[0, c] + behind(after[1, c] + before[1, c])
                 for c in range(4 if extended else 3)]
        scale = DT * Q[n, 0]
        for c in range(3):
            net = -force[c]
            v = W[t, n, 0, c]
            if n == nz + 1:
                net = net + at_bottom * imp[c] * (BI[t // 2, r, c] - v)
            v = v + scale * net
            u = W[t, n, 1, c] + DT * v
            W[t + 1, n, 0, c] = v
            W[t + 1, n, 1, c] = u
            if not extended:
                u_out[c, n - 2] = u
                v_out[c, n - 2] = v
        if extended:
            net = -force[3]
            v = HW[t, n, 0]
            if n == nz + 1:
                net = net + at_bottom * imp_rows * (HB[t // 2] - v)
            v = v + HIM[n] * net
            HW[t + 1, n, 1] = HW[t, n, 1] + DT * v

    def run(t, r, extended, order, nodes, low, high):
        for e in order:
            first_e, last_e = (0, nz + 2) if extended else (1, nz + 1)
            which = (1,) if e == first_e else (0,) if e == last_e else (0, 1)
            sides = element(e, extended, which)
            if 0 in which:
                low[e] = sides[0]
            if 1 in which:
                high[e] = sides[1]
            for n in (e, e + 1):
                if n in nodes and n in low and n - 1 in high:
                    advance(t, r, n, high[n - 1], low[n], extended)
                    nodes.remove(n)

    def follow_tile(t, n):
        HW[t, n, 0] = (HW[t, n, 1] - HW[t - 1, n, 1]) * (1.0 / DT)

    def follow_layer(t, n):
        for c in range(3):
            W[t, n, 0, c] = (W[t, n, 1, c] - W[t - 1, n, 1, c]) * (1.0 / DT)

    top = nz + 2

    @pl.loop(0, rounds)
    def _(i):
        t = 2 * i

        sides = {
            "low": ((0, 2, 3), (1, 0), 1, (1, 0)),
            "high": ((1, 4, 5), (top, top + 1), top, (top - 1, top)),
        }

        def finish_side(name, up, low, high, nodes):
            which, layers_in, edge, order = sides[name]

            @pl.when(i == 0)
            def _():
                for_all(first_copies, True, here, which)
                for n in (0, 1) if name == "low" else (top,):
                    fields(n)
                masses(edge)

            @pl.when(i > 0)
            def _():
                for_all(lambda k: copies(t, k, up), True, here, which)
                follow_tile(t, edge)
                follow_layer(t, edge)

            for n in layers_in:
                operand(t, n, True)
            run(t, 0, True, order, nodes, low, high)

        def work(up):
            near, far = ("low", "high") if up else ("high", "low")
            turn = (lambda x: list(x)) if up else (lambda x: list(x)[::-1])
            own_layers = turn(range(2, top))
            own_elements = turn(range(2, top - 1))
            layers_b = turn(range(1, top + 1))
            elements_b = turn(range(1, top))
            low_a, high_a, nodes_a = {}, {}, set(range(1, top + 1))
            low_b, high_b, nodes_b = {}, {}, set(range(2, top))

            def send(which, part="all"):
                @pl.when(i < rounds - 1)
                def _():
                    for_all(lambda k: copies(t + 2, k, up, part), False, start, which)

            def lat_rows(part, ns):
                @pl.when(i > 0)
                def _():
                    for_all(lambda k: copies(t, k, up, part), True, here, lat_k)
                    for n in ns:
                        follow_tile(t, n)

            def step_a(ns, es):
                for n in ns:
                    operand(t, n, True)
                run(t, 0, True, es, nodes_a, low_a, high_a)

            def step_b(ns, es):
                for n in ns:
                    operand(t + 1, n, False)
                run(t + 1, 1, False, es, nodes_b, low_b, high_b)

            def side_k(name):
                return (1, 4, 5) if name == "low" else (0, 2, 3)

            lat_rows("early", own_layers[:6])
            step_a(own_layers[:6], own_elements[:5])
            finish_side(near, up, low_a, high_a, nodes_a)
            step_b(layers_b[:6], elements_b[:5])
            send(side_k(near))
            lat_rows("late", own_layers[6:])
            step_a(own_layers[6:], own_elements[5:])
            step_b(layers_b[6:8], elements_b[5:7])
            send(lat_k, "early")
            finish_side(far, up, low_a, high_a, nodes_a)
            step_b(layers_b[8:], elements_b[7:])
            send(side_k(far))
            send(lat_k, "late")

        @pl.when(d < nd // 2)
        def _():
            work(True)

        @pl.when(d >= nd // 2)
        def _():
            work(False)

    done = lambda copy: copy.wait_send()
    for_all(first_copies, False, done)
    for_bottom(False, done)

    @pl.loop(1, rounds)
    def _(i):
        @pl.when(d < nd // 2)
        def _():
            for_all(lambda k: copies(2 * i, k, True), False, done)

        @pl.when(d >= nd // 2)
        def _():
            for_all(lambda k: copies(2 * i, k, False), False, done)


def put_out(u, v, u_hbm, v_hbm, sem):
    copies = [pltpu.make_async_copy(a.at[c], b.at[c], sem.at[3 * i + c])
              for i, (a, b) in enumerate(((u, u_hbm), (v, v_hbm))) for c in range(3)]
    for copy in copies:
        copy.start()
    for copy in copies:
        copy.wait()


def per_device(nd, nl, displacement, velocity, inverse_mass, material, dilation_table, shear_table,
               stiffness_pair, impedance, bedrock_mask, incident):
    _, nz, ny, nx = displacement.shape
    steps = incident.shape[0]
    rounds = steps // 2
    nmat = dilation_table.shape[0]
    vmem = pl.BlockSpec(memory_space=pltpu.VMEM)
    hbm = pl.BlockSpec(memory_space=pltpu.MemorySpace.HBM)
    ext = nz + 4
    dma = pltpu.SemaphoreType.DMA
    state = pl.pallas_call(
        functools.partial(kernel, nd, nl),
        out_shape=[jax.ShapeDtypeStruct(displacement.shape, f32)] * 2,
        in_specs=[hbm] * 10,
        out_specs=[vmem, vmem],
        scratch_shapes=[
            pltpu.VMEM((steps + 1, ext, 2, 3, ny, nx), f32),
            pltpu.VMEM((steps, ext, 3, ny, nx), f32),
            pltpu.VMEM((ext, 2, ny, nx), f32),
            pltpu.VMEM((ext, 2, ny, nx), f32),
            pltpu.VMEM((rounds, 2, 3, ny, nx), f32),
            pltpu.VMEM((rounds, ny, nx), f32),
            pltpu.VMEM((nz, ny, nx), i32),
            pltpu.VMEM(stiffness_pair.shape, f32),
            pltpu.VMEM((ny, nx), i32),
            pltpu.VMEM((steps, 3, ny, nx), f32),
            pltpu.VMEM((2, 48, KP), f32),
            pltpu.VMEM((MH, KP), bf16),
            pltpu.VMEM((ext, KL, nx), bf16),
            pltpu.VMEM((ext, KL, nx), bf16),
            pltpu.VMEM((4, MH, nx), f32),
            pltpu.VMEM((ext, 2, 2, ny, nx), f32),
            pltpu.VMEM((ext, 2, 2, ny, nx), f32),
            pltpu.VMEM((ext, ny, nx), f32),
            pltpu.SMEM((nmat,), f32),
            pltpu.SMEM((nmat,), f32),
            pltpu.SMEM((3,), f32),
            dma((14,)),
            dma((rounds, 32)),
            dma((rounds, 32)),
            dma((48,)),
            dma((48,)),
            dma((2,)),
            dma((2,)),
        ],
        compiler_params=pltpu.CompilerParams(
            collective_id=0, has_side_effects=True, vmem_limit_bytes=48 * 1024 * 1024),
    )(*(pltpu.with_memory_space_constraint(x, pltpu.MemorySpace.HBM) for x in (
        displacement, velocity, inverse_mass, material, dilation_table, shear_table,
        stiffness_pair, impedance, bedrock_mask, incident)))
    return pl.pallas_call(
        put_out,
        out_shape=[jax.ShapeDtypeStruct(displacement.shape, f32)] * 2,
        in_specs=[vmem, vmem],
        out_specs=[pl.BlockSpec(memory_space=pltpu.MemorySpace.HBM)] * 2,
        scratch_shapes=[dma((6,))],
        compiler_params=pltpu.CompilerParams(vmem_limit_bytes=2 * 1024 * 1024),
    )(*state)


def solution(mesh):
    in_specs = (
        P(None, "depth", "lat", None),
        P(None, "depth", "lat", None),
        P("depth", "lat", None),
        P("depth", "lat", None),
        P(),
        P(),
        P(),
        P(),
        P("lat", None),
        P(None, None, "lat", None),
    )
    out_specs = (P(None, "depth", "lat", None), P(None, "depth", "lat", None))
    return jax.shard_map(
        functools.partial(per_device, mesh.shape["depth"], mesh.shape["lat"]),
        mesh=mesh, in_specs=in_specs, out_specs=out_specs, check_vma=False)
```
